512 devices in a mesh: samp: 64 (over z, x, y_hi), feat: 8 (over y_lo, core).
Axes of the slice: x: 4, y: 8 (y_hi: 2, y_lo: 4; y = y_hi * 4 + y_lo), z: 8, core: 2. Of those that a mesh axis runs over, the one named last changes fastest.
Arguments:
- design_matrix: bfloat16 [8192, 32768], P('samp', 'feat'), may hold values from -0.09375 to 0.09375
- labels: int32 [8192], P('samp'), may hold values from 0 to 1
- weights: float32 [16, 32768], P(None, ('feat', 'samp')), may hold values from -6 to 6
- lambdas: float32 [16], replicated, may hold values from 0.05 to 1
- sketch: bfloat16 [32768, 384], P(('feat', 'samp')), may hold values from -0.03125 to 0.03125
- sketch_values: float32 [384], replicated, may hold values from 0.05 to 2
Outputs:
- new_weights: float32 [16, 32768], P(None, ('feat', 'samp'))
The draws below stay inside these ranges and needn't reach their ends.
All inputs are finite; a program needn't handle non-finite values.
Results may differ from the reference program's by a relative error of at most 0.004.
Values may be sent and summed in bfloat16 or wider, within the bound.
A program may use at most 64 MiB of HBM per device.

```python
import math
import jax
import jax.numpy as jnp
from jax import lax

FEATURES = 32768
RANK = 384
STRENGTHS = 16
ITERS = 2
SAMPLES = 8192


def place_ends(result, key, low, largest):
    shape = result.shape
    index_at = [jax.random.randint(jax.random.fold_in(key, axis), (), 0, shape[axis]) for axis in range(len(shape))]
    result = result.at[tuple(index_at)].set(low)
    longest = shape.index(max(shape))
    index_at[longest] = (index_at[longest] + 1) % shape[longest]
    return result.at[tuple(index_at)].set(largest)


def strengthened(array, own_key, source, target, blocks, factor):
    owner, partner = [(jnp.arange(array.shape[position]) // (array.shape[position] // blocks)).reshape([-1 if axis == position else 1 for axis in range(array.ndim)]) for position in (source, target)]
    chosen = jax.random.permutation(own_key, blocks)[partner]
    strong = (owner == chosen) | (owner == (partner + blocks // 2) % blocks)
    return jnp.where(strong, factor * array, array)


def shard_levels(own_key, shape, pieces, low, top_value):
    gain, own = 1.0, jax.random.fold_in(own_key, 6)
    for position, shards_of in pieces:
        steps = jnp.exp(jax.random.uniform(jax.random.fold_in(own, position), (shards_of,), jnp.float32, low / len(pieces), top_value / len(pieces)))
        gain = gain * jnp.repeat(steps, shape[position] // shards_of).reshape([-1 if axis == position else 1 for axis in range(len(shape))])
    return gain


def noise(stream_key, extent, width, most, split=(), held_as=jnp.bfloat16):
    gain = shard_levels(stream_key, extent, split, -0.22, 0.18) if split else 1.0
    values = jax.random.normal(stream_key, extent, jnp.float32) * width * gain
    return jnp.minimum(jnp.maximum(values, -most), most).astype(held_as)


def heavy_noise(key, shape, scale, bound, shards, heavy, kind=jnp.bfloat16):
    values = scale * jax.random.normal(key, shape, jnp.float32)
    if shards:
        values = values * shard_levels(key, shape, shards, -0.22, 0.18)
    return jnp.clip(strengthened(values, jax.random.fold_in(key, 3), *heavy), -bound, bound).astype(kind)


def setup_inputs(seed: int = 0) -> dict:
    arg_keys = jax.random.split(jax.random.key(seed), 7)
    design_matrix = heavy_noise(arg_keys[0], (SAMPLES, FEATURES), FEATURES ** -0.5, 0.09375, ((0, 64), (1, 8)), (0, 1, 64, 4.0))
    labels = place_ends(jax.random.randint(arg_keys[1], (SAMPLES,), 0, 2), jax.random.fold_in(arg_keys[1], 1), 0, 1).astype(jnp.int32)
    weights = noise(arg_keys[2], (STRENGTHS, FEATURES), 1.0, 6.0, ((1, 512),), jnp.float32)
    lambdas = jnp.clip(jnp.exp(jax.random.uniform(arg_keys[3], (STRENGTHS,), jnp.float32, math.log(0.05), math.log(1.0))), 0.05, 1.0)
    sketch = noise(arg_keys[4], (FEATURES, RANK), FEATURES ** -0.5, 0.03125, ((0, 512),))
    sketch_values = jnp.clip(jnp.exp(jax.random.uniform(arg_keys[5], (RANK,), jnp.float32, math.log(0.05), math.log(2.0))), 0.05, 2.0)
    return dict(design_matrix=design_matrix, labels=labels, weights=weights, lambdas=lambdas, sketch=sketch, sketch_values=sketch_values)


def reference(design_matrix, labels, weights, lambdas, sketch, sketch_values):
    sketch_full = sketch.astype(jnp.float32)
    smallest = jnp.min(sketch_values)
    ratios = (smallest + lambdas[:, None]) / (sketch_values[None, :] + lambdas[:, None]) - 1.0

    def apply_rows(vector):
        return lax.dot_general(vector.astype(jnp.bfloat16), design_matrix, (((1,), (1,)), ((), ())), preferred_element_type=jnp.float32)

    def apply_columns(values):
        return jnp.dot(values, design_matrix, preferred_element_type=jnp.float32)

    def precondition(residual):
        projected = jnp.dot(residual, sketch_full, precision=lax.Precision.HIGHEST)
        correction = lax.dot_general(ratios * projected, sketch_full, (((1,), (1,)), ((), ())), precision=lax.Precision.HIGHEST)
        precond_res = residual + correction
        return precond_res, jnp.sum(residual * precond_res, axis=1)

    logits = apply_rows(weights)
    probability = jax.nn.sigmoid(logits)
    hessian_diag = probability * (1.0 - probability)
    miss_rows = (probability - labels[None, :].astype(jnp.float32)).astype(jnp.bfloat16)
    gradient = apply_columns(miss_rows) + lambdas[:, None] * weights
    residual = -gradient
    precond_res, res_dot = precondition(residual)
    direction = precond_res
    update = jnp.zeros_like(weights)
    for iteration in range(ITERS):
        image_rows = apply_rows(direction)
        hess_dir = apply_columns((hessian_diag * image_rows).astype(jnp.bfloat16)) + lambdas[:, None] * direction
        step_size = res_dot / jnp.sum(direction * hess_dir, axis=1)
        update = update + step_size[:, None] * direction
        if iteration + 1 < ITERS:
            residual = residual - step_size[:, None] * hess_dir
            precond_res, new_dot = precondition(residual)
            direction = precond_res + (new_dot / res_dot)[:, None] * direction
            res_dot = new_dot
    return weights + update
```

```python
import functools

import jax
import jax.numpy as jnp
from jax import lax
from jax.experimental import pallas as pl
from jax.experimental.pallas import tpu as pltpu
from jax.sharding import Mesh
from jax.sharding import PartitionSpec as P

SAMP = ("samp_0", "samp_1", "samp_2")
FEAT = ("feat_0", "feat_1")
FEAT_SAMP = FEAT + SAMP
F32, BF16 = jnp.float32, jnp.bfloat16
BY_LANES = (((1,), (1,)), ((), ()))
BY_ROWS = (((1,), (0,)), ((), ()))


def far_first(n):
    return sorted(range(n), key=lambda d: -min(d, n - d))


def split3(value):
    high = value.astype(BF16)
    rest = value - high.astype(F32)
    mid = rest.astype(BF16)
    low = (rest - mid.astype(F32)).astype(BF16)
    return jnp.concatenate([high, mid, low], axis=0)


def kernel(sizes, x_hbm, labels_ref, w_ref, lam_ref, s_hbm, sv_ref, out_ref,
           xv, sp, wb, ag, ags, ft, fts, fs, fss, rs, rss, yh, yhs, pr, prs, pz, pzs, pa, pas, kz, kzs, ky, kys,
           local_sem, send_sem, recv_sem):
    nz, nx, nh, nl, nc = sizes
    nzx, nf, ny = nz * nx, nl * nc, nh * nl * nc
    k, half = w_ref.shape
    wide = 2 * half
    rank = s_hbm.shape[1]
    z, x, h, l, c = (lax.axis_index(name) for name in SAMP + FEAT)
    zx, f, y = z * nx + x, l * nc + c, (h * nl + l) * nc + c

    copy_x = pltpu.make_async_copy(x_hbm, xv, local_sem.at[0])
    copy_x.start()
    copy_s = pltpu.make_async_copy(s_hbm, sp.at[h], local_sem.at[1])
    copy_s.start()

    zx_peers = []
    for dz in far_first(nz):
        for dx in far_first(nx):
            if dz or dx:
                zz, xx = lax.rem(z + dz, nz), lax.rem(x + dx, nx)
                zx_peers.append((zz * nx + xx, {"samp_0": zz, "samp_1": xx}))
    y_peers, f_peers = [], []
    for dl in far_first(nl):
        for dh in reversed(range(nh)):
            for dc in reversed(range(nc)):
                if dh or dl or dc:
                    hh, ll, cc = lax.rem(h + dh, nh), lax.rem(l + dl, nl), lax.rem(c + dc, nc)
                    y_peers.append(((hh * nl + ll) * nc + cc, {"samp_2": hh, "feat_0": ll, "feat_1": cc}))
                    if not dh:
                        f_peers.append((ll * nc + cc, {"feat_0": ll, "feat_1": cc}))
    partner = {"samp_2": 1 - h}

    barrier = pltpu.get_barrier_semaphore()
    for _, peer in zx_peers + y_peers:
        pl.semaphore_signal(barrier, inc=1, device_id=peer, device_id_type=pl.DeviceIdType.MESH)

    def copy(phase, src, dst, peer):
        return pltpu.make_async_remote_copy(
            src_ref=src, dst_ref=dst, send_sem=send_sem.at[phase], recv_sem=recv_sem.at[phase],
            device_id=peer, device_id_type=pl.DeviceIdType.MESH)

    sent = []

    def whole(phase, buffer, peer):
        arrived = copy(phase, buffer, buffer, peer)
        arrived.wait_recv()
        sent.append(arrived)

    lane = lax.broadcasted_iota(jnp.int32, (k, wide), 1)
    row = lax.broadcasted_iota(jnp.int32, (k, wide), 0)

    def pack(*columns):
        total = 0.0
        for place, column in enumerate(columns):
            total = total + jnp.where(lane == row + place * k, column, 0.0)
        return jnp.sum(total, axis=0, keepdims=True)

    def unpack(packed, place):
        return jnp.sum(jnp.where(lane == row + place * k, packed, 0.0), axis=1, keepdims=True)

    def lanes(value):
        return jnp.sum(value, axis=1, keepdims=True)

    def gather_start(i, value):
        ags[i] = value.astype(BF16)
        ag[i, zx] = value.astype(BF16)
        for _, peer in zx_peers:
            copy(2 + i, ags.at[i], ag.at[i, zx], peer).start()

    def gather_rows(i):
        whole(2 + i, ag.at[i, pl.ds(0, nzx - 1)], zx_peers[0][1])
        field = jnp.concatenate([ag[i, q] for q in range(nzx)], axis=1)
        return lax.dot_general(field, xv[...], BY_LANES, preferred_element_type=F32)

    def feat_sum(i, value):
        fts[i] = value
        ft[i, f] = value
        for _, peer in f_peers:
            copy(5 + i, fts.at[i], ft.at[i, f], peer).start()
        whole(5 + i, ft.at[i, pl.ds(0, nf - 1)], f_peers[0][1])
        return jnp.sum(ft[i], axis=0)

    def feat_scalars_start(i, value):
        fss[i] = value
        fs[i, f] = value
        for _, peer in f_peers:
            copy(8 + i, fss.at[i], fs.at[i, f], peer).start()

    def feat_scalars(i):
        whole(8 + i, fs.at[i, pl.ds(0, nf - 1)], f_peers[0][1])
        return jnp.sum(fs[i], axis=0)

    def column_sum(i, values):
        for dz in far_first(nz):
            zz = lax.rem(z + dz, nz)
            start = pl.multiple_of(zz * (nx * wide), nx * wide)
            part = lax.dot_general(values, xv[:, pl.ds(start, nx * wide)], BY_ROWS, preferred_element_type=F32)
            for xx in range(nx):
                rss[i, zz * nx + xx] = part[:, xx * wide:(xx + 1) * wide].astype(BF16)
            for dx in far_first(nx):
                if dz or dx:
                    xx = lax.rem(x + dx, nx)
                    copy(10 + i, rss.at[i, zz * nx + xx], rs.at[i, zx], {"samp_0": zz, "samp_1": xx}).start()
        rs[i, zx] = rss[i, zx]
        whole(10 + i, rs.at[i, pl.ds(0, nzx - 1)], zx_peers[0][1])
        return jnp.sum(rs[i].astype(F32), axis=0)

    def pair_start(i, value):
        yhs[i] = value
        copy(12 + i, yhs.at[i], yh.at[i], partner).start()

    def pair_sum(i, value):
        whole(12 + i, yh.at[i], partner)
        return value + yh[i]

    def project(i, value, scalars):
        parts = lax.dot_general(split3(value), sketch, BY_ROWS, preferred_element_type=F32)
        part = parts[:k] + parts[k:2 * k] + parts[2 * k:]
        for q in range(k):
            prs[i, q] = part[q:q + 1, :]
        for j, peer in y_peers:
            copy(14 + i, prs.at[i, j], pr.at[i, y], peer).start()
        pr[i, y] = prs[i, y]
        whole(14 + i, pr.at[i, pl.ds(0, ny - 1)], y_peers[0][1])
        mine = jnp.concatenate([jnp.sum(pr[i], axis=0), scalars], axis=1)
        pzs[i] = mine
        pz[i, zx] = mine
        for _, peer in zx_peers:
            copy(16 + i, pzs.at[i], pz.at[i, zx], peer).start()
        whole(16 + i, pz.at[i, pl.ds(0, nzx - 1)], zx_peers[0][1])
        mine = jnp.sum(pz[i], axis=0)
        pas[i] = mine
        pa[i, y] = mine
        for _, peer in y_peers:
            copy(18 + i, pas.at[i], pa.at[i, y], peer).start()
        whole(18 + i, pa.at[i, pl.ds(0, ny - 1)], y_peers[0][1])
        full = jnp.concatenate([pa[i, q] for q in range(k)], axis=0)
        return full[:, :rank], jnp.sum(full[:, rank:], axis=0, keepdims=True) * (1.0 / nf)

    def spread(projected):
        parts = lax.dot_general(split3(ratios * projected), sketch, BY_LANES, preferred_element_type=F32)
        return parts[:k] + parts[k:2 * k] + parts[2 * k:]

    lam = jnp.sum(jnp.where(lax.broadcasted_iota(jnp.int32, (k, k), 0) == lax.broadcasted_iota(jnp.int32, (k, k), 1),
                            lam_ref[...], 0.0), axis=1, keepdims=True)
    values = sv_ref[...]
    ratios = (jnp.min(values, axis=1, keepdims=True) + lam) / (values + lam) - 1.0
    wb[0, :, :half] = w_ref[...]
    wb[0, :, half:] = w_ref[...]
    pl.semaphore_wait(barrier, len(zx_peers) + len(y_peers))
    copy(0, wb.at[0], wb.at[1], partner).start()
    whole(0, wb.at[1], partner)
    own = (lane // half) == h
    weights = jnp.where(own, wb[0], wb[1])
    gather_start(0, weights)
    copy_s.wait()
    copy(1, sp.at[h], sp.at[h], partner).start()
    copy_x.wait()

    logits = feat_sum(0, gather_rows(0))
    probability = jax.nn.sigmoid(logits)
    diag = probability * (1.0 - probability)
    miss = (probability - labels_ref[...].astype(F32)).astype(BF16)
    part = -(column_sum(0, miss) + (0.5 * lam) * weights)
    pair_start(0, part)
    whole(1, sp.at[1 - h], partner)
    sketch = sp[...].reshape(2 * half, rank)
    projected, _ = project(0, part, jnp.zeros((1, wide), F32))
    residual = pair_sum(0, part)
    direction = residual + spread(projected)

    gather_start(1, direction)
    feat_scalars_start(0, pack(0.5 * lanes(residual * direction), 0.5 * lam * lanes(direction * direction)))
    image = feat_sum(1, gather_rows(1))
    scalars = feat_scalars(0) + pack(jnp.zeros((k, 1), F32), lanes(diag * image * image))
    part = column_sum(1, (diag * image).astype(BF16)) + (0.5 * lam) * direction
    pair_start(1, part)
    projected, scalars = project(1, part, scalars)
    hess_dir = pair_sum(1, part)
    hess_pre = hess_dir + spread(projected)
    res_dot, curvature = unpack(scalars, 0), unpack(scalars, 1)
    step = res_dot / curvature
    residual = residual - step * hess_dir
    precond = direction - step * hess_pre

    gather_start(2, precond)
    feat_scalars_start(1, pack(0.5 * lanes(residual * precond), 0.5 * lam * lanes(precond * precond),
                               0.5 * lam * lanes(precond * direction)))
    image_pre = feat_sum(2, gather_rows(2))
    mine = feat_scalars(1) + pack(jnp.zeros((k, 1), F32), lanes(diag * image_pre * image_pre),
                                  lanes(diag * image_pre * image))
    kzs[...] = mine
    kz[zx] = mine
    for _, peer in zx_peers:
        copy(20, kzs, kz.at[zx], peer).start()
    whole(20, kz.at[pl.ds(0, nzx - 1)], zx_peers[0][1])
    mine = jnp.sum(kz[...], axis=0)
    kys[...] = mine
    copy(21, kys, ky, partner).start()
    whole(21, ky, partner)
    scalars = mine + ky[...]
    new_dot, pre_pre, pre_dir = (unpack(scalars, place) for place in range(3))
    beta = new_dot / res_dot
    last = new_dot / (pre_pre + 2.0 * beta * pre_dir + beta * beta * curvature)
    out_ref[...] = step * direction + last * (precond + beta * direction)
    for arrived in sent:
        arrived.wait_send()


def shards(sizes, design_matrix, labels, weights, lambdas, sketch, sketch_values):
    nz, nx, nh, nl, nc = sizes
    nzx, nf, ny = nz * nx, nl * nc, nh * nl * nc
    k, half = weights.shape
    wide = 2 * half
    rank = sketch.shape[1]
    vmem = pl.BlockSpec(memory_space=pltpu.VMEM)
    anywhere = pl.BlockSpec(memory_space=pl.ANY)
    dma = pltpu.SemaphoreType.DMA
    update = pl.pallas_call(
        functools.partial(kernel, sizes),
        name="step",
        out_shape=jax.ShapeDtypeStruct((k, wide), F32),
        in_specs=[anywhere, vmem, vmem, vmem, anywhere, vmem],
        out_specs=vmem,
        scratch_shapes=[
            pltpu.VMEM(design_matrix.shape, BF16),
            pltpu.VMEM((2, half, rank), BF16),
            pltpu.VMEM((2, k, wide), F32),
            pltpu.VMEM((3, nzx, k, wide), BF16), pltpu.VMEM((3, k, wide), BF16),
            pltpu.VMEM((3, nf, k, wide), F32), pltpu.VMEM((3, k, wide), F32),
            pltpu.VMEM((2, nf, 1, wide), F32), pltpu.VMEM((2, 1, wide), F32),
            pltpu.VMEM((2, nzx, k, wide), BF16), pltpu.VMEM((2, nzx, k, wide), BF16),
            pltpu.VMEM((2, k, wide), F32), pltpu.VMEM((2, k, wide), F32),
            pltpu.VMEM((2, ny, 1, rank), F32), pltpu.VMEM((2, ny, 1, rank), F32),
            pltpu.VMEM((2, nzx, 1, rank + wide), F32), pltpu.VMEM((2, 1, rank + wide), F32),
            pltpu.VMEM((2, ny, 1, rank + wide), F32), pltpu.VMEM((2, 1, rank + wide), F32),
            pltpu.VMEM((nzx, 1, wide), F32), pltpu.VMEM((1, wide), F32),
            pltpu.VMEM((1, wide), F32), pltpu.VMEM((1, wide), F32),
            dma((2,)), dma((22,)), dma((22,)),
        ],
        compiler_params=pltpu.CompilerParams(collective_id=0, has_side_effects=True),
    )(design_matrix, labels.reshape(1, -1), weights, lambdas.reshape(1, -1), sketch, sketch_values.reshape(1, -1))
    return weights + lax.dynamic_slice_in_dim(update, lax.axis_index("samp_2") * half, half, axis=1)


def solution(mesh):
    sizes = (8, 4, 2, 4, 2)
    finer = Mesh(mesh.devices.reshape(sizes), SAMP + FEAT)
    placed = (P(SAMP, FEAT), P(SAMP), P(None, FEAT_SAMP), P(), P(FEAT_SAMP, None), P())
    return jax.shard_map(
        functools.partial(shards, sizes), mesh=finer, in_specs=placed, out_specs=P(None, FEAT_SAMP), check_vma=False
    )
```

```python
import functools

import jax
import jax.numpy as jnp
from jax import lax
from jax.experimental import pallas as pl
from jax.experimental.pallas import tpu as pltpu
from jax.sharding import Mesh
from jax.sharding import PartitionSpec as P

SAMP = ("samp_0", "samp_1", "samp_2")
FEAT = ("feat_0", "feat_1")
FEAT_SAMP = FEAT + SAMP
F32, BF16 = jnp.float32, jnp.bfloat16
BY_LANES = (((1,), (1,)), ((), ()))
BY_ROWS = (((1,), (0,)), ((), ()))


def far_first(n):
    return sorted(range(n), key=lambda d: -min(d, n - d))


def split3(value):
    high = value.astype(BF16)
    rest = value - high.astype(F32)
    mid = rest.astype(BF16)
    low = (rest - mid.astype(F32)).astype(BF16)
    return jnp.concatenate([high, mid, low], axis=0)


def kernel(sizes, x_hbm, labels_hbm, w_hbm, lam_hbm, s_hbm, sv_hbm, out_ref,
           xv, labels_ref, w_ref, lam_ref, sv_ref, sp, wb, ag, ags, ft, fts, fs, fss, rs0, rss0, rs1, rss1, yh, yhs,
           pr, prs, pz, pzs, pa, pas, kz, kzs, local_sem, send_sem, recv_sem, gather_sem):
    nz, nx, nh, nl, nc = sizes
    nzx, nf, ny = nz * nx, nl * nc, nh * nl * nc
    k, half = w_ref.shape
    wide = 2 * half
    rank = s_hbm.shape[1]
    z, x, h, l, c = (lax.axis_index(name) for name in SAMP + FEAT)
    zx, f, y = z * nx + x, l * nc + c, (h * nl + l) * nc + c

    zx_peers = []
    for dz in far_first(nz):
        for dx in far_first(nx):
            if dz or dx:
                zz, xx = lax.rem(z + dz, nz), lax.rem(x + dx, nx)
                zx_peers.append((zz * nx + xx, {"samp_0": zz, "samp_1": xx}))
    y_peers, f_peers = [], []
    for dl in far_first(nl):
        for dh in reversed(range(nh)):
            for dc in reversed(range(nc)):
                if dh or dl or dc:
                    hh, ll, cc = lax.rem(h + dh, nh), lax.rem(l + dl, nl), lax.rem(c + dc, nc)
                    y_peers.append(((hh * nl + ll) * nc + cc, {"samp_2": hh, "feat_0": ll, "feat_1": cc}))
                    if not dh:
                        f_peers.append((ll * nc + cc, {"feat_0": ll, "feat_1": cc}))
    partner = {"samp_2": 1 - h}

    barrier = pltpu.get_barrier_semaphore()
    for _, peer in zx_peers + y_peers:
        pl.semaphore_signal(barrier, inc=1, device_id=peer, device_id_type=pl.DeviceIdType.MESH)

    loads = [pltpu.make_async_copy(src, dst, local_sem.at[j]) for j, (src, dst) in enumerate(
        [(w_hbm, w_ref), (lam_hbm, lam_ref), (sv_hbm, sv_ref), (labels_hbm, labels_ref), (s_hbm, sp.at[h]), (x_hbm, xv)])]
    for load in loads:
        load.start()

    def copy(phase, src, dst, peer):
        return pltpu.make_async_remote_copy(
            src_ref=src, dst_ref=dst, send_sem=send_sem.at[phase], recv_sem=recv_sem.at[phase],
            device_id=peer, device_id_type=pl.DeviceIdType.MESH)

    sent = []

    def whole(phase, buffer, peer):
        arrived = copy(phase, buffer, buffer, peer)
        arrived.wait_recv()
        sent.append(arrived)

    lane = lax.broadcasted_iota(jnp.int32, (k, wide), 1)
    row = lax.broadcasted_iota(jnp.int32, (k, wide), 0)

    def pack(*columns):
        total = 0.0
        for place, column in enumerate(columns):
            total = total + jnp.where(lane == row + place * k, column, 0.0)
        return jnp.sum(total, axis=0, keepdims=True)

    def unpack(packed, place):
        return jnp.sum(jnp.where(lane == row + place * k, packed, 0.0), axis=1, keepdims=True)

    def lanes(value):
        return jnp.sum(value, axis=1, keepdims=True)

    def gather_start(i, value):
        ags[i] = value.astype(BF16)
        ag[i, zx] = value.astype(BF16)
        for dz in far_first(nz):
            for dx in far_first(nx):
                if dz or dx:
                    zz, xx = lax.rem(z + dz, nz), lax.rem(x + dx, nx)
                    pltpu.make_async_remote_copy(
                        src_ref=ags.at[i], dst_ref=ag.at[i, zx], send_sem=send_sem.at[2 + i], recv_sem=gather_sem.at[i, dz],
                        device_id={"samp_0": zz, "samp_1": xx}, device_id_type=pl.DeviceIdType.MESH).start()

    def gather_rows(i):
        total = jnp.zeros((k, xv.shape[0]), F32)
        for dz in reversed(far_first(nz)):
            group = ag.at[i, pl.ds(0, nx if dz else nx - 1)]
            pltpu.make_async_remote_copy(
                src_ref=group, dst_ref=group, send_sem=send_sem.at[2 + i], recv_sem=gather_sem.at[i, dz],
                device_id=zx_peers[0][1], device_id_type=pl.DeviceIdType.MESH).wait_recv()
            zz = lax.rem(z + (nz - dz), nz)
            field = jnp.concatenate([ag[i, zz * nx + q] for q in range(nx)], axis=1)
            start = pl.multiple_of(zz * (nx * wide), nx * wide)
            total = total + lax.dot_general(field, xv[:, pl.ds(start, nx * wide)], BY_LANES, preferred_element_type=F32)
        sent.append(copy(2 + i, ag.at[i, pl.ds(0, nzx - 1)], ag.at[i, pl.ds(0, nzx - 1)], zx_peers[0][1]))
        return total

    def feat_sum(i, value):
        fts[i] = value
        ft[i, f] = value
        for _, peer in f_peers:
            copy(5 + i, fts.at[i], ft.at[i, f], peer).start()
        whole(5 + i, ft.at[i, pl.ds(0, nf - 1)], f_peers[0][1])
        return jnp.sum(ft[i], axis=0)

    def feat_scalars_start(i, value):
        fss[i] = value
        fs[i, f] = value
        for _, peer in f_peers:
            copy(8 + i, fss.at[i], fs.at[i, f], peer).start()

    def feat_scalars(i):
        whole(8 + i, fs.at[i, pl.ds(0, nf - 1)], f_peers[0][1])
        return jnp.sum(fs[i], axis=0)

    def column_sum(i, values):
        rs, rss = ((rs0, rss0), (rs1, rss1))[i]
        for dz in far_first(nz):
            zz = lax.rem(z + dz, nz)
            start = pl.multiple_of(zz * (nx * wide), nx * wide)
            part = lax.dot_general(values, xv[:, pl.ds(start, nx * wide)], BY_ROWS, preferred_element_type=F32)
            for xx in range(nx):
                rss[zz * nx + xx] = part[:, xx * wide:(xx + 1) * wide].astype(rss.dtype)
            for dx in far_first(nx):
                if dz or dx:
                    xx = lax.rem(x + dx, nx)
                    copy(10 + i, rss.at[zz * nx + xx], rs.at[zx], {"samp_0": zz, "samp_1": xx}).start()
        rs[zx] = rss[zx]
        whole(10 + i, rs.at[pl.ds(0, nzx - 1)], zx_peers[0][1])
        return jnp.sum(rs[...].astype(F32), axis=0)

    def pair_start(i, value):
        yhs[i] = value
        copy(12 + i, yhs.at[i], yh.at[i], partner).start()

    def pair_sum(i, value):
        whole(12 + i, yh.at[i], partner)
        return value + yh[i]

    def project(i, value, scalars):
        parts = lax.dot_general(split3(value), sketch, BY_ROWS, preferred_element_type=F32)
        part = parts[:k] + parts[k:2 * k] + parts[2 * k:]
        for q in range(k):
            prs[i, q] = part[q:q + 1, :]
        for j, peer in y_peers:
            copy(14 + i, prs.at[i, j], pr.at[i, y], peer).start()
        pr[i, y] = prs[i, y]
        whole(14 + i, pr.at[i, pl.ds(0, ny - 1)], y_peers[0][1])
        mine = jnp.concatenate([jnp.sum(pr[i], axis=0), scalars], axis=1)
        pzs[i] = mine
        pz[i, zx] = mine
        for _, peer in zx_peers:
            copy(16 + i, pzs.at[i], pz.at[i, zx], peer).start()
        whole(16 + i, pz.at[i, pl.ds(0, nzx - 1)], zx_peers[0][1])
        mine = jnp.sum(pz[i], axis=0)
        pas[i] = mine
        pa[i, y] = mine
        for _, peer in y_peers:
            copy(18 + i, pas.at[i], pa.at[i, y], peer).start()
        whole(18 + i, pa.at[i, pl.ds(0, ny - 1)], y_peers[0][1])
        full = jnp.concatenate([pa[i, q] for q in range(k)], axis=0)
        return full[:, :rank], jnp.sum(full[:, rank:], axis=0, keepdims=True) * (1.0 / nf)

    def spread(projected):
        parts = lax.dot_general(split3(ratios * projected), sketch, BY_LANES, preferred_element_type=F32)
        return parts[:k] + parts[k:2 * k] + parts[2 * k:]

    for load in loads[:4]:
        load.wait()
    lam = jnp.sum(jnp.where(lax.broadcasted_iota(jnp.int32, (k, k), 0) == lax.broadcasted_iota(jnp.int32, (k, k), 1),
                            lam_ref[...], 0.0), axis=1, keepdims=True)
    values = sv_ref[...].reshape(1, rank)
    ratios = (jnp.min(values, axis=1, keepdims=True) + lam) / (values + lam) - 1.0
    wb[0, :, :half] = w_ref[...]
    wb[0, :, half:] = w_ref[...]
    pl.semaphore_wait(barrier, len(zx_peers) + len(y_peers))
    copy(0, wb.at[0], wb.at[1], partner).start()
    whole(0, wb.at[1], partner)
    own = (lane // half) == h
    weights = jnp.where(own, wb[0], wb[1])
    gather_start(0, weights)
    loads[4].wait()
    copy(1, sp.at[h], sp.at[h], partner).start()
    loads[5].wait()

    logits = feat_sum(0, gather_rows(0))
    probability = jax.nn.sigmoid(logits)
    diag = probability * (1.0 - probability)
    miss = (probability - labels_ref[...].astype(F32)).astype(BF16)
    part = -(column_sum(0, miss) + (0.5 * lam) * weights)
    pair_start(0, part)
    whole(1, sp.at[1 - h], partner)
    sketch = sp[...].reshape(2 * half, rank)
    projected, _ = project(0, part, jnp.zeros((1, wide), F32))
    residual = pair_sum(0, part)
    direction = residual + spread(projected)

    gather_start(1, direction)
    feat_scalars_start(0, pack(0.5 * lanes(residual * direction), 0.5 * lam * lanes(direction * direction)))
    image = feat_sum(1, gather_rows(1))
    scalars = feat_scalars(0) + pack(jnp.zeros((k, 1), F32), lanes(diag * image * image))
    part = column_sum(1, (diag * image).astype(BF16)) + (0.5 * lam) * direction
    pair_start(1, part)
    projected, scalars = project(1, part, scalars)
    hess_dir = pair_sum(1, part)
    hess_pre = hess_dir + spread(projected)
    res_dot, curvature = unpack(scalars, 0), unpack(scalars, 1)
    step = res_dot / curvature
    residual = residual - step * hess_dir
    precond = direction - step * hess_pre

    gather_start(2, precond)
    feat_scalars_start(1, pack(0.5 * lanes(residual * precond), 0.5 * lam * lanes(precond * precond),
                               0.5 * lam * lanes(precond * direction)))
    image_pre = feat_sum(2, gather_rows(2))
    mine = feat_scalars(1) + pack(jnp.zeros((k, 1), F32), lanes(diag * image_pre * image_pre),
                                  lanes(diag * image_pre * image))
    kzs[...] = mine
    kz[zx * nh + h] = mine
    for dh in reversed(range(nh)):
        for dz in far_first(nz):
            for dx in far_first(nx):
                if dh or dz or dx:
                    peer = {"samp_0": lax.rem(z + dz, nz), "samp_1": lax.rem(x + dx, nx), "samp_2": lax.rem(h + dh, nh)}
                    copy(20, kzs, kz.at[zx * nh + h], peer).start()
    whole(20, kz.at[pl.ds(0, nzx * nh - 1)], partner)
    scalars = jnp.sum(kz[...], axis=0)
    new_dot, pre_pre, pre_dir = (unpack(scalars, place) for place in range(3))
    beta = new_dot / res_dot
    last = new_dot / (pre_pre + 2.0 * beta * pre_dir + beta * beta * curvature)
    out_ref[...] = step * direction + last * (precond + beta * direction)
    for arrived in sent:
        arrived.wait_send()


def shards(sizes, design_matrix, labels, weights, lambdas, sketch, sketch_values):
    nz, nx, nh, nl, nc = sizes
    nzx, nf, ny = nz * nx, nl * nc, nh * nl * nc
    k, half = weights.shape
    wide = 2 * half
    rank = sketch.shape[1]
    vmem = pl.BlockSpec(memory_space=pltpu.VMEM)
    anywhere = pl.BlockSpec(memory_space=pl.ANY)
    dma = pltpu.SemaphoreType.DMA
    update = pl.pallas_call(
        functools.partial(kernel, sizes),
        name="step",
        out_shape=jax.ShapeDtypeStruct((k, wide), F32),
        in_specs=[anywhere] * 6,
        out_specs=vmem,
        scratch_shapes=[
            pltpu.VMEM(design_matrix.shape, BF16),
            pltpu.VMEM((1, design_matrix.shape[0]), jnp.int32), pltpu.VMEM((k, half), F32), pltpu.VMEM((1, k), F32),
            pltpu.VMEM((rank,), F32),
            pltpu.VMEM((2, half, rank), BF16),
            pltpu.VMEM((2, k, wide), F32),
            pltpu.VMEM((3, nzx, k, wide), BF16), pltpu.VMEM((3, k, wide), BF16),
            pltpu.VMEM((3, nf, k, wide), F32), pltpu.VMEM((3, k, wide), F32),
            pltpu.VMEM((2, nf, 1, wide), F32), pltpu.VMEM((2, 1, wide), F32),
            pltpu.VMEM((nzx, k, wide), F32), pltpu.VMEM((nzx, k, wide), F32),
            pltpu.VMEM((nzx, k, wide), BF16), pltpu.VMEM((nzx, k, wide), BF16),
            pltpu.VMEM((2, k, wide), F32), pltpu.VMEM((2, k, wide), F32),
            pltpu.VMEM((2, ny, 1, rank), F32), pltpu.VMEM((2, ny, 1, rank), F32),
            pltpu.VMEM((2, nzx, 1, rank + wide), F32), pltpu.VMEM((2, 1, rank + wide), F32),
            pltpu.VMEM((2, ny, 1, rank + wide), F32), pltpu.VMEM((2, 1, rank + wide), F32),
            pltpu.VMEM((nzx * nh, 1, wide), F32), pltpu.VMEM((1, wide), F32),
            dma((6,)), dma((21,)), dma((21,)), dma((3, nz)),
        ],
        compiler_params=pltpu.CompilerParams(collective_id=0, has_side_effects=True),
    )(design_matrix, labels.reshape(1, -1), weights, lambdas.reshape(1, -1), sketch, sketch_values)
    return weights + lax.dynamic_slice_in_dim(update, lax.axis_index("samp_2") * half, half, axis=1)


def solution(mesh):
    sizes = (8, 4, 2, 4, 2)
    finer = Mesh(mesh.devices.reshape(sizes), SAMP + FEAT)
    placed = (P(SAMP, FEAT), P(SAMP), P(None, FEAT_SAMP), P(), P(FEAT_SAMP, None), P())
    return jax.shard_map(
        functools.partial(shards, sizes), mesh=finer, in_specs=placed, out_specs=P(None, FEAT_SAMP), check_vma=False
    )
```

```python
import functools

import jax
import jax.numpy as jnp
from jax import lax
from jax.experimental import pallas as pl
from jax.experimental.pallas import tpu as pltpu
from jax.sharding import Mesh
from jax.sharding import PartitionSpec as P

SAMP = ("samp_0", "samp_1", "samp_2")
FEAT = ("feat_0", "feat_1")
FEAT_SAMP = FEAT + SAMP
F32, BF16 = jnp.float32, jnp.bfloat16
BY_LANES = (((1,), (1,)), ((), ()))
BY_ROWS = (((1,), (0,)), ((), ()))


def far_first(n):
    return sorted(range(n), key=lambda d: -min(d, n - d))


def split3(value):
    high = value.astype(BF16)
    rest = value - high.astype(F32)
    mid = rest.astype(BF16)
    low = (rest - mid.astype(F32)).astype(BF16)
    return jnp.concatenate([high, mid, low], axis=0)


def kernel(sizes, x_hbm, labels_hbm, w_hbm, lam_hbm, s_hbm, sv_hbm, out_ref,
           xv, labels_ref, w_ref, lam_ref, sv_ref, sp, wb, ag, ags, ft, fts, fs, fss, rs0, rss0, rs1, rss1, xr, xs, yh, yhs,
           pr, prs, pz, pzs, pa, pas, cz, czs, cf, kz, kzs, local_sem, send_sem, recv_sem, gather_sem):
    nz, nx, nh, nl, nc = sizes
    nzx, nf, ny = nz * nx, nl * nc, nh * nl * nc
    k, half = w_ref.shape
    wide = 2 * half
    rank = s_hbm.shape[1]
    z, x, h, l, c = (lax.axis_index(name) for name in SAMP + FEAT)
    zx, f, y = z * nx + x, l * nc + c, (h * nl + l) * nc + c

    zx_peers = []
    for dz in far_first(nz):
        for dx in far_first(nx):
            if dz or dx:
                zz, xx = lax.rem(z + dz, nz), lax.rem(x + dx, nx)
                zx_peers.append((zz * nx + xx, {"samp_0": zz, "samp_1": xx}))
    y_peers, f_peers = [], []
    for dl in far_first(nl):
        for dh in reversed(range(nh)):
            for dc in reversed(range(nc)):
                if dh or dl or dc:
                    hh, ll, cc = lax.rem(h + dh, nh), lax.rem(l + dl, nl), lax.rem(c + dc, nc)
                    y_peers.append(((hh * nl + ll) * nc + cc, {"samp_2": hh, "feat_0": ll, "feat_1": cc}))
                    if not dh:
                        f_peers.append((ll * nc + cc, {"feat_0": ll, "feat_1": cc}))
    partner = {"samp_2": 1 - h}

    barrier = pltpu.get_barrier_semaphore()
    for _, peer in zx_peers + y_peers:
        pl.semaphore_signal(barrier, inc=1, device_id=peer, device_id_type=pl.DeviceIdType.MESH)

    loads = [pltpu.make_async_copy(src, dst, local_sem.at[j]) for j, (src, dst) in enumerate(
        [(w_hbm, w_ref), (lam_hbm, lam_ref), (sv_hbm, sv_ref), (labels_hbm, labels_ref), (s_hbm, sp.at[x * nh + h]), (x_hbm, xv)])]
    for load in loads:
        load.start()

    def copy(phase, src, dst, peer):
        return pltpu.make_async_remote_copy(
            src_ref=src, dst_ref=dst, send_sem=send_sem.at[phase], recv_sem=recv_sem.at[phase],
            device_id=peer, device_id_type=pl.DeviceIdType.MESH)

    sent = []

    def whole(phase, buffer, peer):
        arrived = copy(phase, buffer, buffer, peer)
        arrived.wait_recv()
        sent.append(arrived)

    lane = lax.broadcasted_iota(jnp.int32, (k, wide), 1)
    row = lax.broadcasted_iota(jnp.int32, (k, wide), 0)

    def pack(*columns):
        total = 0.0
        for place, column in enumerate(columns):
            total = total + jnp.where(lane == row + place * k, column, 0.0)
        return jnp.sum(total, axis=0, keepdims=True)

    def unpack(packed, place):
        return jnp.sum(jnp.where(lane == row + place * k, packed, 0.0), axis=1, keepdims=True)

    def lanes(value):
        return jnp.sum(value, axis=1, keepdims=True)

    def gather_start(i, value):
        ags[i] = value.astype(BF16)
        ag[i, zx] = value.astype(BF16)
        for dz in far_first(nz):
            for dx in far_first(nx):
                if dz or dx:
                    zz, xx = lax.rem(z + dz, nz), lax.rem(x + dx, nx)
                    pltpu.make_async_remote_copy(
                        src_ref=ags.at[i], dst_ref=ag.at[i, zx], send_sem=send_sem.at[2 + i], recv_sem=gather_sem.at[i, dz],
                        device_id={"samp_0": zz, "samp_1": xx}, device_id_type=pl.DeviceIdType.MESH).start()

    def spread_start(i, value):
        czs[i] = value.astype(BF16)
        for dz in far_first(nz):
            zz = lax.rem(z + dz, nz)
            if dz:
                pltpu.make_async_remote_copy(
                    src_ref=czs.at[i], dst_ref=cz.at[i, z], send_sem=send_sem.at[23 + i], recv_sem=gather_sem.at[3 + i, dz],
                    device_id={"samp_0": zz}, device_id_type=pl.DeviceIdType.MESH).start()

    def arrived_group(phase, place, dz, group):
        pltpu.make_async_remote_copy(
            src_ref=group, dst_ref=group, send_sem=send_sem.at[phase], recv_sem=gather_sem.at[place, dz],
            device_id=zx_peers[0][1], device_id_type=pl.DeviceIdType.MESH).wait_recv()

    def rows_of(field, zz):
        start = pl.multiple_of(zz * (nx * wide), nx * wide)
        return lax.dot_general(field, xv[:, pl.ds(start, nx * wide)], BY_LANES, preferred_element_type=F32)

    def gather_rows(i):
        total = jnp.zeros((k, xv.shape[0]), F32)
        for dz in reversed(far_first(nz)):
            arrived_group(2 + i, i, dz, ag.at[i, pl.ds(0, nx if dz else nx - 1)])
            zz = lax.rem(z + (nz - dz), nz)
            total = total + rows_of(jnp.concatenate([ag[i, zz * nx + q] for q in range(nx)], axis=1), zz)
        sent.append(copy(2 + i, ag.at[i, pl.ds(0, nzx - 1)], ag.at[i, pl.ds(0, nzx - 1)], zx_peers[0][1]))
        return total

    def spread_rows(i, total):
        for dz in reversed(far_first(nz)):
            zz = lax.rem(z + (nz - dz), nz)
            if dz:
                arrived_group(23 + i, 3 + i, dz, cz.at[i, 0])
                total = total + rows_of(cz[i, zz], zz)
            else:
                total = total + rows_of(czs[i], zz)
        sent.append(copy(23 + i, cz.at[i, pl.ds(0, nz - 1)], cz.at[i, pl.ds(0, nz - 1)], zx_peers[0][1]))
        return total

    def feat_sum(i, value):
        fts[i] = value
        ft[i, f] = value
        for _, peer in f_peers:
            copy(5 + i, fts.at[i], ft.at[i, f], peer).start()
        whole(5 + i, ft.at[i, pl.ds(0, nf - 1)], f_peers[0][1])
        return jnp.sum(ft[i], axis=0)

    def feat_scalars_start(i, value):
        fss[i] = value
        fs[i, f] = value
        for _, peer in f_peers:
            copy(8 + i, fss.at[i], fs.at[i, f], peer).start()

    def feat_scalars(i):
        whole(8 + i, fs.at[i, pl.ds(0, nf - 1)], f_peers[0][1])
        return jnp.sum(fs[i], axis=0)

    def reduce_columns(i, values, state, scalars):
        rs, rss = ((rs0, rss0), (rs1, rss1))[i]
        for dz in far_first(nz):
            zz = lax.rem(z + dz, nz)
            start = pl.multiple_of(zz * (nx * wide), nx * wide)
            part = lax.dot_general(values, xv[:, pl.ds(start, nx * wide)], BY_ROWS, preferred_element_type=F32)
            rss[zz] = part.astype(rss.dtype)
            if dz:
                copy(10 + i, rss.at[zz], rs.at[z], {"samp_0": zz}).start()
        rs[z] = rss[z]
        whole(10 + i, rs.at[pl.ds(0, nz - 1)], zx_peers[0][1])
        along_z = jnp.sum(rs[...].astype(F32), axis=0)
        ridge = (0.5 * lam) * state
        chunks = [along_z[:, q * wide:(q + 1) * wide] + ridge * jnp.where(x == q, 1.0, 0.0) for q in range(nx)]

        parts = lax.dot_general(split3(jnp.concatenate(chunks, axis=1)), sketch, BY_ROWS, preferred_element_type=F32)
        projected = parts[:k] + parts[k:2 * k] + parts[2 * k:]
        for q in range(k):
            prs[i, q] = projected[q:q + 1, :]
        for j, peer in y_peers:
            copy(14 + i, prs.at[i, j], pr.at[i, y], peer).start()
        pr[i, y] = prs[i, y]

        for q in range(nx):
            xs[i, q] = chunks[q]
        for dx in far_first(nx):
            xx = lax.rem(x + dx, nx)
            if dx:
                copy(21 + i, xs.at[i, xx], xr.at[i, x], {"samp_1": xx}).start()
        xr[i, x] = xs[i, x]
        whole(21 + i, xr.at[i, pl.ds(0, nx - 1)], {"samp_1": lax.rem(x + 1, nx)})
        part = jnp.sum(xr[i], axis=0)
        yhs[i] = part
        copy(12 + i, yhs.at[i], yh.at[i], partner).start()

        whole(14 + i, pr.at[i, pl.ds(0, ny - 1)], y_peers[0][1])
        mine = jnp.sum(pr[i], axis=0)
        if scalars is not None:
            mine = jnp.concatenate([mine, scalars], axis=1)
        across = slice(0, mine.shape[1])
        pzs[i, :, across] = mine
        pz[i, zx, :, across] = mine
        for _, peer in zx_peers:
            copy(16 + i, pzs.at[i, :, across], pz.at[i, zx, :, across], peer).start()

        whole(12 + i, yh.at[i], partner)
        vector = part + yh[i]
        gather_start(1 + i, vector)

        whole(16 + i, pz.at[i, pl.ds(0, nzx - 1), :, across], zx_peers[0][1])
        mine = jnp.sum(pz[i, :, :, across], axis=0)
        pas[i, :, across] = mine
        pa[i, y, :, across] = mine
        for _, peer in y_peers:
            copy(18 + i, pas.at[i, :, across], pa.at[i, y, :, across], peer).start()
        image = gather_rows(1 + i)
        whole(18 + i, pa.at[i, pl.ds(0, ny - 1), :, across], y_peers[0][1])
        full = jnp.concatenate([pa[i, q, :, across] for q in range(k)], axis=0)
        if scalars is not None:
            scalars = jnp.sum(full[:, rank:], axis=0, keepdims=True) * (1.0 / nf)

        parts = lax.dot_general(split3(ratios * full[:, :rank]), sketch, BY_LANES, preferred_element_type=F32)
        correction = parts[:k] + parts[k:2 * k] + parts[2 * k:]
        spread_start(i, correction)
        for q in range(nx):
            cf[i, q] = correction[:, q * wide:(q + 1) * wide]
        return vector, vector + cf[i, x], image, scalars

    for load in loads[:4]:
        load.wait()
    lam = jnp.sum(jnp.where(lax.broadcasted_iota(jnp.int32, (k, k), 0) == lax.broadcasted_iota(jnp.int32, (k, k), 1),
                            lam_ref[...], 0.0), axis=1, keepdims=True)
    values = sv_ref[...].reshape(1, rank)
    ratios = (jnp.min(values, axis=1, keepdims=True) + lam) / (values + lam) - 1.0
    wb[0, :, :half] = w_ref[...]
    wb[0, :, half:] = w_ref[...]
    pl.semaphore_wait(barrier, len(zx_peers) + len(y_peers))
    copy(0, wb.at[0], wb.at[1], partner).start()
    whole(0, wb.at[1], partner)
    own = (lane // half) == h
    weights = jnp.where(own, wb[0], wb[1])
    gather_start(0, weights)
    loads[4].wait()
    for dh in reversed(range(nh)):
        for dx in far_first(nx):
            if dh or dx:
                peer = {"samp_1": lax.rem(x + dx, nx), "samp_2": lax.rem(h + dh, nh)}
                copy(1, sp.at[x * nh + h], sp.at[x * nh + h], peer).start()
    loads[5].wait()

    logits = feat_sum(0, gather_rows(0))
    probability = jax.nn.sigmoid(logits)
    diag = probability * (1.0 - probability)
    miss = (probability - labels_ref[...].astype(F32)).astype(BF16)
    whole(1, sp.at[pl.ds(0, nx * nh - 1)], partner)
    sketch = sp[...].reshape(nx * nh * half, rank)
    gradient, gradient_pre, image, _ = reduce_columns(0, miss, weights, None)
    residual, direction = -gradient, -gradient_pre
    feat_scalars_start(0, pack(0.5 * lanes(residual * direction), 0.5 * lam * lanes(direction * direction)))
    image = -feat_sum(1, spread_rows(0, image))
    scalars = feat_scalars(0) + pack(jnp.zeros((k, 1), F32), lanes(diag * image * image))
    hess_dir, hess_pre, image_pre, scalars = reduce_columns(1, (diag * image).astype(BF16), direction, scalars)
    res_dot, curvature = unpack(scalars, 0), unpack(scalars, 1)
    step = res_dot / curvature
    residual = residual - step * hess_dir
    precond = direction - step * hess_pre
    feat_scalars_start(1, pack(0.5 * lanes(residual * precond), 0.5 * lam * lanes(precond * precond),
                               0.5 * lam * lanes(precond * direction)))
    image_pre = image - step * feat_sum(2, spread_rows(1, image_pre))
    mine = feat_scalars(1) + pack(jnp.zeros((k, 1), F32), lanes(diag * image_pre * image_pre),
                                  lanes(diag * image_pre * image))
    kzs[...] = mine
    kz[zx * nh + h] = mine
    for dh in reversed(range(nh)):
        for dz in far_first(nz):
            for dx in far_first(nx):
                if dh or dz or dx:
                    peer = {"samp_0": lax.rem(z + dz, nz), "samp_1": lax.rem(x + dx, nx), "samp_2": lax.rem(h + dh, nh)}
                    copy(20, kzs, kz.at[zx * nh + h], peer).start()
    whole(20, kz.at[pl.ds(0, nzx * nh - 1)], partner)
    scalars = jnp.sum(kz[...], axis=0)
    new_dot, pre_pre, pre_dir = (unpack(scalars, place) for place in range(3))
    beta = new_dot / res_dot
    last = new_dot / (pre_pre + 2.0 * beta * pre_dir + beta * beta * curvature)
    out_ref[...] = step * direction + last * (precond + beta * direction)
    for arrived in sent:
        arrived.wait_send()


def shards(sizes, design_matrix, labels, weights, lambdas, sketch, sketch_values):
    nz, nx, nh, nl, nc = sizes
    nzx, nf, ny = nz * nx, nl * nc, nh * nl * nc
    k, half = weights.shape
    wide = 2 * half
    rank = sketch.shape[1]
    vmem = pl.BlockSpec(memory_space=pltpu.VMEM)
    anywhere = pl.BlockSpec(memory_space=pl.ANY)
    dma = pltpu.SemaphoreType.DMA
    update = pl.pallas_call(
        functools.partial(kernel, sizes),
        name="step",
        out_shape=jax.ShapeDtypeStruct((k, wide), F32),
        in_specs=[anywhere] * 6,
        out_specs=vmem,
        scratch_shapes=[
            pltpu.VMEM(design_matrix.shape, BF16),
            pltpu.VMEM((1, design_matrix.shape[0]), jnp.int32), pltpu.VMEM((k, half), F32), pltpu.VMEM((1, k), F32),
            pltpu.VMEM((rank,), F32),
            pltpu.VMEM((nx * nh, half, rank), BF16),
            pltpu.VMEM((2, k, wide), F32),
            pltpu.VMEM((3, nzx, k, wide), BF16), pltpu.VMEM((3, k, wide), BF16),
            pltpu.VMEM((3, nf, k, wide), F32), pltpu.VMEM((3, k, wide), F32),
            pltpu.VMEM((2, nf, 1, wide), F32), pltpu.VMEM((2, 1, wide), F32),
            pltpu.VMEM((nz, k, nx * wide), F32), pltpu.VMEM((nz, k, nx * wide), F32),
            pltpu.VMEM((nz, k, nx * wide), BF16), pltpu.VMEM((nz, k, nx * wide), BF16),
            pltpu.VMEM((2, nx, k, wide), F32), pltpu.VMEM((2, nx, k, wide), F32),
            pltpu.VMEM((2, k, wide), F32), pltpu.VMEM((2, k, wide), F32),
            pltpu.VMEM((2, ny, 1, rank), F32), pltpu.VMEM((2, ny, 1, rank), F32),
            pltpu.VMEM((2, nzx, 1, rank + wide), F32), pltpu.VMEM((2, 1, rank + wide), F32),
            pltpu.VMEM((2, ny, 1, rank + wide), F32), pltpu.VMEM((2, 1, rank + wide), F32),
            pltpu.VMEM((2, nz, k, nx * wide), BF16), pltpu.VMEM((2, k, nx * wide), BF16),
            pltpu.VMEM((2, nx, k, wide), F32),
            pltpu.VMEM((nzx * nh, 1, wide), F32), pltpu.VMEM((1, wide), F32),
            dma((6,)), dma((25,)), dma((25,)), dma((5, nz)),
        ],
        compiler_params=pltpu.CompilerParams(collective_id=0, has_side_effects=True),
    )(design_matrix, labels.reshape(1, -1), weights, lambdas.reshape(1, -1), sketch, sketch_values)
    return weights + lax.dynamic_slice_in_dim(update, lax.axis_index("samp_2") * half, half, axis=1)


def solution(mesh):
    sizes = (8, 4, 2, 4, 2)
    finer = Mesh(mesh.devices.reshape(sizes), SAMP + FEAT)
    placed = (P(SAMP, FEAT), P(SAMP), P(None, FEAT_SAMP), P(), P(FEAT_SAMP, None), P())
    return jax.shard_map(
        functools.partial(shards, sizes), mesh=finer, in_specs=placed, out_specs=P(None, FEAT_SAMP), check_vma=False
    )
```

```python
import functools

import jax
import jax.numpy as jnp
from jax import lax
from jax.experimental import pallas as pl
from jax.experimental.pallas import tpu as pltpu
from jax.sharding import Mesh
from jax.sharding import PartitionSpec as P

SAMP = ("samp_0", "samp_1", "samp_2")
FEAT = ("feat_0", "feat_1")
FEAT_SAMP = FEAT + SAMP
F32, BF16 = jnp.float32, jnp.bfloat16
BY_LANES = (((1,), (1,)), ((), ()))
BY_ROWS = (((1,), (0,)), ((), ()))


def far_first(n):
    return sorted(range(n), key=lambda d: -min(d, n - d))


def split3(value):
    high = value.astype(BF16)
    rest = value - high.astype(F32)
    mid = rest.astype(BF16)
    low = (rest - mid.astype(F32)).astype(BF16)
    return jnp.concatenate([high, mid, low], axis=0)


def kernel(sizes, x_hbm, labels_hbm, w_hbm, lam_hbm, s_hbm, sv_hbm, out_ref,
           xv, labels_ref, w_ref, lam_ref, sv_ref, sp, wb, ag, ags, ft, fts, fs, fss, rs, rss, rl, rls, xr, xs, yh, yhs,
           pr, prs, pz, pzs, pa, pas, cz, czs, cf, kz, kzs, local_sem, send_sem, recv_sem, gather_sem):
    nz, nx, nh, nl, nc = sizes
    nzx, nf, ny = nz * nx, nl * nc, nh * nl * nc
    k, half = w_ref.shape
    wide = 2 * half
    rank = s_hbm.shape[1]
    z, x, h, l, c = (lax.axis_index(name) for name in SAMP + FEAT)
    zx, f, y = z * nx + x, l * nc + c, (h * nl + l) * nc + c

    zx_peers = []
    for dz in far_first(nz):
        for dx in far_first(nx):
            if dz or dx:
                zz, xx = lax.rem(z + dz, nz), lax.rem(x + dx, nx)
                zx_peers.append((zz * nx + xx, {"samp_0": zz, "samp_1": xx}))
    y_peers, f_peers = [], []
    for dl in far_first(nl):
        for dh in reversed(range(nh)):
            for dc in reversed(range(nc)):
                if dh or dl or dc:
                    hh, ll, cc = lax.rem(h + dh, nh), lax.rem(l + dl, nl), lax.rem(c + dc, nc)
                    y_peers.append(((hh * nl + ll) * nc + cc, {"samp_2": hh, "feat_0": ll, "feat_1": cc}))
                    if not dh:
                        f_peers.append((ll * nc + cc, {"feat_0": ll, "feat_1": cc}))
    partner = {"samp_2": 1 - h}

    barrier = pltpu.get_barrier_semaphore()
    for _, peer in zx_peers + y_peers:
        pl.semaphore_signal(barrier, inc=1, device_id=peer, device_id_type=pl.DeviceIdType.MESH)

    loads = [pltpu.make_async_copy(src, dst, local_sem.at[j]) for j, (src, dst) in enumerate(
        [(w_hbm, w_ref), (lam_hbm, lam_ref), (sv_hbm, sv_ref), (labels_hbm, labels_ref), (s_hbm, sp.at[x * nh + h]), (x_hbm, xv)])]
    for load in loads:
        load.start()

    def copy(phase, src, dst, peer):
        return pltpu.make_async_remote_copy(
            src_ref=src, dst_ref=dst, send_sem=send_sem.at[phase], recv_sem=recv_sem.at[phase],
            device_id=peer, device_id_type=pl.DeviceIdType.MESH)

    sent = []

    def whole(phase, buffer, peer):
        arrived = copy(phase, buffer, buffer, peer)
        arrived.wait_recv()
        sent.append(arrived)

    lane = lax.broadcasted_iota(jnp.int32, (k, wide), 1)
    row = lax.broadcasted_iota(jnp.int32, (k, wide), 0)

    def pack(*columns):
        total = 0.0
        for place, column in enumerate(columns):
            total = total + jnp.where(lane == row + place * k, column, 0.0)
        return jnp.sum(total, axis=0, keepdims=True)

    def unpack(packed, place):
        return jnp.sum(jnp.where(lane == row + place * k, packed, 0.0), axis=1, keepdims=True)

    def lanes(value):
        return jnp.sum(value, axis=1, keepdims=True)

    def gather_start(i, value):
        ags[i] = value.astype(BF16)
        ag[i, zx] = value.astype(BF16)
        for dz in far_first(nz):
            for dx in far_first(nx):
                if dz or dx:
                    zz, xx = lax.rem(z + dz, nz), lax.rem(x + dx, nx)
                    pltpu.make_async_remote_copy(
                        src_ref=ags.at[i], dst_ref=ag.at[i, zx], send_sem=send_sem.at[2 + i], recv_sem=gather_sem.at[i, dz],
                        device_id={"samp_0": zz, "samp_1": xx}, device_id_type=pl.DeviceIdType.MESH).start()

    def spread_start(i, value):
        czs[i] = value.astype(BF16)
        for dz in far_first(nz):
            zz = lax.rem(z + dz, nz)
            if dz:
                pltpu.make_async_remote_copy(
                    src_ref=czs.at[i], dst_ref=cz.at[i, z], send_sem=send_sem.at[23 + i], recv_sem=gather_sem.at[3 + i, dz],
                    device_id={"samp_0": zz}, device_id_type=pl.DeviceIdType.MESH).start()

    def arrived_group(phase, place, dz, group):
        pltpu.make_async_remote_copy(
            src_ref=group, dst_ref=group, send_sem=send_sem.at[phase], recv_sem=gather_sem.at[place, dz],
            device_id=zx_peers[0][1], device_id_type=pl.DeviceIdType.MESH).wait_recv()

    def rows_of(field, zz):
        start = pl.multiple_of(zz * (nx * wide), nx * wide)
        return lax.dot_general(field, xv[:, pl.ds(start, nx * wide)], BY_LANES, preferred_element_type=F32)

    def gather_rows(i, before_last=None):
        total = jnp.zeros((k, xv.shape[0]), F32)
        for dz in reversed(far_first(nz)):
            if before_last is not None and dz == nz // 2:
                before_last()
            arrived_group(2 + i, i, dz, ag.at[i, pl.ds(0, nx if dz else nx - 1)])
            zz = lax.rem(z + (nz - dz), nz)
            total = total + rows_of(jnp.concatenate([ag[i, zz * nx + q] for q in range(nx)], axis=1), zz)
        sent.append(copy(2 + i, ag.at[i, pl.ds(0, nzx - 1)], ag.at[i, pl.ds(0, nzx - 1)], zx_peers[0][1]))
        return total

    def spread_rows(i, total):
        for dz in reversed(far_first(nz)):
            zz = lax.rem(z + (nz - dz), nz)
            if dz:
                arrived_group(23 + i, 3 + i, dz, cz.at[i, 0])
                total = total + rows_of(cz[i, zz], zz)
            else:
                total = total + rows_of(czs[i], zz)
        sent.append(copy(23 + i, cz.at[i, pl.ds(0, nz - 1)], cz.at[i, pl.ds(0, nz - 1)], zx_peers[0][1]))
        return total

    def feat_sum(i, value):
        fts[i] = value
        ft[i, f] = value
        for _, peer in f_peers:
            copy(5 + i, fts.at[i], ft.at[i, f], peer).start()
        whole(5 + i, ft.at[i, pl.ds(0, nf - 1)], f_peers[0][1])
        return jnp.sum(ft[i], axis=0)

    def feat_scalars_start(i, value):
        fss[i] = value
        fs[i, f] = value
        for _, peer in f_peers:
            copy(8 + i, fss.at[i], fs.at[i, f], peer).start()

    def feat_scalars(i):
        whole(8 + i, fs.at[i, pl.ds(0, nf - 1)], f_peers[0][1])
        return jnp.sum(fs[i], axis=0)

    def reduce_columns(i, values, state, scalars, low_too):
        for dz in far_first(nz):
            zz = lax.rem(z + dz, nz)
            start = pl.multiple_of(zz * (nx * wide), nx * wide)
            part = lax.dot_general(values, xv[:, pl.ds(start, nx * wide)], BY_ROWS, preferred_element_type=F32)
            high = part.astype(BF16)
            rss[i, zz] = high
            if low_too:
                rls[zz] = (part - high.astype(F32)).astype(BF16)
            if dz:
                copy(10 + i, rss.at[i, zz], rs.at[i, z], {"samp_0": zz}).start()
        rs[i, z] = rss[i, z]
        if low_too:
            for dz in far_first(nz):
                zz = lax.rem(z + dz, nz)
                if dz:
                    copy(25, rls.at[zz], rl.at[z], {"samp_0": zz}).start()
            rl[z] = rls[z]
        whole(10 + i, rs.at[i, pl.ds(0, nz - 1)], zx_peers[0][1])
        along_z = jnp.sum(rs[i].astype(F32), axis=0)
        ridge = (0.5 * lam) * state
        chunks = [along_z[:, q * wide:(q + 1) * wide] + ridge * jnp.where(x == q, 1.0, 0.0) for q in range(nx)]

        parts = lax.dot_general(split3(jnp.concatenate(chunks, axis=1)), sketch, BY_ROWS, preferred_element_type=F32)
        projected = parts[:k] + parts[k:2 * k] + parts[2 * k:]
        for q in range(k):
            prs[i, q] = projected[q:q + 1, :]
        for j, peer in y_peers:
            copy(14 + i, prs.at[i, j], pr.at[i, y], peer).start()
        pr[i, y] = prs[i, y]

        if low_too:
            whole(25, rl.at[pl.ds(0, nz - 1)], zx_peers[0][1])
            low = jnp.sum(rl[...].astype(F32), axis=0)
            chunks = [chunks[q] + low[:, q * wide:(q + 1) * wide] for q in range(nx)]
        for q in range(nx):
            xs[i, q] = chunks[q]
        for dx in far_first(nx):
            xx = lax.rem(x + dx, nx)
            if dx:
                copy(21 + i, xs.at[i, xx], xr.at[i, x], {"samp_1": xx}).start()
        xr[i, x] = xs[i, x]
        whole(21 + i, xr.at[i, pl.ds(0, nx - 1)], {"samp_1": lax.rem(x + 1, nx)})
        part = jnp.sum(xr[i], axis=0)
        yhs[i] = part
        copy(12 + i, yhs.at[i], yh.at[i], partner).start()

        whole(14 + i, pr.at[i, pl.ds(0, ny - 1)], y_peers[0][1])
        mine = jnp.sum(pr[i], axis=0)
        if scalars is not None:
            mine = jnp.concatenate([mine, scalars], axis=1)
        across = slice(0, mine.shape[1])
        pzs[i, :, across] = mine
        pz[i, zx, :, across] = mine
        for _, peer in zx_peers:
            copy(16 + i, pzs.at[i, :, across], pz.at[i, zx, :, across], peer).start()

        whole(12 + i, yh.at[i], partner)
        vector = part + yh[i]
        gather_start(1 + i, vector)

        whole(16 + i, pz.at[i, pl.ds(0, nzx - 1), :, across], zx_peers[0][1])
        mine = jnp.sum(pz[i, :, :, across], axis=0)
        pas[i, :, across] = mine
        pa[i, y, :, across] = mine
        for _, peer in y_peers:
            copy(18 + i, pas.at[i, :, across], pa.at[i, y, :, across], peer).start()
        image = gather_rows(1 + i)
        whole(18 + i, pa.at[i, pl.ds(0, ny - 1), :, across], y_peers[0][1])
        full = jnp.concatenate([pa[i, q, :, across] for q in range(k)], axis=0)
        if scalars is not None:
            scalars = jnp.sum(full[:, rank:], axis=0, keepdims=True) * (1.0 / nf)

        parts = lax.dot_general(split3(ratios * full[:, :rank]), sketch, BY_LANES, preferred_element_type=F32)
        correction = parts[:k] + parts[k:2 * k] + parts[2 * k:]
        spread_start(i, correction)
        for q in range(nx):
            cf[i, q] = correction[:, q * wide:(q + 1) * wide]
        return vector, vector + cf[i, x], image, scalars

    for load in loads[:4]:
        load.wait()
    lam = jnp.sum(jnp.where(lax.broadcasted_iota(jnp.int32, (k, k), 0) == lax.broadcasted_iota(jnp.int32, (k, k), 1),
                            lam_ref[...], 0.0), axis=1, keepdims=True)
    values = sv_ref[...].reshape(1, rank)
    ratios = (jnp.min(values, axis=1, keepdims=True) + lam) / (values + lam) - 1.0
    wb[0, :, :half] = w_ref[...]
    wb[0, :, half:] = w_ref[...]
    pl.semaphore_wait(barrier, len(zx_peers) + len(y_peers))
    copy(0, wb.at[0], wb.at[1], partner).start()
    whole(0, wb.at[1], partner)
    own = (lane // half) == h
    weights = jnp.where(own, wb[0], wb[1])
    gather_start(0, weights)
    loads[4].wait()

    def sketch_start():
        for dh in reversed(range(nh)):
            for dx in far_first(nx):
                if dh or dx:
                    peer = {"samp_1": lax.rem(x + dx, nx), "samp_2": lax.rem(h + dh, nh)}
                    copy(1, sp.at[x * nh + h], sp.at[x * nh + h], peer).start()

    loads[5].wait()

    logits = feat_sum(0, gather_rows(0, sketch_start))
    probability = jax.nn.sigmoid(logits)
    diag = probability * (1.0 - probability)
    miss = (probability - labels_ref[...].astype(F32)).astype(BF16)
    whole(1, sp.at[pl.ds(0, nx * nh - 1)], partner)
    sketch = sp[...].reshape(nx * nh * half, rank)
    gradient, gradient_pre, image, _ = reduce_columns(0, miss, weights, None, True)
    residual, direction = -gradient, -gradient_pre
    feat_scalars_start(0, pack(0.5 * lanes(residual * direction), 0.5 * lam * lanes(direction * direction)))
    image = -feat_sum(1, spread_rows(0, image))
    scalars = feat_scalars(0) + pack(jnp.zeros((k, 1), F32), lanes(diag * image * image))
    hess_dir, hess_pre, image_pre, scalars = reduce_columns(1, (diag * image).astype(BF16), direction, scalars, False)
    res_dot, curvature = unpack(scalars, 0), unpack(scalars, 1)
    step = res_dot / curvature
    residual = residual - step * hess_dir
    precond = direction - step * hess_pre
    feat_scalars_start(1, pack(0.5 * lanes(residual * precond), 0.5 * lam * lanes(precond * precond),
                               0.5 * lam * lanes(precond * direction)))
    image_pre = image - step * feat_sum(2, spread_rows(1, image_pre))
    mine = feat_scalars(1) + pack(jnp.zeros((k, 1), F32), lanes(diag * image_pre * image_pre),
                                  lanes(diag * image_pre * image))
    kzs[...] = mine
    kz[zx * nh + h] = mine
    for dh in reversed(range(nh)):
        for dz in far_first(nz):
            for dx in far_first(nx):
                if dh or dz or dx:
                    peer = {"samp_0": lax.rem(z + dz, nz), "samp_1": lax.rem(x + dx, nx), "samp_2": lax.rem(h + dh, nh)}
                    copy(20, kzs, kz.at[zx * nh + h], peer).start()
    whole(20, kz.at[pl.ds(0, nzx * nh - 1)], partner)
    scalars = jnp.sum(kz[...], axis=0)
    new_dot, pre_pre, pre_dir = (unpack(scalars, place) for place in range(3))
    beta = new_dot / res_dot
    last = new_dot / (pre_pre + 2.0 * beta * pre_dir + beta * beta * curvature)
    update = step * direction + last * (precond + beta * direction)
    update = jnp.where(h == 0, update, pltpu.roll(update, half, 1))
    out_ref[...] = w_ref[...] + update[:, :half]
    for arrived in sent:
        arrived.wait_send()


def shards(sizes, design_matrix, labels, weights, lambdas, sketch, sketch_values):
    nz, nx, nh, nl, nc = sizes
    nzx, nf, ny = nz * nx, nl * nc, nh * nl * nc
    k, half = weights.shape
    wide = 2 * half
    rank = sketch.shape[1]
    vmem = pl.BlockSpec(memory_space=pltpu.VMEM)
    anywhere = pl.BlockSpec(memory_space=pl.ANY)
    dma = pltpu.SemaphoreType.DMA
    return pl.pallas_call(
        functools.partial(kernel, sizes),
        name="step",
        out_shape=jax.ShapeDtypeStruct((k, half), F32),
        in_specs=[anywhere] * 6,
        out_specs=vmem,
        scratch_shapes=[
            pltpu.VMEM(design_matrix.shape, BF16),
            pltpu.VMEM((1, design_matrix.shape[0]), jnp.int32), pltpu.VMEM((k, half), F32), pltpu.VMEM((1, k), F32),
            pltpu.VMEM((rank,), F32),
            pltpu.VMEM((nx * nh, half, rank), BF16),
            pltpu.VMEM((2, k, wide), F32),
            pltpu.VMEM((3, nzx, k, wide), BF16), pltpu.VMEM((3, k, wide), BF16),
            pltpu.VMEM((3, nf, k, wide), F32), pltpu.VMEM((3, k, wide), F32),
            pltpu.VMEM((2, nf, 1, wide), F32), pltpu.VMEM((2, 1, wide), F32),
            pltpu.VMEM((2, nz, k, nx * wide), BF16), pltpu.VMEM((2, nz, k, nx * wide), BF16),
            pltpu.VMEM((nz, k, nx * wide), BF16), pltpu.VMEM((nz, k, nx * wide), BF16),
            pltpu.VMEM((2, nx, k, wide), F32), pltpu.VMEM((2, nx, k, wide), F32),
            pltpu.VMEM((2, k, wide), F32), pltpu.VMEM((2, k, wide), F32),
            pltpu.VMEM((2, ny, 1, rank), F32), pltpu.VMEM((2, ny, 1, rank), F32),
            pltpu.VMEM((2, nzx, 1, rank + wide), F32), pltpu.VMEM((2, 1, rank + wide), F32),
            pltpu.VMEM((2, ny, 1, rank + wide), F32), pltpu.VMEM((2, 1, rank + wide), F32),
            pltpu.VMEM((2, nz, k, nx * wide), BF16), pltpu.VMEM((2, k, nx * wide), BF16),
            pltpu.VMEM((2, nx, k, wide), F32),
            pltpu.VMEM((nzx * nh, 1, wide), F32), pltpu.VMEM((1, wide), F32),
            dma((6,)), dma((26,)), dma((26,)), dma((5, nz)),
        ],
        compiler_params=pltpu.CompilerParams(collective_id=0, has_side_effects=True),
    )(design_matrix, labels.reshape(1, -1), weights, lambdas.reshape(1, -1), sketch, sketch_values)


def solution(mesh):
    sizes = (8, 4, 2, 4, 2)
    finer = Mesh(mesh.devices.reshape(sizes), SAMP + FEAT)
    placed = (P(SAMP, FEAT), P(SAMP), P(None, FEAT_SAMP), P(), P(FEAT_SAMP, None), P())
    return jax.shard_map(
        functools.partial(shards, sizes), mesh=finer, in_specs=placed, out_specs=P(None, FEAT_SAMP), check_vma=False
    )
```

```python
import functools

import jax
import jax.numpy as jnp
from jax import lax
from jax.experimental import pallas as pl
from jax.experimental.pallas import tpu as pltpu
from jax.sharding import Mesh
from jax.sharding import PartitionSpec as P

SAMP = ("samp_0", "samp_1", "samp_2")
FEAT = ("feat_0", "feat_1")
FEAT_SAMP = FEAT + SAMP
F32, BF16 = jnp.float32, jnp.bfloat16
BY_LANES = (((1,), (1,)), ((), ()))
BY_ROWS = (((1,), (0,)), ((), ()))


def far_first(n):
    return sorted(range(n), key=lambda d: -min(d, n - d))


def split3(value):
    high = value.astype(BF16)
    rest = value - high.astype(F32)
    mid = rest.astype(BF16)
    low = (rest - mid.astype(F32)).astype(BF16)
    return jnp.concatenate([high, mid, low], axis=0)


def kernel(sizes, x_hbm, labels_hbm, w_hbm, lam_hbm, s_hbm, sv_hbm, out_ref,
           xv, labels_ref, w_ref, lam_ref, sv_ref, sp, wb, ag, ags, ft, fts, fs, fss, rs, rss, rl, rls, xr, xs, yh, yhs,
           pr, prs, pz, pzs, pa, pas, cz, czs, cf, kz, kzs, local_sem, send_sem, recv_sem, gather_sem):
    nz, nx, nh, nl, nc = sizes
    nzx, nf, ny = nz * nx, nl * nc, nh * nl * nc
    k, half = w_ref.shape
    wide = 2 * half
    rank = s_hbm.shape[1]
    z, x, h, l, c = (lax.axis_index(name) for name in SAMP + FEAT)
    zx, f, y = z * nx + x, l * nc + c, (h * nl + l) * nc + c

    zx_peers = []
    for dz in far_first(nz):
        for dx in far_first(nx):
            if dz or dx:
                zz, xx = lax.rem(z + dz, nz), lax.rem(x + dx, nx)
                zx_peers.append((zz * nx + xx, {"samp_0": zz, "samp_1": xx}))
    y_peers, f_peers = [], []
    for dl in far_first(nl):
        for dh in reversed(range(nh)):
            for dc in reversed(range(nc)):
                if dh or dl or dc:
                    hh, ll, cc = lax.rem(h + dh, nh), lax.rem(l + dl, nl), lax.rem(c + dc, nc)
                    y_peers.append(((hh * nl + ll) * nc + cc, {"samp_2": hh, "feat_0": ll, "feat_1": cc}))
                    if not dh:
                        f_peers.append((ll * nc + cc, {"feat_0": ll, "feat_1": cc}))
    partner = {"samp_2": 1 - h}

    barrier = pltpu.get_barrier_semaphore()
    for _, peer in zx_peers + y_peers:
        pl.semaphore_signal(barrier, inc=1, device_id=peer, device_id_type=pl.DeviceIdType.MESH)

    loads = [pltpu.make_async_copy(src, dst, local_sem.at[j]) for j, (src, dst) in enumerate(
        [(w_hbm, w_ref), (lam_hbm, lam_ref), (sv_hbm, sv_ref), (labels_hbm, labels_ref), (s_hbm, sp.at[x * nh + h]), (x_hbm, xv)])]
    for load in loads:
        load.start()

    def copy(phase, src, dst, peer):
        return pltpu.make_async_remote_copy(
            src_ref=src, dst_ref=dst, send_sem=send_sem.at[phase], recv_sem=recv_sem.at[phase],
            device_id=peer, device_id_type=pl.DeviceIdType.MESH)

    sent = []

    def whole(phase, buffer, peer):
        arrived = copy(phase, buffer, buffer, peer)
        arrived.wait_recv()
        sent.append(arrived)

    lane = lax.broadcasted_iota(jnp.int32, (k, wide), 1)
    row = lax.broadcasted_iota(jnp.int32, (k, wide), 0)

    def pack(*columns):
        total = 0.0
        for place, column in enumerate(columns):
            total = total + jnp.where(lane == row + place * k, column, 0.0)
        return jnp.sum(total, axis=0, keepdims=True)

    def unpack(packed, place):
        return jnp.sum(jnp.where(lane == row + place * k, packed, 0.0), axis=1, keepdims=True)

    def lanes(value):
        return jnp.sum(value, axis=1, keepdims=True)

    def gather_start(i, value):
        ags[i] = value.astype(BF16)
        ag[i, zx] = value.astype(BF16)
        for dz in far_first(nz):
            for dx in far_first(nx):
                if dz or dx:
                    zz, xx = lax.rem(z + dz, nz), lax.rem(x + dx, nx)
                    pltpu.make_async_remote_copy(
                        src_ref=ags.at[i], dst_ref=ag.at[i, zx], send_sem=send_sem.at[2 + i], recv_sem=gather_sem.at[i, dz],
                        device_id={"samp_0": zz, "samp_1": xx}, device_id_type=pl.DeviceIdType.MESH).start()

    def spread_start(i, value):
        czs[i] = value.astype(BF16)
        for dz in far_first(nz):
            zz = lax.rem(z + dz, nz)
            if dz:
                pltpu.make_async_remote_copy(
                    src_ref=czs.at[i], dst_ref=cz.at[i, z], send_sem=send_sem.at[23 + i], recv_sem=gather_sem.at[3 + i, dz],
                    device_id={"samp_0": zz}, device_id_type=pl.DeviceIdType.MESH).start()

    def arrived_group(phase, place, dz, group):
        pltpu.make_async_remote_copy(
            src_ref=group, dst_ref=group, send_sem=send_sem.at[phase], recv_sem=gather_sem.at[place, dz],
            device_id=zx_peers[0][1], device_id_type=pl.DeviceIdType.MESH).wait_recv()

    def rows_of(field, zz):
        start = pl.multiple_of(zz * (nx * wide), nx * wide)
        return lax.dot_general(field, xv[:, pl.ds(start, nx * wide)], BY_LANES, preferred_element_type=F32)

    def gather_rows(i):
        total = jnp.zeros((k, xv.shape[0]), F32)
        for dz in reversed(far_first(nz)):
            arrived_group(2 + i, i, dz, ag.at[i, pl.ds(0, nx if dz else nx - 1)])
            zz = lax.rem(z + (nz - dz), nz)
            total = total + rows_of(jnp.concatenate([ag[i, zz * nx + q] for q in range(nx)], axis=1), zz)
        sent.append(copy(2 + i, ag.at[i, pl.ds(0, nzx - 1)], ag.at[i, pl.ds(0, nzx - 1)], zx_peers[0][1]))
        return total

    def spread_rows(i, total):
        for dz in reversed(far_first(nz)):
            zz = lax.rem(z + (nz - dz), nz)
            if dz:
                arrived_group(23 + i, 3 + i, dz, cz.at[i, 0])
                total = total + rows_of(cz[i, zz], zz)
            else:
                total = total + rows_of(czs[i], zz)
        sent.append(copy(23 + i, cz.at[i, pl.ds(0, nz - 1)], cz.at[i, pl.ds(0, nz - 1)], zx_peers[0][1]))
        return total

    def feat_sum(i, value):
        fts[i] = value
        ft[i, f] = value
        for _, peer in f_peers:
            copy(5 + i, fts.at[i], ft.at[i, f], peer).start()
        whole(5 + i, ft.at[i, pl.ds(0, nf - 1)], f_peers[0][1])
        return jnp.sum(ft[i], axis=0)

    def feat_scalars_start(i, value):
        fss[i] = value
        fs[i, f] = value
        for _, peer in f_peers:
            copy(8 + i, fss.at[i], fs.at[i, f], peer).start()

    def feat_scalars(i):
        whole(8 + i, fs.at[i, pl.ds(0, nf - 1)], f_peers[0][1])
        return jnp.sum(fs[i], axis=0)

    def reduce_columns(i, values, state, scalars, low_too):
        for dz in far_first(nz):
            zz = lax.rem(z + dz, nz)
            start = pl.multiple_of(zz * (nx * wide), nx * wide)
            part = lax.dot_general(values, xv[:, pl.ds(start, nx * wide)], BY_ROWS, preferred_element_type=F32)
            high = part.astype(BF16)
            rss[i, zz] = high
            if low_too:
                rls[zz] = (part - high.astype(F32)).astype(BF16)
            if dz:
                copy(10 + i, rss.at[i, zz], rs.at[i, z], {"samp_0": zz}).start()
        rs[i, z] = rss[i, z]
        if low_too:
            for dz in far_first(nz):
                zz = lax.rem(z + dz, nz)
                if dz:
                    copy(25, rls.at[zz], rl.at[z], {"samp_0": zz}).start()
            rl[z] = rls[z]
        whole(10 + i, rs.at[i, pl.ds(0, nz - 1)], zx_peers[0][1])
        along_z = jnp.sum(rs[i].astype(F32), axis=0)
        ridge = (0.5 * lam) * state
        chunks = [along_z[:, q * wide:(q + 1) * wide] + ridge * jnp.where(x == q, 1.0, 0.0) for q in range(nx)]

        if i == 0:
            whole(1, sp.at[pl.ds(0, nx * nh - 1)], partner)
        sketch = sp[...].reshape(nx * nh * half, rank)
        parts = lax.dot_general(split3(jnp.concatenate(chunks, axis=1)), sketch, BY_ROWS, preferred_element_type=F32)
        projected = parts[:k] + parts[k:2 * k] + parts[2 * k:]
        for q in range(k):
            prs[i, q] = projected[q:q + 1, :]
        for j, peer in y_peers:
            copy(14 + i, prs.at[i, j], pr.at[i, y], peer).start()
        pr[i, y] = prs[i, y]

        if low_too:
            whole(25, rl.at[pl.ds(0, nz - 1)], zx_peers[0][1])
            low = jnp.sum(rl[...].astype(F32), axis=0)
            chunks = [chunks[q] + low[:, q * wide:(q + 1) * wide] for q in range(nx)]
        for q in range(nx):
            xs[i, q] = chunks[q]
        for dx in far_first(nx):
            xx = lax.rem(x + dx, nx)
            if dx:
                copy(21 + i, xs.at[i, xx], xr.at[i, x], {"samp_1": xx}).start()
        xr[i, x] = xs[i, x]
        whole(21 + i, xr.at[i, pl.ds(0, nx - 1)], {"samp_1": lax.rem(x + 1, nx)})
        part = jnp.sum(xr[i], axis=0)
        yhs[i] = part
        copy(12 + i, yhs.at[i], yh.at[i], partner).start()

        whole(14 + i, pr.at[i, pl.ds(0, ny - 1)], y_peers[0][1])
        mine = jnp.sum(pr[i], axis=0)
        if scalars is not None:
            mine = jnp.concatenate([mine, scalars], axis=1)
        across = slice(0, mine.shape[1])
        pzs[i, :, across] = mine
        pz[i, zx, :, across] = mine
        for _, peer in zx_peers:
            copy(16 + i, pzs.at[i, :, across], pz.at[i, zx, :, across], peer).start()

        whole(12 + i, yh.at[i], partner)
        vector = part + yh[i]
        gather_start(1 + i, vector)

        whole(16 + i, pz.at[i, pl.ds(0, nzx - 1), :, across], zx_peers[0][1])
        mine = jnp.sum(pz[i, :, :, across], axis=0)
        pas[i, :, across] = mine
        pa[i, y, :, across] = mine
        for _, peer in y_peers:
            copy(18 + i, pas.at[i, :, across], pa.at[i, y, :, across], peer).start()
        image = gather_rows(1 + i)
        whole(18 + i, pa.at[i, pl.ds(0, ny - 1), :, across], y_peers[0][1])
        full = jnp.concatenate([pa[i, q, :, across] for q in range(k)], axis=0)
        if scalars is not None:
            scalars = jnp.sum(full[:, rank:], axis=0, keepdims=True) * (1.0 / nf)

        parts = lax.dot_general(split3(ratios * full[:, :rank]), sketch, BY_LANES, preferred_element_type=F32)
        correction = parts[:k] + parts[k:2 * k] + parts[2 * k:]
        spread_start(i, correction)
        for q in range(nx):
            cf[i, q] = correction[:, q * wide:(q + 1) * wide]
        return vector, vector + cf[i, x], image, scalars

    for load in loads[:4]:
        load.wait()
    lam = jnp.sum(jnp.where(lax.broadcasted_iota(jnp.int32, (k, k), 0) == lax.broadcasted_iota(jnp.int32, (k, k), 1),
                            lam_ref[...], 0.0), axis=1, keepdims=True)
    values = sv_ref[...].reshape(1, rank)
    ratios = (jnp.min(values, axis=1, keepdims=True) + lam) / (values + lam) - 1.0
    wb[0, :, :half] = w_ref[...]
    wb[0, :, half:] = w_ref[...]
    pl.semaphore_wait(barrier, len(zx_peers) + len(y_peers))
    copy(0, wb.at[0], wb.at[1], partner).start()
    whole(0, wb.at[1], partner)
    own = (lane // half) == h
    weights = jnp.where(own, wb[0], wb[1])
    gather_start(0, weights)
    loads[4].wait()
    for dh in reversed(range(nh)):
        for dx in far_first(nx):
            if dh or dx:
                peer = {"samp_1": lax.rem(x + dx, nx), "samp_2": lax.rem(h + dh, nh)}
                copy(1, sp.at[x * nh + h], sp.at[x * nh + h], peer).start()
    loads[5].wait()

    logits = feat_sum(0, gather_rows(0))
    probability = jax.nn.sigmoid(logits)
    diag = probability * (1.0 - probability)
    miss = (probability - labels_ref[...].astype(F32)).astype(BF16)
    gradient, gradient_pre, image, _ = reduce_columns(0, miss, weights, None, True)
    residual, direction = -gradient, -gradient_pre
    feat_scalars_start(0, pack(0.5 * lanes(residual * direction), 0.5 * lam * lanes(direction * direction)))
    image = -feat_sum(1, spread_rows(0, image))
    scalars = feat_scalars(0) + pack(jnp.zeros((k, 1), F32), lanes(diag * image * image))
    hess_dir, hess_pre, image_pre, scalars = reduce_columns(1, (diag * image).astype(BF16), direction, scalars, False)
    res_dot, curvature = unpack(scalars, 0), unpack(scalars, 1)
    step = res_dot / curvature
    residual = residual - step * hess_dir
    precond = direction - step * hess_pre
    feat_scalars_start(1, pack(0.5 * lanes(residual * precond), 0.5 * lam * lanes(precond * precond),
                               0.5 * lam * lanes(precond * direction)))
    image_pre = image - step * feat_sum(2, spread_rows(1, image_pre))
    mine = feat_scalars(1) + pack(jnp.zeros((k, 1), F32), lanes(diag * image_pre * image_pre),
                                  lanes(diag * image_pre * image))
    kzs[...] = mine
    kz[zx * nh + h] = mine
    for dh in reversed(range(nh)):
        for dz in far_first(nz):
            for dx in far_first(nx):
                if dh or dz or dx:
                    peer = {"samp_0": lax.rem(z + dz, nz), "samp_1": lax.rem(x + dx, nx), "samp_2": lax.rem(h + dh, nh)}
                    copy(20, kzs, kz.at[zx * nh + h], peer).start()
    whole(20, kz.at[pl.ds(0, nzx * nh - 1)], partner)
    scalars = jnp.sum(kz[...], axis=0)
    new_dot, pre_pre, pre_dir = (unpack(scalars, place) for place in range(3))
    beta = new_dot / res_dot
    last = new_dot / (pre_pre + 2.0 * beta * pre_dir + beta * beta * curvature)
    update = step * direction + last * (precond + beta * direction)
    update = jnp.where(h == 0, update, pltpu.roll(update, half, 1))
    out_ref[...] = w_ref[...] + update[:, :half]
    for arrived in sent:
        arrived.wait_send()


def shards(sizes, design_matrix, labels, weights, lambdas, sketch, sketch_values):
    nz, nx, nh, nl, nc = sizes
    nzx, nf, ny = nz * nx, nl * nc, nh * nl * nc
    k, half = weights.shape
    wide = 2 * half
    rank = sketch.shape[1]
    vmem = pl.BlockSpec(memory_space=pltpu.VMEM)
    anywhere = pl.BlockSpec(memory_space=pl.ANY)
    dma = pltpu.SemaphoreType.DMA
    return pl.pallas_call(
        functools.partial(kernel, sizes),
        name="step",
        out_shape=jax.ShapeDtypeStruct((k, half), F32),
        in_specs=[anywhere] * 6,
        out_specs=vmem,
        scratch_shapes=[
            pltpu.VMEM(design_matrix.shape, BF16),
            pltpu.VMEM((1, design_matrix.shape[0]), jnp.int32), pltpu.VMEM((k, half), F32), pltpu.VMEM((1, k), F32),
            pltpu.VMEM((rank,), F32),
            pltpu.VMEM((nx * nh, half, rank), BF16),
            pltpu.VMEM((2, k, wide), F32),
            pltpu.VMEM((3, nzx, k, wide), BF16), pltpu.VMEM((3, k, wide), BF16),
            pltpu.VMEM((3, nf, k, wide), F32), pltpu.VMEM((3, k, wide), F32),
            pltpu.VMEM((2, nf, 1, wide), F32), pltpu.VMEM((2, 1, wide), F32),
            pltpu.VMEM((2, nz, k, nx * wide), BF16), pltpu.VMEM((2, nz, k, nx * wide), BF16),
            pltpu.VMEM((nz, k, nx * wide), BF16), pltpu.VMEM((nz, k, nx * wide), BF16),
            pltpu.VMEM((2, nx, k, wide), F32), pltpu.VMEM((2, nx, k, wide), F32),
            pltpu.VMEM((2, k, wide), F32), pltpu.VMEM((2, k, wide), F32),
            pltpu.VMEM((2, ny, 1, rank), F32), pltpu.VMEM((2, ny, 1, rank), F32),
            pltpu.VMEM((2, nzx, 1, rank + wide), F32), pltpu.VMEM((2, 1, rank + wide), F32),
            pltpu.VMEM((2, ny, 1, rank + wide), F32), pltpu.VMEM((2, 1, rank + wide), F32),
            pltpu.VMEM((2, nz, k, nx * wide), BF16), pltpu.VMEM((2, k, nx * wide), BF16),
            pltpu.VMEM((2, nx, k, wide), F32),
            pltpu.VMEM((nzx * nh, 1, wide), F32), pltpu.VMEM((1, wide), F32),
            dma((6,)), dma((26,)), dma((26,)), dma((5, nz)),
        ],
        compiler_params=pltpu.CompilerParams(collective_id=0, has_side_effects=True),
    )(design_matrix, labels.reshape(1, -1), weights, lambdas.reshape(1, -1), sketch, sketch_values)


def solution(mesh):
    sizes = (8, 4, 2, 4, 2)
    finer = Mesh(mesh.devices.reshape(sizes), SAMP + FEAT)
    placed = (P(SAMP, FEAT), P(SAMP), P(None, FEAT_SAMP), P(), P(FEAT_SAMP, None), P())
    return jax.shard_map(
        functools.partial(shards, sizes), mesh=finer, in_specs=placed, out_specs=P(None, FEAT_SAMP), check_vma=False
    )
```

```python
import functools

import jax
import jax.numpy as jnp
from jax import lax
from jax.experimental import pallas as pl
from jax.experimental.pallas import tpu as pltpu
from jax.sharding import Mesh
from jax.sharding import PartitionSpec as P

SAMP = ("samp_0", "samp_1", "samp_2")
FEAT = ("feat_0", "feat_1")
FEAT_SAMP = FEAT + SAMP
F32, BF16 = jnp.float32, jnp.bfloat16
BY_LANES = (((1,), (1,)), ((), ()))
BY_ROWS = (((1,), (0,)), ((), ()))


def far_first(n):
    return sorted(range(n), key=lambda d: -min(d, n - d))


def split3(value):
    high = value.astype(BF16)
    rest = value - high.astype(F32)
    mid = rest.astype(BF16)
    low = (rest - mid.astype(F32)).astype(BF16)
    return jnp.concatenate([high, mid, low], axis=0)


def kernel(sizes, x_hbm, labels_hbm, w_hbm, lam_hbm, s_hbm, sv_hbm, out_ref,
           xv, labels_ref, w_ref, lam_ref, sv_ref, sp, wb, ag, ags, ft, fts, fs, fss, rs, rss, rl, rls, ws, wss, xr, xs, zr, zs, spz, yh, yhs,
           pr, prs, pz, pzs, pa, pas, cz, czs, cf, dz_ref, dzs, df, kz, kzs, local_sem, send_sem, recv_sem, gather_sem, ring_sem):
    nz, nx, nh, nl, nc = sizes
    nzx, nf, ny = nz * nx, nl * nc, nh * nl * nc
    k, half = w_ref.shape
    wide = 2 * half
    rank = s_hbm.shape[1]
    z, x, h, l, c = (lax.axis_index(name) for name in SAMP + FEAT)
    zx, f, y = z * nx + x, l * nc + c, (h * nl + l) * nc + c

    zx_peers = []
    for dz in far_first(nz):
        for dx in far_first(nx):
            if dz or dx:
                zz, xx = lax.rem(z + dz, nz), lax.rem(x + dx, nx)
                zx_peers.append((zz * nx + xx, {"samp_0": zz, "samp_1": xx}))
    y_peers, f_peers = [], []
    for dl in far_first(nl):
        for dh in reversed(range(nh)):
            for dc in reversed(range(nc)):
                if dh or dl or dc:
                    hh, ll, cc = lax.rem(h + dh, nh), lax.rem(l + dl, nl), lax.rem(c + dc, nc)
                    y_peers.append(((hh * nl + ll) * nc + cc, {"samp_2": hh, "feat_0": ll, "feat_1": cc}))
                    if not dh:
                        f_peers.append((ll * nc + cc, {"feat_0": ll, "feat_1": cc}))
    partner = {"samp_2": 1 - h}

    barrier = pltpu.get_barrier_semaphore()
    for _, peer in zx_peers + y_peers:
        pl.semaphore_signal(barrier, inc=1, device_id=peer, device_id_type=pl.DeviceIdType.MESH)

    loads = [pltpu.make_async_copy(src, dst, local_sem.at[j]) for j, (src, dst) in enumerate(
        [(w_hbm, w_ref), (lam_hbm, lam_ref), (sv_hbm, sv_ref), (labels_hbm, labels_ref), (s_hbm, sp.at[x * nh + h]), (x_hbm, xv)])]
    for load in loads:
        load.start()

    def copy(phase, src, dst, peer):
        return pltpu.make_async_remote_copy(
            src_ref=src, dst_ref=dst, send_sem=send_sem.at[phase], recv_sem=recv_sem.at[phase],
            device_id=peer, device_id_type=pl.DeviceIdType.MESH)

    sent = []

    def whole(phase, buffer, peer):
        arrived = copy(phase, buffer, buffer, peer)
        arrived.wait_recv()
        sent.append(arrived)

    lane = lax.broadcasted_iota(jnp.int32, (k, wide), 1)
    row = lax.broadcasted_iota(jnp.int32, (k, wide), 0)

    def pack(*columns):
        total = 0.0
        for place, column in enumerate(columns):
            total = total + jnp.where(lane == row + place * k, column, 0.0)
        return jnp.sum(total, axis=0, keepdims=True)

    def unpack(packed, place):
        return jnp.sum(jnp.where(lane == row + place * k, packed, 0.0), axis=1, keepdims=True)

    def lanes(value):
        return jnp.sum(value, axis=1, keepdims=True)

    def gather_start(i, value):
        ags[i] = value.astype(BF16)
        ag[i, zx] = value.astype(BF16)
        for dz in far_first(nz):
            for dx in far_first(nx):
                if dz or dx:
                    zz, xx = lax.rem(z + dz, nz), lax.rem(x + dx, nx)
                    pltpu.make_async_remote_copy(
                        src_ref=ags.at[i], dst_ref=ag.at[i, zx], send_sem=send_sem.at[2 + i], recv_sem=gather_sem.at[i, dz],
                        device_id={"samp_0": zz, "samp_1": xx}, device_id_type=pl.DeviceIdType.MESH).start()

    def spread_start(value):
        czs[...] = value.astype(BF16)
        for dz in far_first(nz):
            zz = lax.rem(z + dz, nz)
            if dz:
                pltpu.make_async_remote_copy(
                    src_ref=czs, dst_ref=cz.at[z], send_sem=send_sem.at[23], recv_sem=gather_sem.at[3, dz],
                    device_id={"samp_0": zz}, device_id_type=pl.DeviceIdType.MESH).start()

    def arrived_group(phase, place, dz, group):
        pltpu.make_async_remote_copy(
            src_ref=group, dst_ref=group, send_sem=send_sem.at[phase], recv_sem=gather_sem.at[place, dz],
            device_id=zx_peers[0][1], device_id_type=pl.DeviceIdType.MESH).wait_recv()

    def rows_of(field, zz):
        start = pl.multiple_of(zz * (nx * wide), nx * wide)
        return lax.dot_general(field, xv[:, pl.ds(start, nx * wide)], BY_LANES, preferred_element_type=F32)

    def gather_rows(i):
        total = jnp.zeros((k, xv.shape[0]), F32)
        for dz in reversed(far_first(nz)):
            arrived_group(2 + i, i, dz, ag.at[i, pl.ds(0, nx if dz else nx - 1)])
            zz = lax.rem(z + (nz - dz), nz)
            total = total + rows_of(jnp.concatenate([ag[i, zz * nx + q] for q in range(nx)], axis=1), zz)
        sent.append(copy(2 + i, ag.at[i, pl.ds(0, nzx - 1)], ag.at[i, pl.ds(0, nzx - 1)], zx_peers[0][1]))
        return total

    def spread_rows(total):
        for dz in reversed(far_first(nz)):
            zz = lax.rem(z + (nz - dz), nz)
            if dz:
                arrived_group(23, 3, dz, cz.at[0])
                total = total + rows_of(cz[zz], zz)
            else:
                total = total + rows_of(czs[...], zz)
        sent.append(copy(23, cz.at[pl.ds(0, nz - 1)], cz.at[pl.ds(0, nz - 1)], zx_peers[0][1]))
        return total

    def x_spread_rows(total):
        whole(24, dz_ref.at[pl.ds(0, nx - 1)], {"samp_1": lax.rem(x + 1, nx)})
        for zz in range(nz):
            field = jnp.concatenate([dz_ref[q, :, zz * wide:(zz + 1) * wide] for q in range(nx)], axis=1)
            total = total + rows_of(field, zz)
        return total

    def ring(step):
        ahead, behind = {"samp_0": lax.rem(z + 1, nz)}, {"samp_0": lax.rem(z + nz - 1, nz)}
        for way, peer in ((0, ahead), (1, behind)):
            if step > 1 and (way == 0 or step <= nz // 2):
                last = spz.at[0]
                pltpu.make_async_remote_copy(
                    src_ref=last, dst_ref=last, send_sem=send_sem.at[26], recv_sem=ring_sem.at[step - 2, way],
                    device_id=peer, device_id_type=pl.DeviceIdType.MESH).wait_recv()
            if step <= nz // 2 - way:
                offset = step - 1 if way else nz - (step - 1)
                block = lax.rem(z + offset, nz)
                pltpu.make_async_remote_copy(
                    src_ref=sp.at[pl.ds(x * nh, nh)] if step == 1 else spz.at[block], dst_ref=spz.at[block],
                    send_sem=send_sem.at[26], recv_sem=ring_sem.at[step - 1, way],
                    device_id=peer, device_id_type=pl.DeviceIdType.MESH).start()
        if step == 1:
            spz[z] = sp[pl.ds(x * nh, nh)]
        if step == nz // 2 + 1:
            sent.append(copy(26, spz.at[pl.ds(0, nz - 1)], spz.at[pl.ds(0, nz - 1)], ahead))

    def feat_sum(i, value, step=None):
        fts[i] = value
        ft[i, f] = value
        for _, peer in f_peers:
            copy(5 + i, fts.at[i], ft.at[i, f], peer).start()
        if step:
            ring(step)
        whole(5 + i, ft.at[i, pl.ds(0, nf - 1)], f_peers[0][1])
        return jnp.sum(ft[i], axis=0)

    def feat_scalars_start(i, value):
        fss[i] = value
        fs[i, f] = value
        for _, peer in f_peers:
            copy(8 + i, fss.at[i], fs.at[i, f], peer).start()

    def feat_scalars(i):
        whole(8 + i, fs.at[i, pl.ds(0, nf - 1)], f_peers[0][1])
        return jnp.sum(fs[i], axis=0)

    def along_z(values, state):
        for dz in far_first(nz):
            zz = lax.rem(z + dz, nz)
            start = pl.multiple_of(zz * (nx * wide), nx * wide)
            part = lax.dot_general(values, xv[:, pl.ds(start, nx * wide)], BY_ROWS, preferred_element_type=F32)
            high = part.astype(BF16)
            rss[zz] = high
            rls[zz] = (part - high.astype(F32)).astype(BF16)
            if dz:
                copy(10, rss.at[zz], rs.at[z], {"samp_0": zz}).start()
        rs[z] = rss[z]
        for dz in far_first(nz):
            zz = lax.rem(z + dz, nz)
            if dz:
                copy(25, rls.at[zz], rl.at[z], {"samp_0": zz}).start()
        rl[z] = rls[z]
        whole(10, rs.at[pl.ds(0, nz - 1)], zx_peers[0][1])
        total = jnp.sum(rs[...].astype(F32), axis=0)
        ridge = (0.5 * lam) * state
        chunks = [total[:, q * wide:(q + 1) * wide] + ridge * jnp.where(x == q, 1.0, 0.0) for q in range(nx)]
        whole(1, sp.at[pl.ds(0, nx * nh - 1)], partner)
        sketch = sp[...].reshape(nx * nh * half, rank)
        project_start(0, chunks, sketch)
        ring(1)

        whole(25, rl.at[pl.ds(0, nz - 1)], zx_peers[0][1])
        low = jnp.sum(rl[...].astype(F32), axis=0)
        for q in range(nx):
            xs[q] = chunks[q] + low[:, q * wide:(q + 1) * wide]
        for dx in far_first(nx):
            xx = lax.rem(x + dx, nx)
            if dx:
                copy(21, xs.at[xx], xr.at[x], {"samp_1": xx}).start()
        xr[x] = xs[x]
        whole(21, xr.at[pl.ds(0, nx - 1)], {"samp_1": lax.rem(x + 1, nx)})
        vector, image, full = project_finish(0, jnp.sum(xr[...], axis=0), None, 2)
        correction = spread(full, sketch)
        spread_start(correction)
        for q in range(nx):
            cf[q] = correction[:, q * wide:(q + 1) * wide]
        return vector, vector + cf[x], image

    def along_x(values, state, scalars):
        for zz in range(nz):
            part = lax.dot_general(values, xv[:, zz * nx * wide:(zz + 1) * nx * wide], BY_ROWS, preferred_element_type=F32)
            for q in range(nx):
                wss[q, :, zz * wide:(zz + 1) * wide] = part[:, q * wide:(q + 1) * wide].astype(BF16)
        for dx in far_first(nx):
            xx = lax.rem(x + dx, nx)
            if dx:
                copy(11, wss.at[xx], ws.at[x], {"samp_1": xx}).start()
        ws[x] = wss[x]
        ring(4)
        whole(11, ws.at[pl.ds(0, nx - 1)], {"samp_1": lax.rem(x + 1, nx)})
        total = jnp.sum(ws[...].astype(F32), axis=0)
        ridge = (0.5 * lam) * state
        chunks = [total[:, q * wide:(q + 1) * wide] + ridge * jnp.where(z == q, 1.0, 0.0) for q in range(nz)]
        ring(5)
        sketch = spz[...].reshape(nz * nh * half, rank)
        project_start(1, chunks, sketch)

        for q in range(nz):
            zs[q] = chunks[q]
        for dz in far_first(nz):
            zz = lax.rem(z + dz, nz)
            if dz:
                copy(22, zs.at[zz], zr.at[z], {"samp_0": zz}).start()
        zr[z] = zs[z]
        whole(22, zr.at[pl.ds(0, nz - 1)], zx_peers[0][1])
        vector, image, full = project_finish(1, jnp.sum(zr[...], axis=0), scalars, None)
        correction = spread(full, sketch)
        dzs[...] = correction.astype(BF16)
        for dx in far_first(nx):
            if dx:
                copy(24, dzs, dz_ref.at[x], {"samp_1": lax.rem(x + dx, nx)}).start()
        dz_ref[x] = dzs[...]
        for q in range(nz):
            df[q] = correction[:, q * wide:(q + 1) * wide]
        return vector, vector + df[z], image, jnp.sum(full[:, rank:], axis=0, keepdims=True) * (1.0 / nf)

    def project_start(i, chunks, sketch):
        parts = lax.dot_general(split3(jnp.concatenate(chunks, axis=1)), sketch, BY_ROWS, preferred_element_type=F32)
        projected = parts[:k] + parts[k:2 * k] + parts[2 * k:]
        for q in range(k):
            prs[i, q] = projected[q:q + 1, :]
        for j, peer in y_peers:
            copy(14 + i, prs.at[i, j], pr.at[i, y], peer).start()
        pr[i, y] = prs[i, y]

    def spread(full, sketch):
        parts = lax.dot_general(split3(ratios * full[:, :rank]), sketch, BY_LANES, preferred_element_type=F32)
        return parts[:k] + parts[k:2 * k] + parts[2 * k:]

    def project_finish(i, part, scalars, step):
        yhs[i] = part
        copy(12 + i, yhs.at[i], yh.at[i], partner).start()

        whole(14 + i, pr.at[i, pl.ds(0, ny - 1)], y_peers[0][1])
        mine = jnp.sum(pr[i], axis=0)
        if scalars is not None:
            mine = jnp.concatenate([mine, scalars], axis=1)
        across = slice(0, mine.shape[1])
        pzs[i, :, across] = mine
        pz[i, zx, :, across] = mine
        for _, peer in zx_peers:
            copy(16 + i, pzs.at[i, :, across], pz.at[i, zx, :, across], peer).start()

        whole(12 + i, yh.at[i], partner)
        vector = part + yh[i]
        gather_start(1 + i, vector)

        whole(16 + i, pz.at[i, pl.ds(0, nzx - 1), :, across], zx_peers[0][1])
        mine = jnp.sum(pz[i, :, :, across], axis=0)
        pas[i, :, across] = mine
        pa[i, y, :, across] = mine
        for _, peer in y_peers:
            copy(18 + i, pas.at[i, :, across], pa.at[i, y, :, across], peer).start()
        if step:
            ring(step)
        image = gather_rows(1 + i)
        whole(18 + i, pa.at[i, pl.ds(0, ny - 1), :, across], y_peers[0][1])
        return vector, image, jnp.concatenate([pa[i, q, :, across] for q in range(k)], axis=0)

    for load in loads[:4]:
        load.wait()
    lam = jnp.sum(jnp.where(lax.broadcasted_iota(jnp.int32, (k, k), 0) == lax.broadcasted_iota(jnp.int32, (k, k), 1),
                            lam_ref[...], 0.0), axis=1, keepdims=True)
    values = sv_ref[...].reshape(1, rank)
    ratios = (jnp.min(values, axis=1, keepdims=True) + lam) / (values + lam) - 1.0
    wb[0, :, :half] = w_ref[...]
    wb[0, :, half:] = w_ref[...]
    pl.semaphore_wait(barrier, len(zx_peers) + len(y_peers))
    copy(0, wb.at[0], wb.at[1], partner).start()
    whole(0, wb.at[1], partner)
    own = (lane // half) == h
    weights = jnp.where(own, wb[0], wb[1])
    gather_start(0, weights)
    loads[4].wait()
    for dh in reversed(range(nh)):
        for dx in far_first(nx):
            if dh or dx:
                peer = {"samp_1": lax.rem(x + dx, nx), "samp_2": lax.rem(h + dh, nh)}
                copy(1, sp.at[x * nh + h], sp.at[x * nh + h], peer).start()
    loads[5].wait()

    logits = feat_sum(0, gather_rows(0))
    probability = jax.nn.sigmoid(logits)
    diag = probability * (1.0 - probability)
    miss = (probability - labels_ref[...].astype(F32)).astype(BF16)
    gradient, gradient_pre, image = along_z(miss, weights)
    residual, direction = -gradient, -gradient_pre
    feat_scalars_start(0, pack(0.5 * lanes(residual * direction), 0.5 * lam * lanes(direction * direction)))
    image = -feat_sum(1, spread_rows(image), 3)
    scalars = feat_scalars(0) + pack(jnp.zeros((k, 1), F32), lanes(diag * image * image))
    hess_dir, hess_pre, image_pre, scalars = along_x((diag * image).astype(BF16), direction, scalars)
    res_dot, curvature = unpack(scalars, 0), unpack(scalars, 1)
    step = res_dot / curvature
    residual = residual - step * hess_dir
    precond = direction - step * hess_pre
    feat_scalars_start(1, pack(0.5 * lanes(residual * precond), 0.5 * lam * lanes(precond * precond),
                               0.5 * lam * lanes(precond * direction)))
    image_pre = image - step * feat_sum(2, x_spread_rows(image_pre))
    mine = feat_scalars(1) + pack(jnp.zeros((k, 1), F32), lanes(diag * image_pre * image_pre),
                                  lanes(diag * image_pre * image))
    kzs[...] = mine
    kz[zx * nh + h] = mine
    for dh in reversed(range(nh)):
        for dz in far_first(nz):
            for dx in far_first(nx):
                if dh or dz or dx:
                    peer = {"samp_0": lax.rem(z + dz, nz), "samp_1": lax.rem(x + dx, nx), "samp_2": lax.rem(h + dh, nh)}
                    copy(20, kzs, kz.at[zx * nh + h], peer).start()
    whole(20, kz.at[pl.ds(0, nzx * nh - 1)], partner)
    scalars = jnp.sum(kz[...], axis=0)
    new_dot, pre_pre, pre_dir = (unpack(scalars, place) for place in range(3))
    beta = new_dot / res_dot
    last = new_dot / (pre_pre + 2.0 * beta * pre_dir + beta * beta * curvature)
    update = step * direction + last * (precond + beta * direction)
    update = jnp.where(h == 0, update, pltpu.roll(update, half, 1))
    out_ref[...] = w_ref[...] + update[:, :half]
    for arrived in sent:
        arrived.wait_send()


def shards(sizes, design_matrix, labels, weights, lambdas, sketch, sketch_values):
    nz, nx, nh, nl, nc = sizes
    nzx, nf, ny = nz * nx, nl * nc, nh * nl * nc
    k, half = weights.shape
    wide = 2 * half
    rank = sketch.shape[1]
    vmem = pl.BlockSpec(memory_space=pltpu.VMEM)
    anywhere = pl.BlockSpec(memory_space=pl.ANY)
    dma = pltpu.SemaphoreType.DMA
    return pl.pallas_call(
        functools.partial(kernel, sizes),
        name="step",
        out_shape=jax.ShapeDtypeStruct((k, half), F32),
        in_specs=[anywhere] * 6,
        out_specs=vmem,
        scratch_shapes=[
            pltpu.VMEM(design_matrix.shape, BF16),
            pltpu.VMEM((1, design_matrix.shape[0]), jnp.int32), pltpu.VMEM((k, half), F32), pltpu.VMEM((1, k), F32),
            pltpu.VMEM((rank,), F32),
            pltpu.VMEM((nx * nh, half, rank), BF16),
            pltpu.VMEM((2, k, wide), F32),
            pltpu.VMEM((3, nzx, k, wide), BF16), pltpu.VMEM((3, k, wide), BF16),
            pltpu.VMEM((3, nf, k, wide), F32), pltpu.VMEM((3, k, wide), F32),
            pltpu.VMEM((2, nf, 1, wide), F32), pltpu.VMEM((2, 1, wide), F32),
            pltpu.VMEM((nz, k, nx * wide), BF16), pltpu.VMEM((nz, k, nx * wide), BF16),
            pltpu.VMEM((nz, k, nx * wide), BF16), pltpu.VMEM((nz, k, nx * wide), BF16),
            pltpu.VMEM((nx, k, nz * wide), BF16), pltpu.VMEM((nx, k, nz * wide), BF16),
            pltpu.VMEM((nx, k, wide), F32), pltpu.VMEM((nx, k, wide), F32),
            pltpu.VMEM((nz, k, wide), F32), pltpu.VMEM((nz, k, wide), F32),
            pltpu.VMEM((nz, nh, half, rank), BF16),
            pltpu.VMEM((2, k, wide), F32), pltpu.VMEM((2, k, wide), F32),
            pltpu.VMEM((2, ny, 1, rank), F32), pltpu.VMEM((2, ny, 1, rank), F32),
            pltpu.VMEM((2, nzx, 1, rank + wide), F32), pltpu.VMEM((2, 1, rank + wide), F32),
            pltpu.VMEM((2, ny, 1, rank + wide), F32), pltpu.VMEM((2, 1, rank + wide), F32),
            pltpu.VMEM((nz, k, nx * wide), BF16), pltpu.VMEM((k, nx * wide), BF16),
            pltpu.VMEM((nx, k, wide), F32),
            pltpu.VMEM((nx, k, nz * wide), BF16), pltpu.VMEM((k, nz * wide), BF16),
            pltpu.VMEM((nz, k, wide), F32),
            pltpu.VMEM((nzx * nh, 1, wide), F32), pltpu.VMEM((1, wide), F32),
            dma((6,)), dma((27,)), dma((27,)), dma((4, nz)), dma((nz // 2, 2)),
        ],
        compiler_params=pltpu.CompilerParams(collective_id=0, has_side_effects=True),
    )(design_matrix, labels.reshape(1, -1), weights, lambdas.reshape(1, -1), sketch, sketch_values)


def solution(mesh):
    sizes = (8, 4, 2, 4, 2)
    finer = Mesh(mesh.devices.reshape(sizes), SAMP + FEAT)
    placed = (P(SAMP, FEAT), P(SAMP), P(None, FEAT_SAMP), P(), P(FEAT_SAMP, None), P())
    return jax.shard_map(
        functools.partial(shards, sizes), mesh=finer, in_specs=placed, out_specs=P(None, FEAT_SAMP), check_vma=False
    )
```

```python
import functools

import jax
import jax.numpy as jnp
from jax import lax
from jax.experimental import pallas as pl
from jax.experimental.pallas import tpu as pltpu
from jax.sharding import Mesh
from jax.sharding import PartitionSpec as P

SAMP = ("samp_0", "samp_1", "samp_2")
FEAT = ("feat_0", "feat_1")
FEAT_SAMP = FEAT + SAMP
F32, BF16 = jnp.float32, jnp.bfloat16
BY_LANES = (((1,), (1,)), ((), ()))
BY_ROWS = (((1,), (0,)), ((), ()))


def far_first(n):
    return sorted(range(n), key=lambda d: -min(d, n - d))


def split3(value):
    high = value.astype(BF16)
    rest = value - high.astype(F32)
    mid = rest.astype(BF16)
    low = (rest - mid.astype(F32)).astype(BF16)
    return jnp.concatenate([high, mid, low], axis=0)


def kernel(sizes, x_hbm, labels_hbm, w_hbm, lam_hbm, s_hbm, sv_hbm, out_ref,
           xv, xw, labels_ref, w_ref, lam_ref, sv_ref, sp, wb, ag, ags, ft, fts, fs, fss, rs, rss, rl, rls, ws, wss, xr, xs, zr, zs, spz, yh, yhs,
           pr, prs, pz, pzs, pa, pas, cx, cxs, cf, kz, kzs, local_sem, send_sem, recv_sem, gather_sem, ring_sem, x_sem):
    nz, nx, nh, nl, nc = sizes
    nzx, nf, ny = nz * nx, nl * nc, nh * nl * nc
    k, half = w_ref.shape
    wide = 2 * half
    rank = s_hbm.shape[1]
    z, x, h, l, c = (lax.axis_index(name) for name in SAMP + FEAT)
    zx, f, y = z * nx + x, l * nc + c, (h * nl + l) * nc + c

    zx_peers = []
    for dz in far_first(nz):
        for dx in far_first(nx):
            if dz or dx:
                zz, xx = lax.rem(z + dz, nz), lax.rem(x + dx, nx)
                zx_peers.append((zz * nx + xx, {"samp_0": zz, "samp_1": xx}))
    y_peers, f_peers = [], []
    for dl in far_first(nl):
        for dh in reversed(range(nh)):
            for dc in reversed(range(nc)):
                if dh or dl or dc:
                    hh, ll, cc = lax.rem(h + dh, nh), lax.rem(l + dl, nl), lax.rem(c + dc, nc)
                    y_peers.append(((hh * nl + ll) * nc + cc, {"samp_2": hh, "feat_0": ll, "feat_1": cc}))
                    if not dh:
                        f_peers.append((ll * nc + cc, {"feat_0": ll, "feat_1": cc}))
    partner = {"samp_2": 1 - h}

    barrier = pltpu.get_barrier_semaphore()
    for _, peer in zx_peers + y_peers:
        pl.semaphore_signal(barrier, inc=1, device_id=peer, device_id_type=pl.DeviceIdType.MESH)

    loads = [pltpu.make_async_copy(src, dst, local_sem.at[j]) for j, (src, dst) in enumerate(
        [(w_hbm, w_ref), (lam_hbm, lam_ref), (sv_hbm, sv_ref), (labels_hbm, labels_ref), (s_hbm, sp.at[x * nh + h]), (x_hbm, xv)])]
    for load in loads:
        load.start()
    for q in range(nx):
        for zz in range(nz):
            pltpu.make_async_copy(x_hbm.at[:, pl.ds((zz * nx + q) * wide, wide)], xw.at[:, pl.ds((q * nz + zz) * wide, wide)],
                                  local_sem.at[6]).start()

    def copy(phase, src, dst, peer):
        return pltpu.make_async_remote_copy(
            src_ref=src, dst_ref=dst, send_sem=send_sem.at[phase], recv_sem=recv_sem.at[phase],
            device_id=peer, device_id_type=pl.DeviceIdType.MESH)

    sent = []

    def whole(phase, buffer, peer):
        arrived = copy(phase, buffer, buffer, peer)
        arrived.wait_recv()
        sent.append(arrived)

    lane = lax.broadcasted_iota(jnp.int32, (k, wide), 1)
    row = lax.broadcasted_iota(jnp.int32, (k, wide), 0)

    def pack(*columns):
        total = 0.0
        for place, column in enumerate(columns):
            total = total + jnp.where(lane == row + place * k, column, 0.0)
        return jnp.sum(total, axis=0, keepdims=True)

    def unpack(packed, place):
        return jnp.sum(jnp.where(lane == row + place * k, packed, 0.0), axis=1, keepdims=True)

    def lanes(value):
        return jnp.sum(value, axis=1, keepdims=True)

    def gather_start(i, value):
        ags[i] = value.astype(BF16)
        ag[i, zx] = value.astype(BF16)
        for dz in far_first(nz):
            for dx in far_first(nx):
                if dz or dx:
                    zz, xx = lax.rem(z + dz, nz), lax.rem(x + dx, nx)
                    pltpu.make_async_remote_copy(
                        src_ref=ags.at[i], dst_ref=ag.at[i, zx], send_sem=send_sem.at[2 + i], recv_sem=gather_sem.at[i, dz],
                        device_id={"samp_0": zz, "samp_1": xx}, device_id_type=pl.DeviceIdType.MESH).start()

    def arrived_group(phase, place, dz, group):
        pltpu.make_async_remote_copy(
            src_ref=group, dst_ref=group, send_sem=send_sem.at[phase], recv_sem=gather_sem.at[place, dz],
            device_id=zx_peers[0][1], device_id_type=pl.DeviceIdType.MESH).wait_recv()

    def rows_of(field, zz):
        start = pl.multiple_of(zz * (nx * wide), nx * wide)
        return lax.dot_general(field, xv[:, pl.ds(start, nx * wide)], BY_LANES, preferred_element_type=F32)

    def gather_rows(i):
        total = jnp.zeros((k, xv.shape[0]), F32)
        for dz in reversed(far_first(nz)):
            arrived_group(2 + i, i, dz, ag.at[i, pl.ds(0, nx if dz else nx - 1)])
            zz = lax.rem(z + (nz - dz), nz)
            total = total + rows_of(jnp.concatenate([ag[i, zz * nx + q] for q in range(nx)], axis=1), zz)
        sent.append(copy(2 + i, ag.at[i, pl.ds(0, nzx - 1)], ag.at[i, pl.ds(0, nzx - 1)], zx_peers[0][1]))
        return total

    def by_x(xx):
        return pl.ds(pl.multiple_of(xx * (nz * wide), nz * wide), nz * wide)

    def spread_start(i, value):
        cxs[i] = value.astype(BF16)
        for dx in far_first(nx):
            if dx:
                pltpu.make_async_remote_copy(
                    src_ref=cxs.at[i], dst_ref=cx.at[i, x], send_sem=send_sem.at[23 + i], recv_sem=x_sem.at[i, dx],
                    device_id={"samp_1": lax.rem(x + dx, nx)}, device_id_type=pl.DeviceIdType.MESH).start()
        for q in range(nz):
            cf[q] = value[:, q * wide:(q + 1) * wide]

    def spread_rows(i, total):
        for dx in reversed(far_first(nx)):
            xx = lax.rem(x + (nx - dx), nx)
            if dx:
                pltpu.make_async_remote_copy(
                    src_ref=cxs.at[i], dst_ref=cx.at[i, xx], send_sem=send_sem.at[23 + i], recv_sem=x_sem.at[i, dx],
                    device_id={"samp_1": xx}, device_id_type=pl.DeviceIdType.MESH).wait_recv()
                field = cx[i, xx]
            else:
                field = cxs[i]
            total = total + lax.dot_general(field, xw[:, by_x(xx)], BY_LANES, preferred_element_type=F32)
        sent.append(copy(23 + i, cx.at[i, pl.ds(0, nx - 1)], cx.at[i, pl.ds(0, nx - 1)], zx_peers[0][1]))
        return total

    def ring(step):
        ahead, behind = {"samp_0": lax.rem(z + 1, nz)}, {"samp_0": lax.rem(z + nz - 1, nz)}
        for way, peer in ((0, ahead), (1, behind)):
            if step > 1 and (way == 0 or step <= nz // 2):
                last = spz.at[0]
                pltpu.make_async_remote_copy(
                    src_ref=last, dst_ref=last, send_sem=send_sem.at[26], recv_sem=ring_sem.at[step - 2, way],
                    device_id=peer, device_id_type=pl.DeviceIdType.MESH).wait_recv()
            if step <= nz // 2 - way:
                offset = step - 1 if way else nz - (step - 1)
                block = lax.rem(z + offset, nz)
                pltpu.make_async_remote_copy(
                    src_ref=sp.at[pl.ds(x * nh, nh)] if step == 1 else spz.at[block], dst_ref=spz.at[block],
                    send_sem=send_sem.at[26], recv_sem=ring_sem.at[step - 1, way],
                    device_id=peer, device_id_type=pl.DeviceIdType.MESH).start()
        if step == 1:
            spz[z] = sp[pl.ds(x * nh, nh)]
        if step == nz // 2 + 1:
            sent.append(copy(26, spz.at[pl.ds(0, nz - 1)], spz.at[pl.ds(0, nz - 1)], ahead))

    def feat_sum(i, value):
        fts[i] = value
        ft[i, f] = value
        for _, peer in f_peers:
            copy(5 + i, fts.at[i], ft.at[i, f], peer).start()
        if i == 0:
            whole(27, sp.at[x * nh + 1 - h], partner)
            ring(1)
        whole(5 + i, ft.at[i, pl.ds(0, nf - 1)], f_peers[0][1])
        return jnp.sum(ft[i], axis=0)

    def feat_scalars_start(i, value):
        fss[i] = value
        fs[i, f] = value
        for _, peer in f_peers:
            copy(8 + i, fss.at[i], fs.at[i, f], peer).start()

    def feat_scalars(i):
        whole(8 + i, fs.at[i, pl.ds(0, nf - 1)], f_peers[0][1])
        return jnp.sum(fs[i], axis=0)

    def along_z(values, state):
        for dz in far_first(nz):
            zz = lax.rem(z + dz, nz)
            start = pl.multiple_of(zz * (nx * wide), nx * wide)
            part = lax.dot_general(values, xv[:, pl.ds(start, nx * wide)], BY_ROWS, preferred_element_type=F32)
            high = part.astype(BF16)
            rss[zz] = high
            rls[zz] = (part - high.astype(F32)).astype(BF16)
            if dz:
                copy(10, rss.at[zz], rs.at[z], {"samp_0": zz}).start()
        rs[z] = rss[z]
        for dz in far_first(nz):
            zz = lax.rem(z + dz, nz)
            if dz:
                copy(25, rls.at[zz], rl.at[z], {"samp_0": zz}).start()
        rl[z] = rls[z]
        whole(10, rs.at[pl.ds(0, nz - 1)], zx_peers[0][1])
        total = jnp.sum(rs[...].astype(F32), axis=0)
        ridge = (0.5 * lam) * state
        chunks = [total[:, q * wide:(q + 1) * wide] + ridge * jnp.where(x == q, 1.0, 0.0) for q in range(nx)]
        whole(1, sp.at[pl.ds(0, (nx - 1) * nh)], partner)
        project_start(0, chunks, sp[...].reshape(nx * nh * half, rank))
        ring(2)

        whole(25, rl.at[pl.ds(0, nz - 1)], zx_peers[0][1])
        low = jnp.sum(rl[...].astype(F32), axis=0)
        for q in range(nx):
            xs[q] = chunks[q] + low[:, q * wide:(q + 1) * wide]
        for dx in far_first(nx):
            xx = lax.rem(x + dx, nx)
            if dx:
                copy(21, xs.at[xx], xr.at[x], {"samp_1": xx}).start()
        xr[x] = xs[x]
        whole(21, xr.at[pl.ds(0, nx - 1)], {"samp_1": lax.rem(x + 1, nx)})
        vector, image, full = project_finish(0, jnp.sum(xr[...], axis=0), None)
        ring(5)
        spread_start(0, spread(full))
        return vector, vector + cf[z], image

    def along_x(values, state, scalars):
        for dx in far_first(nx):
            xx = lax.rem(x + dx, nx)
            part = lax.dot_general(values, xw[:, by_x(xx)], BY_ROWS, preferred_element_type=F32)
            wss[xx] = part.astype(BF16)
            if dx:
                copy(11, wss.at[xx], ws.at[x], {"samp_1": xx}).start()
        ws[x] = wss[x]
        whole(11, ws.at[pl.ds(0, nx - 1)], {"samp_1": lax.rem(x + 1, nx)})
        total = jnp.sum(ws[...].astype(F32), axis=0)
        ridge = (0.5 * lam) * state
        chunks = [total[:, q * wide:(q + 1) * wide] + ridge * jnp.where(z == q, 1.0, 0.0) for q in range(nz)]
        project_start(1, chunks, spz[...].reshape(nz * nh * half, rank))

        for q in range(nz):
            zs[q] = chunks[q]
        for dz in far_first(nz):
            zz = lax.rem(z + dz, nz)
            if dz:
                copy(22, zs.at[zz], zr.at[z], {"samp_0": zz}).start()
        zr[z] = zs[z]
        whole(22, zr.at[pl.ds(0, nz - 1)], zx_peers[0][1])
        vector, image, full = project_finish(1, jnp.sum(zr[...], axis=0), scalars)
        spread_start(1, spread(full))
        return vector, vector + cf[z], image, jnp.sum(full[:, rank:], axis=0, keepdims=True) * (1.0 / nf)

    def project_start(i, chunks, sketch):
        parts = lax.dot_general(split3(jnp.concatenate(chunks, axis=1)), sketch, BY_ROWS, preferred_element_type=F32)
        projected = parts[:k] + parts[k:2 * k] + parts[2 * k:]
        for q in range(k):
            prs[i, q] = projected[q:q + 1, :]
        for j, peer in y_peers:
            copy(14 + i, prs.at[i, j], pr.at[i, y], peer).start()
        pr[i, y] = prs[i, y]

    def spread(full):
        sketch = spz[...].reshape(nz * nh * half, rank)
        parts = lax.dot_general(split3(ratios * full[:, :rank]), sketch, BY_LANES, preferred_element_type=F32)
        return parts[:k] + parts[k:2 * k] + parts[2 * k:]

    def project_finish(i, part, scalars):
        yhs[i] = part
        copy(12 + i, yhs.at[i], yh.at[i], partner).start()

        whole(14 + i, pr.at[i, pl.ds(0, ny - 1)], y_peers[0][1])
        mine = jnp.sum(pr[i], axis=0)
        if scalars is not None:
            mine = jnp.concatenate([mine, scalars], axis=1)
        across = slice(0, mine.shape[1])
        pzs[i, :, across] = mine
        pz[i, zx, :, across] = mine
        for _, peer in zx_peers:
            copy(16 + i, pzs.at[i, :, across], pz.at[i, zx, :, across], peer).start()
        if i == 0:
            ring(3)

        whole(12 + i, yh.at[i], partner)
        vector = part + yh[i]
        gather_start(1 + i, vector)

        whole(16 + i, pz.at[i, pl.ds(0, nzx - 1), :, across], zx_peers[0][1])
        mine = jnp.sum(pz[i, :, :, across], axis=0)
        pas[i, :, across] = mine
        pa[i, y, :, across] = mine
        for _, peer in y_peers:
            copy(18 + i, pas.at[i, :, across], pa.at[i, y, :, across], peer).start()
        if i == 0:
            ring(4)
        image = gather_rows(1 + i)
        whole(18 + i, pa.at[i, pl.ds(0, ny - 1), :, across], y_peers[0][1])
        return vector, image, jnp.concatenate([pa[i, q, :, across] for q in range(k)], axis=0)

    for load in loads[:4]:
        load.wait()
    lam = jnp.sum(jnp.where(lax.broadcasted_iota(jnp.int32, (k, k), 0) == lax.broadcasted_iota(jnp.int32, (k, k), 1),
                            lam_ref[...], 0.0), axis=1, keepdims=True)
    values = sv_ref[...].reshape(1, rank)
    ratios = (jnp.min(values, axis=1, keepdims=True) + lam) / (values + lam) - 1.0
    wb[0, :, :half] = w_ref[...]
    wb[0, :, half:] = w_ref[...]
    pl.semaphore_wait(barrier, len(zx_peers) + len(y_peers))
    copy(0, wb.at[0], wb.at[1], partner).start()
    loads[4].wait()
    copy(27, sp.at[x * nh + h], sp.at[x * nh + h], partner).start()
    whole(0, wb.at[1], partner)
    own = (lane // half) == h
    weights = jnp.where(own, wb[0], wb[1])
    gather_start(0, weights)
    for dh in reversed(range(nh)):
        for dx in far_first(nx):
            if dx:
                peer = {"samp_1": lax.rem(x + dx, nx), "samp_2": lax.rem(h + dh, nh)}
                copy(1, sp.at[x * nh + h], sp.at[x * nh + h], peer).start()
    loads[5].wait()
    pltpu.make_async_copy(x_hbm, xw, local_sem.at[6]).wait()

    logits = feat_sum(0, gather_rows(0))
    probability = jax.nn.sigmoid(logits)
    diag = probability * (1.0 - probability)
    miss = (probability - labels_ref[...].astype(F32)).astype(BF16)
    gradient, gradient_pre, image = along_z(miss, weights)
    residual, direction = -gradient, -gradient_pre
    feat_scalars_start(0, pack(0.5 * lanes(residual * direction), 0.5 * lam * lanes(direction * direction)))
    image = -feat_sum(1, spread_rows(0, image))
    scalars = feat_scalars(0) + pack(jnp.zeros((k, 1), F32), lanes(diag * image * image))
    hess_dir, hess_pre, image_pre, scalars = along_x((diag * image).astype(BF16), direction, scalars)
    res_dot, curvature = unpack(scalars, 0), unpack(scalars, 1)
    step = res_dot / curvature
    residual = residual - step * hess_dir
    precond = direction - step * hess_pre
    feat_scalars_start(1, pack(0.5 * lanes(residual * precond), 0.5 * lam * lanes(precond * precond),
                               0.5 * lam * lanes(precond * direction)))
    image_pre = image - step * feat_sum(2, spread_rows(1, image_pre))
    mine = feat_scalars(1) + pack(jnp.zeros((k, 1), F32), lanes(diag * image_pre * image_pre),
                                  lanes(diag * image_pre * image))
    kzs[...] = mine
    kz[zx * nh + h] = mine
    for dh in reversed(range(nh)):
        for dz in far_first(nz):
            for dx in far_first(nx):
                if dh or dz or dx:
                    peer = {"samp_0": lax.rem(z + dz, nz), "samp_1": lax.rem(x + dx, nx), "samp_2": lax.rem(h + dh, nh)}
                    copy(20, kzs, kz.at[zx * nh + h], peer).start()
    whole(20, kz.at[pl.ds(0, nzx * nh - 1)], partner)
    scalars = jnp.sum(kz[...], axis=0)
    new_dot, pre_pre, pre_dir = (unpack(scalars, place) for place in range(3))
    beta = new_dot / res_dot
    last = new_dot / (pre_pre + 2.0 * beta * pre_dir + beta * beta * curvature)
    update = step * direction + last * (precond + beta * direction)
    update = jnp.where(h == 0, update, pltpu.roll(update, half, 1))
    out_ref[...] = w_ref[...] + update[:, :half]
    for arrived in sent:
        arrived.wait_send()


def shards(sizes, design_matrix, labels, weights, lambdas, sketch, sketch_values):
    nz, nx, nh, nl, nc = sizes
    nzx, nf, ny = nz * nx, nl * nc, nh * nl * nc
    k, half = weights.shape
    wide = 2 * half
    rank = sketch.shape[1]
    vmem = pl.BlockSpec(memory_space=pltpu.VMEM)
    anywhere = pl.BlockSpec(memory_space=pl.ANY)
    dma = pltpu.SemaphoreType.DMA
    return pl.pallas_call(
        functools.partial(kernel, sizes),
        name="step",
        out_shape=jax.ShapeDtypeStruct((k, half), F32),
        in_specs=[anywhere] * 6,
        out_specs=vmem,
        scratch_shapes=[
            pltpu.VMEM(design_matrix.shape, BF16), pltpu.VMEM(design_matrix.shape, BF16),
            pltpu.VMEM((1, design_matrix.shape[0]), jnp.int32), pltpu.VMEM((k, half), F32), pltpu.VMEM((1, k), F32),
            pltpu.VMEM((rank,), F32),
            pltpu.VMEM((nx * nh, half, rank), BF16),
            pltpu.VMEM((2, k, wide), F32),
            pltpu.VMEM((3, nzx, k, wide), BF16), pltpu.VMEM((3, k, wide), BF16),
            pltpu.VMEM((3, nf, k, wide), F32), pltpu.VMEM((3, k, wide), F32),
            pltpu.VMEM((2, nf, 1, wide), F32), pltpu.VMEM((2, 1, wide), F32),
            pltpu.VMEM((nz, k, nx * wide), BF16), pltpu.VMEM((nz, k, nx * wide), BF16),
            pltpu.VMEM((nz, k, nx * wide), BF16), pltpu.VMEM((nz, k, nx * wide), BF16),
            pltpu.VMEM((nx, k, nz * wide), BF16), pltpu.VMEM((nx, k, nz * wide), BF16),
            pltpu.VMEM((nx, k, wide), F32), pltpu.VMEM((nx, k, wide), F32),
            pltpu.VMEM((nz, k, wide), F32), pltpu.VMEM((nz, k, wide), F32),
            pltpu.VMEM((nz, nh, half, rank), BF16),
            pltpu.VMEM((2, k, wide), F32), pltpu.VMEM((2, k, wide), F32),
            pltpu.VMEM((2, ny, 1, rank), F32), pltpu.VMEM((2, ny, 1, rank), F32),
            pltpu.VMEM((2, nzx, 1, rank + wide), F32), pltpu.VMEM((2, 1, rank + wide), F32),
            pltpu.VMEM((2, ny, 1, rank + wide), F32), pltpu.VMEM((2, 1, rank + wide), F32),
            pltpu.VMEM((2, nx, k, nz * wide), BF16), pltpu.VMEM((2, k, nz * wide), BF16),
            pltpu.VMEM((nz, k, wide), F32),
            pltpu.VMEM((nzx * nh, 1, wide), F32), pltpu.VMEM((1, wide), F32),
            dma((7,)), dma((28,)), dma((28,)), dma((3, nz)), dma((nz // 2, 2)), dma((2, nx)),
        ],
        compiler_params=pltpu.CompilerParams(collective_id=0, has_side_effects=True),
    )(design_matrix, labels.reshape(1, -1), weights, lambdas.reshape(1, -1), sketch, sketch_values)


def solution(mesh):
    sizes = (8, 4, 2, 4, 2)
    finer = Mesh(mesh.devices.reshape(sizes), SAMP + FEAT)
    placed = (P(SAMP, FEAT), P(SAMP), P(None, FEAT_SAMP), P(), P(FEAT_SAMP, None), P())
    return jax.shard_map(
        functools.partial(shards, sizes), mesh=finer, in_specs=placed, out_specs=P(None, FEAT_SAMP), check_vma=False
    )
```

```python
import functools

import jax
import jax.numpy as jnp
from jax import lax
from jax.experimental import pallas as pl
from jax.experimental.pallas import tpu as pltpu
from jax.sharding import Mesh
from jax.sharding import PartitionSpec as P

SAMP = ("samp_0", "samp_1", "samp_2")
FEAT = ("feat_0", "feat_1")
FEAT_SAMP = FEAT + SAMP
F32, BF16 = jnp.float32, jnp.bfloat16
BY_LANES = (((1,), (1,)), ((), ()))
BY_ROWS = (((1,), (0,)), ((), ()))


def far_first(n):
    return sorted(range(n), key=lambda d: -min(d, n - d))


def split3(value):
    high = value.astype(BF16)
    rest = value - high.astype(F32)
    mid = rest.astype(BF16)
    low = (rest - mid.astype(F32)).astype(BF16)
    return jnp.concatenate([high, mid, low], axis=0)


def kernel(sizes, x_hbm, labels_hbm, w_hbm, lam_hbm, s_hbm, sv_hbm, out_ref,
           xv, xw, labels_ref, w_ref, lam_ref, sv_ref, sp, wb, ag, ags, ft, fts, fs, fss, rs, rss, rl, rls, ws, wss, xr, xs, zr, zs, spz, yh, yhs,
           pr, prs, pz, pzs, pa, pas, cx, cxs, cf, kz, kzs, local_sem, send_sem, recv_sem, gather_sem, ring_sem, x_sem):
    nz, nx, nh, nl, nc = sizes
    nzx, nf, ny = nz * nx, nl * nc, nh * nl * nc
    k, half = w_ref.shape
    wide = 2 * half
    rank = s_hbm.shape[1]
    z, x, h, l, c = (lax.axis_index(name) for name in SAMP + FEAT)
    zx, f, y = z * nx + x, l * nc + c, (h * nl + l) * nc + c

    zx_peers = []
    for dz in far_first(nz):
        for dx in far_first(nx):
            if dz or dx:
                zz, xx = lax.rem(z + dz, nz), lax.rem(x + dx, nx)
                zx_peers.append((zz * nx + xx, {"samp_0": zz, "samp_1": xx}))
    y_peers, f_peers = [], []
    for dl in far_first(nl):
        for dh in reversed(range(nh)):
            for dc in reversed(range(nc)):
                if dh or dl or dc:
                    hh, ll, cc = lax.rem(h + dh, nh), lax.rem(l + dl, nl), lax.rem(c + dc, nc)
                    y_peers.append(((hh * nl + ll) * nc + cc, {"samp_2": hh, "feat_0": ll, "feat_1": cc}))
                    if not dh:
                        f_peers.append((ll * nc + cc, {"feat_0": ll, "feat_1": cc}))
    partner = {"samp_2": 1 - h}

    loads = [pltpu.make_async_copy(src, dst, local_sem.at[j]) for j, (src, dst) in enumerate(
        [(w_hbm, w_ref), (lam_hbm, lam_ref), (sv_hbm, sv_ref), (labels_hbm, labels_ref), (s_hbm, sp.at[x * nh + h]), (x_hbm, xv)])]
    loads[0].start()
    loads[4].start()
    barrier = pltpu.get_barrier_semaphore()
    for _, peer in zx_peers + y_peers:
        pl.semaphore_signal(barrier, inc=1, device_id=peer, device_id_type=pl.DeviceIdType.MESH)

    for j in (1, 2, 3, 5):
        loads[j].start()
    for q in range(nx):
        for zz in range(nz):
            pltpu.make_async_copy(x_hbm.at[:, pl.ds((zz * nx + q) * wide, wide)], xw.at[:, pl.ds((q * nz + zz) * wide, wide)],
                                  local_sem.at[6]).start()

    def copy(phase, src, dst, peer):
        return pltpu.make_async_remote_copy(
            src_ref=src, dst_ref=dst, send_sem=send_sem.at[phase], recv_sem=recv_sem.at[phase],
            device_id=peer, device_id_type=pl.DeviceIdType.MESH)

    sent = []

    def whole(phase, buffer, peer):
        arrived = copy(phase, buffer, buffer, peer)
        arrived.wait_recv()
        sent.append(arrived)

    lane = lax.broadcasted_iota(jnp.int32, (k, wide), 1)
    row = lax.broadcasted_iota(jnp.int32, (k, wide), 0)

    def pack(*columns):
        total = 0.0
        for place, column in enumerate(columns):
            total = total + jnp.where(lane == row + place * k, column, 0.0)
        return jnp.sum(total, axis=0, keepdims=True)

    def unpack(packed, place):
        return jnp.sum(jnp.where(lane == row + place * k, packed, 0.0), axis=1, keepdims=True)

    def lanes(value):
        return jnp.sum(value, axis=1, keepdims=True)

    def gather_start(i, value):
        ags[i] = value.astype(BF16)
        ag[i, zx] = value.astype(BF16)
        for dz in far_first(nz):
            for dx in far_first(nx):
                if dz or dx:
                    zz, xx = lax.rem(z + dz, nz), lax.rem(x + dx, nx)
                    pltpu.make_async_remote_copy(
                        src_ref=ags.at[i], dst_ref=ag.at[i, zx], send_sem=send_sem.at[2 + i], recv_sem=gather_sem.at[i, dz],
                        device_id={"samp_0": zz, "samp_1": xx}, device_id_type=pl.DeviceIdType.MESH).start()

    def arrived_group(phase, place, dz, group):
        pltpu.make_async_remote_copy(
            src_ref=group, dst_ref=group, send_sem=send_sem.at[phase], recv_sem=gather_sem.at[place, dz],
            device_id=zx_peers[0][1], device_id_type=pl.DeviceIdType.MESH).wait_recv()

    def rows_of(field, zz):
        start = pl.multiple_of(zz * (nx * wide), nx * wide)
        return lax.dot_general(field, xv[:, pl.ds(start, nx * wide)], BY_LANES, preferred_element_type=F32)

    def gather_rows(i):
        total = jnp.zeros((k, xv.shape[0]), F32)
        for dz in reversed(far_first(nz)):
            arrived_group(2 + i, i, dz, ag.at[i, pl.ds(0, nx if dz else nx - 1)])
            zz = lax.rem(z + (nz - dz), nz)
            total = total + rows_of(jnp.concatenate([ag[i, zz * nx + q] for q in range(nx)], axis=1), zz)
        sent.append(copy(2 + i, ag.at[i, pl.ds(0, nzx - 1)], ag.at[i, pl.ds(0, nzx - 1)], zx_peers[0][1]))
        return total

    def by_x(xx):
        return pl.ds(pl.multiple_of(xx * (nz * wide), nz * wide), nz * wide)

    def spread_start(i, value):
        cxs[i] = value.astype(BF16)
        for dx in far_first(nx):
            if dx:
                pltpu.make_async_remote_copy(
                    src_ref=cxs.at[i], dst_ref=cx.at[i, x], send_sem=send_sem.at[23 + i], recv_sem=x_sem.at[i, dx],
                    device_id={"samp_1": lax.rem(x + dx, nx)}, device_id_type=pl.DeviceIdType.MESH).start()
        for q in range(nz):
            cf[q] = value[:, q * wide:(q + 1) * wide]

    def spread_rows(i, total):
        for dx in reversed(far_first(nx)):
            xx = lax.rem(x + (nx - dx), nx)
            if dx:
                pltpu.make_async_remote_copy(
                    src_ref=cxs.at[i], dst_ref=cx.at[i, xx], send_sem=send_sem.at[23 + i], recv_sem=x_sem.at[i, dx],
                    device_id={"samp_1": xx}, device_id_type=pl.DeviceIdType.MESH).wait_recv()
                field = cx[i, xx]
            else:
                field = cxs[i]
            total = total + lax.dot_general(field, xw[:, by_x(xx)], BY_LANES, preferred_element_type=F32)
        sent.append(copy(23 + i, cx.at[i, pl.ds(0, nx - 1)], cx.at[i, pl.ds(0, nx - 1)], zx_peers[0][1]))
        return total

    def ring(step):
        ahead, behind = {"samp_0": lax.rem(z + 1, nz)}, {"samp_0": lax.rem(z + nz - 1, nz)}
        for way, peer in ((0, ahead), (1, behind)):
            if step > 1 and (way == 0 or step <= nz // 2):
                last = spz.at[0]
                pltpu.make_async_remote_copy(
                    src_ref=last, dst_ref=last, send_sem=send_sem.at[26], recv_sem=ring_sem.at[step - 2, way],
                    device_id=peer, device_id_type=pl.DeviceIdType.MESH).wait_recv()
            if step <= nz // 2 - way:
                offset = step - 1 if way else nz - (step - 1)
                block = lax.rem(z + offset, nz)
                pltpu.make_async_remote_copy(
                    src_ref=sp.at[pl.ds(x * nh, nh)] if step == 1 else spz.at[block], dst_ref=spz.at[block],
                    send_sem=send_sem.at[26], recv_sem=ring_sem.at[step - 1, way],
                    device_id=peer, device_id_type=pl.DeviceIdType.MESH).start()
        if step == 1:
            spz[z] = sp[pl.ds(x * nh, nh)]
        if step == nz // 2 + 1:
            sent.append(copy(26, spz.at[pl.ds(0, nz - 1)], spz.at[pl.ds(0, nz - 1)], ahead))

    def feat_sum(i, value):
        fts[i] = value
        ft[i, f] = value
        for _, peer in f_peers:
            copy(5 + i, fts.at[i], ft.at[i, f], peer).start()
        if i == 0:
            whole(27, sp.at[x * nh + 1 - h], partner)
            block = sp.at[pl.ds(x * nh, nh)]
            for dx in far_first(nx):
                if dx:
                    copy(1, block, block, {"samp_1": lax.rem(x + dx, nx)}).start()
            ring(1)
        whole(5 + i, ft.at[i, pl.ds(0, nf - 1)], f_peers[0][1])
        return jnp.sum(ft[i], axis=0)

    def feat_scalars_start(i, value):
        fss[i] = value
        fs[i, f] = value
        for _, peer in f_peers:
            copy(8 + i, fss.at[i], fs.at[i, f], peer).start()

    def feat_scalars(i):
        whole(8 + i, fs.at[i, pl.ds(0, nf - 1)], f_peers[0][1])
        return jnp.sum(fs[i], axis=0)

    def along_z(values, state):
        for dz in far_first(nz):
            zz = lax.rem(z + dz, nz)
            start = pl.multiple_of(zz * (nx * wide), nx * wide)
            part = lax.dot_general(values, xv[:, pl.ds(start, nx * wide)], BY_ROWS, preferred_element_type=F32)
            high = part.astype(BF16)
            rss[zz] = high
            rls[zz] = (part - high.astype(F32)).astype(BF16)
            if dz:
                copy(10, rss.at[zz], rs.at[z], {"samp_0": zz}).start()
        rs[z] = rss[z]
        for dz in far_first(nz):
            zz = lax.rem(z + dz, nz)
            if dz:
                copy(25, rls.at[zz], rl.at[z], {"samp_0": zz}).start()
        rl[z] = rls[z]
        whole(10, rs.at[pl.ds(0, nz - 1)], zx_peers[0][1])
        total = jnp.sum(rs[...].astype(F32), axis=0)
        ridge = (0.5 * lam) * state
        chunks = [total[:, q * wide:(q + 1) * wide] + ridge * jnp.where(x == q, 1.0, 0.0) for q in range(nx)]
        whole(1, sp.at[pl.ds(0, (nx - 1) * nh)], partner)
        project_start(0, chunks, sp[...].reshape(nx * nh * half, rank))
        ring(2)

        whole(25, rl.at[pl.ds(0, nz - 1)], zx_peers[0][1])
        low = jnp.sum(rl[...].astype(F32), axis=0)
        for q in range(nx):
            xs[q] = chunks[q] + low[:, q * wide:(q + 1) * wide]
        for dx in far_first(nx):
            xx = lax.rem(x + dx, nx)
            if dx:
                copy(21, xs.at[xx], xr.at[x], {"samp_1": xx}).start()
        xr[x] = xs[x]
        whole(21, xr.at[pl.ds(0, nx - 1)], {"samp_1": lax.rem(x + 1, nx)})
        vector, image, full = project_finish(0, jnp.sum(xr[...], axis=0), None)
        ring(5)
        spread_start(0, spread(full))
        return vector, vector + cf[z], image

    def along_x(values, state, scalars):
        for dx in far_first(nx):
            xx = lax.rem(x + dx, nx)
            part = lax.dot_general(values, xw[:, by_x(xx)], BY_ROWS, preferred_element_type=F32)
            wss[xx] = part.astype(BF16)
            if dx:
                copy(11, wss.at[xx], ws.at[x], {"samp_1": xx}).start()
        ws[x] = wss[x]
        whole(11, ws.at[pl.ds(0, nx - 1)], {"samp_1": lax.rem(x + 1, nx)})
        total = jnp.sum(ws[...].astype(F32), axis=0)
        ridge = (0.5 * lam) * state
        chunks = [total[:, q * wide:(q + 1) * wide] + ridge * jnp.where(z == q, 1.0, 0.0) for q in range(nz)]
        project_start(1, chunks, spz[...].reshape(nz * nh * half, rank))

        for q in range(nz):
            zs[q] = chunks[q]
        for dz in far_first(nz):
            zz = lax.rem(z + dz, nz)
            if dz:
                copy(22, zs.at[zz], zr.at[z], {"samp_0": zz}).start()
        zr[z] = zs[z]
        whole(22, zr.at[pl.ds(0, nz - 1)], zx_peers[0][1])
        vector, image, full = project_finish(1, jnp.sum(zr[...], axis=0), scalars)
        spread_start(1, spread(full))
        return vector, vector + cf[z], image, jnp.sum(full[:, rank:], axis=0, keepdims=True) * (1.0 / nf)

    def project_start(i, chunks, sketch):
        parts = lax.dot_general(split3(jnp.concatenate(chunks, axis=1)), sketch, BY_ROWS, preferred_element_type=F32)
        projected = parts[:k] + parts[k:2 * k] + parts[2 * k:]
        for q in range(k):
            prs[i, q] = projected[q:q + 1, :]
        for j, peer in y_peers:
            copy(14 + i, prs.at[i, j], pr.at[i, y], peer).start()
        pr[i, y] = prs[i, y]

    def spread(full):
        sketch = spz[...].reshape(nz * nh * half, rank)
        parts = lax.dot_general(split3(ratios * full[:, :rank]), sketch, BY_LANES, preferred_element_type=F32)
        return parts[:k] + parts[k:2 * k] + parts[2 * k:]

    def project_finish(i, part, scalars):
        yhs[i] = part
        copy(12 + i, yhs.at[i], yh.at[i], partner).start()

        whole(14 + i, pr.at[i, pl.ds(0, ny - 1)], y_peers[0][1])
        mine = jnp.sum(pr[i], axis=0)
        if scalars is not None:
            mine = jnp.concatenate([mine, scalars], axis=1)
        across = slice(0, mine.shape[1])
        pzs[i, :, across] = mine
        pz[i, zx, :, across] = mine
        for _, peer in zx_peers:
            copy(16 + i, pzs.at[i, :, across], pz.at[i, zx, :, across], peer).start()
        if i == 0:
            ring(3)

        whole(12 + i, yh.at[i], partner)
        vector = part + yh[i]
        gather_start(1 + i, vector)

        whole(16 + i, pz.at[i, pl.ds(0, nzx - 1), :, across], zx_peers[0][1])
        mine = jnp.sum(pz[i, :, :, across], axis=0)
        pas[i, :, across] = mine
        pa[i, y, :, across] = mine
        for _, peer in y_peers:
            copy(18 + i, pas.at[i, :, across], pa.at[i, y, :, across], peer).start()
        if i == 0:
            ring(4)
        image = gather_rows(1 + i)
        whole(18 + i, pa.at[i, pl.ds(0, ny - 1), :, across], y_peers[0][1])
        return vector, image, jnp.concatenate([pa[i, q, :, across] for q in range(k)], axis=0)

    loads[0].wait()
    wb[0, :, :half] = w_ref[...]
    wb[0, :, half:] = w_ref[...]
    pl.semaphore_wait(barrier, len(zx_peers) + len(y_peers))
    copy(0, wb.at[0], wb.at[1], partner).start()
    loads[4].wait()
    copy(27, sp.at[x * nh + h], sp.at[x * nh + h], partner).start()
    for load in loads[1:4]:
        load.wait()
    lam = jnp.sum(jnp.where(lax.broadcasted_iota(jnp.int32, (k, k), 0) == lax.broadcasted_iota(jnp.int32, (k, k), 1),
                            lam_ref[...], 0.0), axis=1, keepdims=True)
    values = sv_ref[...].reshape(1, rank)
    ratios = (jnp.min(values, axis=1, keepdims=True) + lam) / (values + lam) - 1.0
    whole(0, wb.at[1], partner)
    own = (lane // half) == h
    weights = jnp.where(own, wb[0], wb[1])
    gather_start(0, weights)
    loads[5].wait()
    pltpu.make_async_copy(x_hbm, xw, local_sem.at[6]).wait()

    logits = feat_sum(0, gather_rows(0))
    probability = jax.nn.sigmoid(logits)
    diag = probability * (1.0 - probability)
    miss = (probability - labels_ref[...].astype(F32)).astype(BF16)
    gradient, gradient_pre, image = along_z(miss, weights)
    residual, direction = -gradient, -gradient_pre
    feat_scalars_start(0, pack(0.5 * lanes(residual * direction), 0.5 * lam * lanes(direction * direction)))
    image = -feat_sum(1, spread_rows(0, image))
    scalars = feat_scalars(0) + pack(jnp.zeros((k, 1), F32), lanes(diag * image * image))
    hess_dir, hess_pre, image_pre, scalars = along_x((diag * image).astype(BF16), direction, scalars)
    res_dot, curvature = unpack(scalars, 0), unpack(scalars, 1)
    step = res_dot / curvature
    residual = residual - step * hess_dir
    precond = direction - step * hess_pre
    feat_scalars_start(1, pack(0.5 * lanes(residual * precond), 0.5 * lam * lanes(precond * precond),
                               0.5 * lam * lanes(precond * direction)))
    image_pre = image - step * feat_sum(2, spread_rows(1, image_pre))
    mine = feat_scalars(1) + pack(jnp.zeros((k, 1), F32), lanes(diag * image_pre * image_pre),
                                  lanes(diag * image_pre * image))
    kzs[...] = mine
    kz[zx * nh + h] = mine
    for dh in reversed(range(nh)):
        for dz in far_first(nz):
            for dx in far_first(nx):
                if dh or dz or dx:
                    peer = {"samp_0": lax.rem(z + dz, nz), "samp_1": lax.rem(x + dx, nx), "samp_2": lax.rem(h + dh, nh)}
                    copy(20, kzs, kz.at[zx * nh + h], peer).start()
    whole(20, kz.at[pl.ds(0, nzx * nh - 1)], partner)
    scalars = jnp.sum(kz[...], axis=0)
    new_dot, pre_pre, pre_dir = (unpack(scalars, place) for place in range(3))
    beta = new_dot / res_dot
    last = new_dot / (pre_pre + 2.0 * beta * pre_dir + beta * beta * curvature)
    update = step * direction + last * (precond + beta * direction)
    update = jnp.where(h == 0, update, pltpu.roll(update, half, 1))
    out_ref[...] = w_ref[...] + update[:, :half]
    for arrived in sent:
        arrived.wait_send()


def shards(sizes, design_matrix, labels, weights, lambdas, sketch, sketch_values):
    nz, nx, nh, nl, nc = sizes
    nzx, nf, ny = nz * nx, nl * nc, nh * nl * nc
    k, half = weights.shape
    wide = 2 * half
    rank = sketch.shape[1]
    vmem = pl.BlockSpec(memory_space=pltpu.VMEM)
    anywhere = pl.BlockSpec(memory_space=pl.ANY)
    dma = pltpu.SemaphoreType.DMA
    return pl.pallas_call(
        functools.partial(kernel, sizes),
        name="step",
        out_shape=jax.ShapeDtypeStruct((k, half), F32),
        in_specs=[anywhere] * 6,
        out_specs=vmem,
        scratch_shapes=[
            pltpu.VMEM(design_matrix.shape, BF16), pltpu.VMEM(design_matrix.shape, BF16),
            pltpu.VMEM((1, design_matrix.shape[0]), jnp.int32), pltpu.VMEM((k, half), F32), pltpu.VMEM((1, k), F32),
            pltpu.VMEM((rank,), F32),
            pltpu.VMEM((nx * nh, half, rank), BF16),
            pltpu.VMEM((2, k, wide), F32),
            pltpu.VMEM((3, nzx, k, wide), BF16), pltpu.VMEM((3, k, wide), BF16),
            pltpu.VMEM((3, nf, k, wide), F32), pltpu.VMEM((3, k, wide), F32),
            pltpu.VMEM((2, nf, 1, wide), F32), pltpu.VMEM((2, 1, wide), F32),
            pltpu.VMEM((nz, k, nx * wide), BF16), pltpu.VMEM((nz, k, nx * wide), BF16),
            pltpu.VMEM((nz, k, nx * wide), BF16), pltpu.VMEM((nz, k, nx * wide), BF16),
            pltpu.VMEM((nx, k, nz * wide), BF16), pltpu.VMEM((nx, k, nz * wide), BF16),
            pltpu.VMEM((nx, k, wide), F32), pltpu.VMEM((nx, k, wide), F32),
            pltpu.VMEM((nz, k, wide), F32), pltpu.VMEM((nz, k, wide), F32),
            pltpu.VMEM((nz, nh, half, rank), BF16),
            pltpu.VMEM((2, k, wide), F32), pltpu.VMEM((2, k, wide), F32),
            pltpu.VMEM((2, ny, 1, rank), F32), pltpu.VMEM((2, ny, 1, rank), F32),
            pltpu.VMEM((2, nzx, 1, rank + wide), F32), pltpu.VMEM((2, 1, rank + wide), F32),
            pltpu.VMEM((2, ny, 1, rank + wide), F32), pltpu.VMEM((2, 1, rank + wide), F32),
            pltpu.VMEM((2, nx, k, nz * wide), BF16), pltpu.VMEM((2, k, nz * wide), BF16),
            pltpu.VMEM((nz, k, wide), F32),
            pltpu.VMEM((nzx * nh, 1, wide), F32), pltpu.VMEM((1, wide), F32),
            dma((7,)), dma((28,)), dma((28,)), dma((3, nz)), dma((nz // 2, 2)), dma((2, nx)),
        ],
        compiler_params=pltpu.CompilerParams(collective_id=0, has_side_effects=True),
    )(design_matrix, labels.reshape(1, -1), weights, lambdas.reshape(1, -1), sketch, sketch_values)


def solution(mesh):
    sizes = (8, 4, 2, 4, 2)
    finer = Mesh(mesh.devices.reshape(sizes), SAMP + FEAT)
    placed = (P(SAMP, FEAT), P(SAMP), P(None, FEAT_SAMP), P(), P(FEAT_SAMP, None), P())
    return jax.shard_map(
        functools.partial(shards, sizes), mesh=finer, in_specs=placed, out_specs=P(None, FEAT_SAMP), check_vma=False
    )
```

```python
import functools

import jax
import jax.numpy as jnp
from jax import lax
from jax.experimental import pallas as pl
from jax.experimental.pallas import tpu as pltpu
from jax.sharding import Mesh
from jax.sharding import PartitionSpec as P

SAMP = ("samp_0", "samp_1", "samp_2")
FEAT = ("feat_0", "feat_1")
FEAT_SAMP = FEAT + SAMP
F32, BF16 = jnp.float32, jnp.bfloat16
BY_LANES = (((1,), (1,)), ((), ()))
BY_ROWS = (((1,), (0,)), ((), ()))


def far_first(n):
    return sorted(range(n), key=lambda d: -min(d, n - d))


def split3(value):
    high = value.astype(BF16)
    rest = value - high.astype(F32)
    mid = rest.astype(BF16)
    low = (rest - mid.astype(F32)).astype(BF16)
    return jnp.concatenate([high, mid, low], axis=0)


def kernel(sizes, x_hbm, labels_hbm, w_hbm, lam_hbm, s_hbm, sv_hbm, out_ref,
           xv, xw, labels_ref, w_ref, lam_ref, sv_ref, sp, wb, ag, ags, ft, fts, fs, fss, rs, rss, rl, rls, ws, wss, xr, xs, zr, zs, spz, yh, yhs,
           pr, prs, pz, pzs, pa, pas, cx, cxs, cf, kz, kzs, local_sem, send_sem, recv_sem, gather_sem, ring_sem, x_sem):
    nz, nx, nh, nl, nc = sizes
    nzx, nf, ny = nz * nx, nl * nc, nh * nl * nc
    k, half = w_ref.shape
    wide = 2 * half
    rank = s_hbm.shape[1]
    z, x, h, l, c = (lax.axis_index(name) for name in SAMP + FEAT)
    zx, f, y = z * nx + x, l * nc + c, (h * nl + l) * nc + c

    zx_peers = []
    for dz in far_first(nz):
        for dx in far_first(nx):
            if dz or dx:
                zz, xx = lax.rem(z + dz, nz), lax.rem(x + dx, nx)
                zx_peers.append((zz * nx + xx, {"samp_0": zz, "samp_1": xx}))
    y_peers, f_peers = [], []
    for dl in far_first(nl):
        for dh in reversed(range(nh)):
            for dc in reversed(range(nc)):
                if dh or dl or dc:
                    hh, ll, cc = lax.rem(h + dh, nh), lax.rem(l + dl, nl), lax.rem(c + dc, nc)
                    y_peers.append(((hh * nl + ll) * nc + cc, {"samp_2": hh, "feat_0": ll, "feat_1": cc}))
                    if not dh:
                        f_peers.append((ll * nc + cc, {"feat_0": ll, "feat_1": cc}))
    partner = {"samp_2": 1 - h}

    loads = [pltpu.make_async_copy(src, dst, local_sem.at[j]) for j, (src, dst) in enumerate(
        [(w_hbm, w_ref), (lam_hbm, lam_ref), (sv_hbm, sv_ref), (labels_hbm, labels_ref), (s_hbm, sp.at[x * nh + h]), (x_hbm, xv)])]
    loads[0].start()
    loads[4].start()
    barrier = pltpu.get_barrier_semaphore()
    for _, peer in zx_peers + y_peers:
        pl.semaphore_signal(barrier, inc=1, device_id=peer, device_id_type=pl.DeviceIdType.MESH)

    for j in (1, 2, 3, 5):
        loads[j].start()
    for q in range(nx):
        for zz in range(nz):
            pltpu.make_async_copy(x_hbm.at[:, pl.ds((zz * nx + q) * wide, wide)], xw.at[:, pl.ds((q * nz + zz) * wide, wide)],
                                  local_sem.at[6]).start()

    def copy(phase, src, dst, peer):
        return pltpu.make_async_remote_copy(
            src_ref=src, dst_ref=dst, send_sem=send_sem.at[phase], recv_sem=recv_sem.at[phase],
            device_id=peer, device_id_type=pl.DeviceIdType.MESH)

    sent = []

    def whole(phase, buffer, peer):
        arrived = copy(phase, buffer, buffer, peer)
        arrived.wait_recv()
        sent.append(arrived)

    lane = lax.broadcasted_iota(jnp.int32, (k, wide), 1)
    row = lax.broadcasted_iota(jnp.int32, (k, wide), 0)

    def pack(*columns):
        total = 0.0
        for place, column in enumerate(columns):
            total = total + jnp.where(lane == row + place * k, column, 0.0)
        return jnp.sum(total, axis=0, keepdims=True)

    def unpack(packed, place):
        return jnp.sum(jnp.where(lane == row + place * k, packed, 0.0), axis=1, keepdims=True)

    def lanes(value):
        return jnp.sum(value, axis=1, keepdims=True)

    def gather_start(i, value):
        ags[i] = value.astype(BF16)
        ag[i, zx] = value.astype(BF16)
        for dz in far_first(nz):
            for dx in far_first(nx):
                if dz or dx:
                    zz, xx = lax.rem(z + dz, nz), lax.rem(x + dx, nx)
                    pltpu.make_async_remote_copy(
                        src_ref=ags.at[i], dst_ref=ag.at[i, zx], send_sem=send_sem.at[2 + i], recv_sem=gather_sem.at[i, dz],
                        device_id={"samp_0": zz, "samp_1": xx}, device_id_type=pl.DeviceIdType.MESH).start()

    def arrived_group(phase, place, dz, group):
        pltpu.make_async_remote_copy(
            src_ref=group, dst_ref=group, send_sem=send_sem.at[phase], recv_sem=gather_sem.at[place, dz],
            device_id=zx_peers[0][1], device_id_type=pl.DeviceIdType.MESH).wait_recv()

    def rows_of(field, zz):
        start = pl.multiple_of(zz * (nx * wide), nx * wide)
        return lax.dot_general(field, xv[:, pl.ds(start, nx * wide)], BY_LANES, preferred_element_type=F32)

    def gather_rows(i):
        total = jnp.zeros((k, xv.shape[0]), F32)
        for dz in reversed(far_first(nz)):
            arrived_group(2 + i, i, dz, ag.at[i, pl.ds(0, nx if dz else nx - 1)])
            zz = lax.rem(z + (nz - dz), nz)
            total = total + rows_of(jnp.concatenate([ag[i, zz * nx + q] for q in range(nx)], axis=1), zz)
        sent.append(copy(2 + i, ag.at[i, pl.ds(0, nzx - 1)], ag.at[i, pl.ds(0, nzx - 1)], zx_peers[0][1]))
        return total

    def by_x(xx):
        return pl.ds(pl.multiple_of(xx * (nz * wide), nz * wide), nz * wide)

    def spread_start(i, value):
        cxs[i] = value.astype(BF16)
        for dx in far_first(nx):
            if dx:
                pltpu.make_async_remote_copy(
                    src_ref=cxs.at[i], dst_ref=cx.at[i, x], send_sem=send_sem.at[23 + i], recv_sem=x_sem.at[i, dx],
                    device_id={"samp_1": lax.rem(x + dx, nx)}, device_id_type=pl.DeviceIdType.MESH).start()
        for q in range(nz):
            cf[q] = value[:, q * wide:(q + 1) * wide]

    def spread_rows(i, total):
        for dx in reversed(far_first(nx)):
            xx = lax.rem(x + (nx - dx), nx)
            if dx:
                pltpu.make_async_remote_copy(
                    src_ref=cxs.at[i], dst_ref=cx.at[i, xx], send_sem=send_sem.at[23 + i], recv_sem=x_sem.at[i, dx],
                    device_id={"samp_1": xx}, device_id_type=pl.DeviceIdType.MESH).wait_recv()
                field = cx[i, xx]
            else:
                field = cxs[i]
            total = total + lax.dot_general(field, xw[:, by_x(xx)], BY_LANES, preferred_element_type=F32)
        sent.append(copy(23 + i, cx.at[i, pl.ds(0, nx - 1)], cx.at[i, pl.ds(0, nx - 1)], zx_peers[0][1]))
        return total

    def ring(step):
        ahead, behind = {"samp_0": lax.rem(z + 1, nz)}, {"samp_0": lax.rem(z + nz - 1, nz)}
        for way, peer in ((0, ahead), (1, behind)):
            if step > 1 and (way == 0 or step <= nz // 2):
                last = spz.at[0]
                pltpu.make_async_remote_copy(
                    src_ref=last, dst_ref=last, send_sem=send_sem.at[26], recv_sem=ring_sem.at[step - 2, way],
                    device_id=peer, device_id_type=pl.DeviceIdType.MESH).wait_recv()
            if step <= nz // 2 - way:
                offset = step - 1 if way else nz - (step - 1)
                block = lax.rem(z + offset, nz)
                pltpu.make_async_remote_copy(
                    src_ref=sp.at[pl.ds(x * nh, nh)] if step == 1 else spz.at[block], dst_ref=spz.at[block],
                    send_sem=send_sem.at[26], recv_sem=ring_sem.at[step - 1, way],
                    device_id=peer, device_id_type=pl.DeviceIdType.MESH).start()
        if step == 1:
            spz[z] = sp[pl.ds(x * nh, nh)]
        if step == nz // 2 + 1:
            sent.append(copy(26, spz.at[pl.ds(0, nz - 1)], spz.at[pl.ds(0, nz - 1)], ahead))

    def feat_sum(i, value):
        fts[i] = value
        ft[i, f] = value
        for _, peer in f_peers:
            copy(5 + i, fts.at[i], ft.at[i, f], peer).start()
        if i == 0:
            whole(27, sp.at[x * nh + 1 - h], partner)
            block = sp.at[pl.ds(x * nh, nh)]
            for dx in far_first(nx):
                if dx:
                    copy(1, block, block, {"samp_1": lax.rem(x + dx, nx)}).start()
            ring(1)
        whole(5 + i, ft.at[i, pl.ds(0, nf - 1)], f_peers[0][1])
        return jnp.sum(ft[i], axis=0)

    def feat_scalars_start(i, value):
        fss[i] = value
        fs[i, f] = value
        for _, peer in f_peers:
            copy(8 + i, fss.at[i], fs.at[i, f], peer).start()

    def feat_scalars(i):
        whole(8 + i, fs.at[i, pl.ds(0, nf - 1)], f_peers[0][1])
        return jnp.sum(fs[i], axis=0)

    def along_z(values, state):
        for dz in far_first(nz):
            zz = lax.rem(z + dz, nz)
            start = pl.multiple_of(zz * (nx * wide), nx * wide)
            part = lax.dot_general(values, xv[:, pl.ds(start, nx * wide)], BY_ROWS, preferred_element_type=F32)
            high = part.astype(BF16)
            rss[zz] = high
            rls[zz] = (part - high.astype(F32)).astype(BF16)
            if dz:
                copy(10, rss.at[zz], rs.at[z], {"samp_0": zz}).start()
        rs[z] = rss[z]
        for dz in far_first(nz):
            zz = lax.rem(z + dz, nz)
            if dz:
                copy(25, rls.at[zz], rl.at[z], {"samp_0": zz}).start()
        rl[z] = rls[z]
        whole(10, rs.at[pl.ds(0, nz - 1)], zx_peers[0][1])
        total = jnp.sum(rs[...].astype(F32), axis=0)
        ridge = (0.5 * lam) * state
        chunks = [total[:, q * wide:(q + 1) * wide] + ridge * jnp.where(x == q, 1.0, 0.0) for q in range(nx)]
        whole(1, sp.at[pl.ds(0, (nx - 1) * nh)], partner)
        project_start(0, chunks, sp[...].reshape(nx * nh * half, rank))
        ring(2)

        whole(25, rl.at[pl.ds(0, nz - 1)], zx_peers[0][1])
        low = jnp.sum(rl[...].astype(F32), axis=0)
        for q in range(nx):
            xs[q] = chunks[q] + low[:, q * wide:(q + 1) * wide]
        for dx in far_first(nx):
            xx = lax.rem(x + dx, nx)
            if dx:
                copy(21, xs.at[xx], xr.at[x], {"samp_1": xx}).start()
        xr[x] = xs[x]
        whole(21, xr.at[pl.ds(0, nx - 1)], {"samp_1": lax.rem(x + 1, nx)})
        vector, image, full = project_finish(0, jnp.sum(xr[...], axis=0), None)
        ring(5)
        spread_start(0, spread(full))
        return vector, vector + cf[z], image

    def along_x(values, state, scalars):
        for dx in far_first(nx):
            xx = lax.rem(x + dx, nx)
            part = lax.dot_general(values, xw[:, by_x(xx)], BY_ROWS, preferred_element_type=F32)
            wss[xx] = part.astype(BF16)
            if dx:
                copy(11, wss.at[xx], ws.at[x], {"samp_1": xx}).start()
        ws[x] = wss[x]
        whole(11, ws.at[pl.ds(0, nx - 1)], {"samp_1": lax.rem(x + 1, nx)})
        total = jnp.sum(ws[...].astype(F32), axis=0)
        ridge = (0.5 * lam) * state
        chunks = [total[:, q * wide:(q + 1) * wide] + ridge * jnp.where(z == q, 1.0, 0.0) for q in range(nz)]
        project_start(1, chunks, spz[...].reshape(nz * nh * half, rank))

        for q in range(nz):
            zs[q] = chunks[q]
        for dz in far_first(nz):
            zz = lax.rem(z + dz, nz)
            if dz:
                copy(22, zs.at[zz], zr.at[z], {"samp_0": zz}).start()
        zr[z] = zs[z]
        whole(22, zr.at[pl.ds(0, nz - 1)], zx_peers[0][1])
        vector, image, full = project_finish(1, jnp.sum(zr[...], axis=0), scalars)
        spread_start(1, spread(full))
        return vector, vector + cf[z], image, jnp.sum(full[:, rank:], axis=0, keepdims=True) * (1.0 / nf)

    def project_start(i, chunks, sketch):
        parts = lax.dot_general(split3(jnp.concatenate(chunks, axis=1)), sketch, BY_ROWS, preferred_element_type=F32)
        projected = parts[:k] + parts[k:2 * k] + parts[2 * k:]
        for q in range(k):
            prs[i, q] = projected[q:q + 1, :]
        for j, peer in y_peers:
            copy(14 + i, prs.at[i, j], pr.at[i, y], peer).start()
        pr[i, y] = prs[i, y]

    def spread(full):
        sketch = spz[...].reshape(nz * nh * half, rank)
        parts = lax.dot_general(split3(ratios * full[:, :rank]), sketch, BY_LANES, preferred_element_type=F32)
        return parts[:k] + parts[k:2 * k] + parts[2 * k:]

    def project_finish(i, part, scalars):
        yhs[i] = part
        copy(12 + i, yhs.at[i], yh.at[i], partner).start()

        whole(14 + i, pr.at[i, pl.ds(0, ny - 1)], y_peers[0][1])
        mine = jnp.sum(pr[i], axis=0)
        if scalars is not None:
            mine = jnp.concatenate([mine, scalars], axis=1)
        across = slice(0, mine.shape[1])
        pzs[i, :, across] = mine
        pz[i, zx, :, across] = mine
        for _, peer in zx_peers:
            copy(16 + i, pzs.at[i, :, across], pz.at[i, zx, :, across], peer).start()
        if i == 0:
            ring(3)

        whole(12 + i, yh.at[i], partner)
        vector = part + yh[i]
        gather_start(1 + i, vector)

        whole(16 + i, pz.at[i, pl.ds(0, nzx - 1), :, across], zx_peers[0][1])
        mine = jnp.sum(pz[i, :, :, across], axis=0)
        pas[i, :, across] = mine
        pa[i, y, :, across] = mine
        for _, peer in y_peers:
            copy(18 + i, pas.at[i, :, across], pa.at[i, y, :, across], peer).start()
        if i == 0:
            ring(4)
        image = gather_rows(1 + i)
        whole(18 + i, pa.at[i, pl.ds(0, ny - 1), :, across], y_peers[0][1])
        return vector, image, jnp.concatenate([pa[i, q, :, across] for q in range(k)], axis=0)

    loads[0].wait()
    wb[0, :, :half] = w_ref[...]
    wb[0, :, half:] = w_ref[...]
    pl.semaphore_wait(barrier, len(zx_peers) + len(y_peers))
    copy(0, wb.at[0], wb.at[1], partner).start()
    loads[4].wait()
    copy(27, sp.at[x * nh + h], sp.at[x * nh + h], partner).start()
    for load in loads[1:4]:
        load.wait()
    lam = jnp.sum(jnp.where(lax.broadcasted_iota(jnp.int32, (k, k), 0) == lax.broadcasted_iota(jnp.int32, (k, k), 1),
                            lam_ref[...], 0.0), axis=1, keepdims=True)
    values = sv_ref[...].reshape(1, rank)
    ratios = (jnp.min(values, axis=1, keepdims=True) + lam) / (values + lam) - 1.0
    whole(0, wb.at[1], partner)
    own = (lane // half) == h
    weights = jnp.where(own, wb[0], wb[1])
    gather_start(0, weights)
    loads[5].wait()
    pltpu.make_async_copy(x_hbm, xw, local_sem.at[6]).wait()

    logits = feat_sum(0, gather_rows(0))
    probability = jax.nn.sigmoid(logits)
    diag = probability * (1.0 - probability)
    miss = (probability - labels_ref[...].astype(F32)).astype(BF16)
    gradient, gradient_pre, image = along_z(miss, weights)
    residual, direction = -gradient, -gradient_pre
    feat_scalars_start(0, pack(0.5 * lanes(residual * direction), 0.5 * lam * lanes(direction * direction)))
    image = -feat_sum(1, spread_rows(0, image))
    scalars = feat_scalars(0) + pack(jnp.zeros((k, 1), F32), lanes(diag * image * image))
    hess_dir, hess_pre, image_pre, scalars = along_x((diag * image).astype(BF16), direction, scalars)
    res_dot, curvature = unpack(scalars, 0), unpack(scalars, 1)
    step = res_dot / curvature
    residual = residual - step * hess_dir
    precond = direction - step * hess_pre
    feat_scalars_start(1, pack(0.5 * lanes(residual * precond), 0.5 * lam * lanes(precond * precond),
                               0.5 * lam * lanes(precond * direction)))
    image_pre = image - step * feat_sum(2, spread_rows(1, image_pre))
    mine = feat_scalars(1) + pack(jnp.zeros((k, 1), F32), lanes(diag * image_pre * image_pre),
                                  lanes(diag * image_pre * image))
    kzs[...] = mine
    kz[zx * nh + h] = mine
    for dh in reversed(range(nh)):
        for dz in far_first(nz):
            for dx in far_first(nx):
                if dh or dz or dx:
                    peer = {"samp_0": lax.rem(z + dz, nz), "samp_1": lax.rem(x + dx, nx), "samp_2": lax.rem(h + dh, nh)}
                    copy(20, kzs, kz.at[zx * nh + h], peer).start()
    whole(20, kz.at[pl.ds(0, nzx * nh - 1)], partner)
    scalars = jnp.sum(kz[...], axis=0)
    new_dot, pre_pre, pre_dir = (unpack(scalars, place) for place in range(3))
    beta = new_dot / res_dot
    last = new_dot / (pre_pre + 2.0 * beta * pre_dir + beta * beta * curvature)
    update = step * direction + last * (precond + beta * direction)
    update = jnp.where(h == 0, update, pltpu.roll(update, half, 1))
    out_ref[...] = w_ref[...] + update[:, :half]
    for arrived in sent:
        arrived.wait_send()


def shards(sizes, design_matrix, labels, weights, lambdas, sketch, sketch_values):
    nz, nx, nh, nl, nc = sizes
    nzx, nf, ny = nz * nx, nl * nc, nh * nl * nc
    k, half = weights.shape
    wide = 2 * half
    rank = sketch.shape[1]
    vmem = pl.BlockSpec(memory_space=pltpu.VMEM)
    anywhere = pl.BlockSpec(memory_space=pl.ANY)
    dma = pltpu.SemaphoreType.DMA
    return pl.pallas_call(
        functools.partial(kernel, sizes),
        name="step",
        out_shape=jax.ShapeDtypeStruct((k, half), F32),
        in_specs=[anywhere] * 6,
        out_specs=vmem,
        scratch_shapes=[
            pltpu.VMEM(design_matrix.shape, BF16), pltpu.VMEM(design_matrix.shape, BF16),
            pltpu.VMEM((1, design_matrix.shape[0]), jnp.int32), pltpu.VMEM((k, half), F32), pltpu.VMEM((1, k), F32),
            pltpu.VMEM((rank,), F32),
            pltpu.VMEM((nx * nh, half, rank), BF16),
            pltpu.VMEM((2, k, wide), F32),
            pltpu.VMEM((3, nzx, k, wide), BF16), pltpu.VMEM((3, k, wide), BF16),
            pltpu.VMEM((3, nf, k, wide), F32), pltpu.VMEM((3, k, wide), F32),
            pltpu.VMEM((2, nf, 1, wide), F32), pltpu.VMEM((2, 1, wide), F32),
            pltpu.VMEM((nz, k, nx * wide), BF16), pltpu.VMEM((nz, k, nx * wide), BF16),
            pltpu.VMEM((nz, k, nx * wide), BF16), pltpu.VMEM((nz, k, nx * wide), BF16),
            pltpu.VMEM((nx, k, nz * wide), BF16), pltpu.VMEM((nx, k, nz * wide), BF16),
            pltpu.VMEM((nx, k, wide), F32), pltpu.VMEM((nx, k, wide), F32),
            pltpu.VMEM((nz, k, wide), F32), pltpu.VMEM((nz, k, wide), F32),
            pltpu.VMEM((nz, nh, half, rank), BF16),
            pltpu.VMEM((2, k, wide), F32), pltpu.VMEM((2, k, wide), F32),
            pltpu.VMEM((2, ny, 1, rank), F32), pltpu.VMEM((2, ny, 1, rank), F32),
            pltpu.VMEM((2, nzx, 1, rank + wide), F32), pltpu.VMEM((2, 1, rank + wide), F32),
            pltpu.VMEM((2, ny, 1, rank + wide), F32), pltpu.VMEM((2, 1, rank + wide), F32),
            pltpu.VMEM((2, nx, k, nz * wide), BF16), pltpu.VMEM((2, k, nz * wide), BF16),
            pltpu.VMEM((nz, k, wide), F32),
            pltpu.VMEM((nzx * nh, 1, wide), F32), pltpu.VMEM((1, wide), F32),
            dma((7,)), dma((28,)), dma((28,)), dma((3, nz)), dma((nz // 2, 2)), dma((2, nx)),
        ],
        compiler_params=pltpu.CompilerParams(collective_id=0, has_side_effects=True, vmem_limit_bytes=32 << 20),
    )(*(pltpu.with_memory_space_constraint(operand, pltpu.HBM) for operand in (
        design_matrix, labels.reshape(1, -1), weights, lambdas.reshape(1, -1), sketch, sketch_values)))


def solution(mesh):
    sizes = (8, 4, 2, 4, 2)
    finer = Mesh(mesh.devices.reshape(sizes), SAMP + FEAT)
    placed = (P(SAMP, FEAT), P(SAMP), P(None, FEAT_SAMP), P(), P(FEAT_SAMP, None), P())
    return jax.shard_map(
        functools.partial(shards, sizes), mesh=finer, in_specs=placed, out_specs=P(None, FEAT_SAMP), check_vma=False
    )
```

```python
import functools

import jax
import jax.numpy as jnp
from jax import lax
from jax.experimental import pallas as pl
from jax.experimental.pallas import tpu as pltpu
from jax.sharding import Mesh
from jax.sharding import PartitionSpec as P

SAMP = ("samp_0", "samp_1", "samp_2")
FEAT = ("feat_0", "feat_1")
FEAT_SAMP = FEAT + SAMP
F32, BF16 = jnp.float32, jnp.bfloat16
BY_LANES = (((1,), (1,)), ((), ()))
BY_ROWS = (((1,), (0,)), ((), ()))


def far_first(n):
    return sorted(range(n), key=lambda d: -min(d, n - d))


def split3(value):
    high = value.astype(BF16)
    rest = value - high.astype(F32)
    mid = rest.astype(BF16)
    low = (rest - mid.astype(F32)).astype(BF16)
    return jnp.concatenate([high, mid, low], axis=0)


def kernel(sizes, x_hbm, labels_hbm, w_hbm, lam_hbm, s_hbm, sv_hbm, out_ref,
           xv, xw, labels_ref, w_ref, lam_ref, sv_ref, sp, wb, ag, ags, ft, fts, fs, fss, rs, rss, rl, rls, ws, wss, xr, xs, zr, zs, spz, yh, yhs,
           pr, prs, pz, pzs, pa, pas, cx, cxs, cf, kz, kzs, local_sem, send_sem, recv_sem, gather_sem, ring_sem, x_sem):
    nz, nx, nh, nl, nc = sizes
    nzx, nf, ny = nz * nx, nl * nc, nh * nl * nc
    k, half = w_ref.shape
    wide = 2 * half
    rank = s_hbm.shape[1]
    z, x, h, l, c = (lax.axis_index(name) for name in SAMP + FEAT)
    zx, f, y = z * nx + x, l * nc + c, (h * nl + l) * nc + c

    zx_peers = []
    for dz in far_first(nz):
        for dx in far_first(nx):
            if dz or dx:
                zz, xx = lax.rem(z + dz, nz), lax.rem(x + dx, nx)
                zx_peers.append((zz * nx + xx, {"samp_0": zz, "samp_1": xx}))
    y_peers, f_peers = [], []
    for dl in far_first(nl):
        for dh in reversed(range(nh)):
            for dc in reversed(range(nc)):
                if dh or dl or dc:
                    hh, ll, cc = lax.rem(h + dh, nh), lax.rem(l + dl, nl), lax.rem(c + dc, nc)
                    y_peers.append(((hh * nl + ll) * nc + cc, {"samp_2": hh, "feat_0": ll, "feat_1": cc}))
                    if not dh:
                        f_peers.append((ll * nc + cc, {"feat_0": ll, "feat_1": cc}))
    partner = {"samp_2": 1 - h}

    loads = [pltpu.make_async_copy(src, dst, local_sem.at[j]) for j, (src, dst) in enumerate(
        [(w_hbm, w_ref), (lam_hbm, lam_ref), (sv_hbm, sv_ref), (labels_hbm, labels_ref), (s_hbm, sp.at[x * nh + h]), (x_hbm, xv)])]
    loads[0].start()
    loads[4].start()
    barrier = pltpu.get_barrier_semaphore()
    for _, peer in zx_peers + y_peers:
        pl.semaphore_signal(barrier, inc=1, device_id=peer, device_id_type=pl.DeviceIdType.MESH)

    for j in (1, 2, 3, 5):
        loads[j].start()
    for q in range(nx):
        for zz in range(nz):
            pltpu.make_async_copy(x_hbm.at[:, pl.ds((zz * nx + q) * wide, wide)], xw.at[:, pl.ds((q * nz + zz) * wide, wide)],
                                  local_sem.at[6]).start()

    def copy(phase, src, dst, peer):
        return pltpu.make_async_remote_copy(
            src_ref=src, dst_ref=dst, send_sem=send_sem.at[phase], recv_sem=recv_sem.at[phase],
            device_id=peer, device_id_type=pl.DeviceIdType.MESH)

    sent = []

    def whole(phase, buffer, peer):
        arrived = copy(phase, buffer, buffer, peer)
        arrived.wait_recv()
        sent.append(arrived)

    lane = lax.broadcasted_iota(jnp.int32, (k, wide), 1)
    row = lax.broadcasted_iota(jnp.int32, (k, wide), 0)

    def pack(*columns):
        total = 0.0
        for place, column in enumerate(columns):
            total = total + jnp.where(lane == row + place * k, column, 0.0)
        return jnp.sum(total, axis=0, keepdims=True)

    def unpack(packed, place):
        return jnp.sum(jnp.where(lane == row + place * k, packed, 0.0), axis=1, keepdims=True)

    def lanes(value):
        return jnp.sum(value, axis=1, keepdims=True)

    def gather_start(i, value):
        ags[i] = value.astype(BF16)
        ag[i, zx] = value.astype(BF16)
        for dz in far_first(nz):
            for dx in far_first(nx):
                if dz or dx:
                    zz, xx = lax.rem(z + dz, nz), lax.rem(x + dx, nx)
                    pltpu.make_async_remote_copy(
                        src_ref=ags.at[i], dst_ref=ag.at[i, zx], send_sem=send_sem.at[2 + i], recv_sem=gather_sem.at[i, dz],
                        device_id={"samp_0": zz, "samp_1": xx}, device_id_type=pl.DeviceIdType.MESH).start()

    def arrived_group(phase, place, dz, group):
        pltpu.make_async_remote_copy(
            src_ref=group, dst_ref=group, send_sem=send_sem.at[phase], recv_sem=gather_sem.at[place, dz],
            device_id=zx_peers[0][1], device_id_type=pl.DeviceIdType.MESH).wait_recv()

    def rows_of(field, zz):
        start = pl.multiple_of(zz * (nx * wide), nx * wide)
        return lax.dot_general(field, xv[:, pl.ds(start, nx * wide)], BY_LANES, preferred_element_type=F32)

    def gather_rows(i):
        total = jnp.zeros((k, xv.shape[0]), F32)
        for dz in reversed(far_first(nz)):
            arrived_group(2 + i, i, dz, ag.at[i, pl.ds(0, nx if dz else nx - 1)])
            zz = lax.rem(z + (nz - dz), nz)
            total = total + rows_of(jnp.concatenate([ag[i, zz * nx + q] for q in range(nx)], axis=1), zz)
        sent.append(copy(2 + i, ag.at[i, pl.ds(0, nzx - 1)], ag.at[i, pl.ds(0, nzx - 1)], zx_peers[0][1]))
        return total

    def by_x(xx):
        return pl.ds(pl.multiple_of(xx * (nz * wide), nz * wide), nz * wide)

    def spread_start(i, value):
        cxs[i] = value.astype(BF16)
        for dx in far_first(nx):
            if dx:
                pltpu.make_async_remote_copy(
                    src_ref=cxs.at[i], dst_ref=cx.at[i, x], send_sem=send_sem.at[23 + i], recv_sem=x_sem.at[i, dx],
                    device_id={"samp_1": lax.rem(x + dx, nx)}, device_id_type=pl.DeviceIdType.MESH).start()
        for q in range(nz):
            cf[q] = value[:, q * wide:(q + 1) * wide]

    def spread_rows(i, total):
        for dx in reversed(far_first(nx)):
            xx = lax.rem(x + (nx - dx), nx)
            if dx:
                pltpu.make_async_remote_copy(
                    src_ref=cxs.at[i], dst_ref=cx.at[i, xx], send_sem=send_sem.at[23 + i], recv_sem=x_sem.at[i, dx],
                    device_id={"samp_1": xx}, device_id_type=pl.DeviceIdType.MESH).wait_recv()
                field = cx[i, xx]
            else:
                field = cxs[i]
            total = total + lax.dot_general(field, xw[:, by_x(xx)], BY_LANES, preferred_element_type=F32)
        sent.append(copy(23 + i, cx.at[i, pl.ds(0, nx - 1)], cx.at[i, pl.ds(0, nx - 1)], zx_peers[0][1]))
        return total

    def ring(step):
        ahead, behind = {"samp_0": lax.rem(z + 1, nz)}, {"samp_0": lax.rem(z + nz - 1, nz)}
        for way, peer in ((0, ahead), (1, behind)):
            if step > 1 and (way == 0 or step <= nz // 2):
                last = spz.at[0]
                pltpu.make_async_remote_copy(
                    src_ref=last, dst_ref=last, send_sem=send_sem.at[26], recv_sem=ring_sem.at[step - 2, way],
                    device_id=peer, device_id_type=pl.DeviceIdType.MESH).wait_recv()
            if step <= nz // 2 - way:
                offset = step - 1 if way else nz - (step - 1)
                block = lax.rem(z + offset, nz)
                pltpu.make_async_remote_copy(
                    src_ref=sp.at[pl.ds(x * nh, nh)] if step == 1 else spz.at[block], dst_ref=spz.at[block],
                    send_sem=send_sem.at[26], recv_sem=ring_sem.at[step - 1, way],
                    device_id=peer, device_id_type=pl.DeviceIdType.MESH).start()
        if step == 1:
            spz[z] = sp[pl.ds(x * nh, nh)]
        if step == nz // 2 + 1:
            sent.append(copy(26, spz.at[pl.ds(0, nz - 1)], spz.at[pl.ds(0, nz - 1)], ahead))

    def feat_sum(i, value):
        fts[i] = value
        ft[i, f] = value
        for _, peer in f_peers:
            copy(5 + i, fts.at[i], ft.at[i, f], peer).start()
        if i == 0:
            whole(27, sp.at[x * nh + 1 - h], partner)
            block = sp.at[pl.ds(x * nh, nh)]
            for dx in far_first(nx):
                if dx:
                    copy(1, block, block, {"samp_1": lax.rem(x + dx, nx)}).start()
            ring(1)
        whole(5 + i, ft.at[i, pl.ds(0, nf - 1)], f_peers[0][1])
        return jnp.sum(ft[i], axis=0)

    def feat_scalars_start(i, value):
        fss[i] = value
        fs[i, f] = value
        for _, peer in f_peers:
            copy(8 + i, fss.at[i], fs.at[i, f], peer).start()

    def feat_scalars(i):
        whole(8 + i, fs.at[i, pl.ds(0, nf - 1)], f_peers[0][1])
        return jnp.sum(fs[i], axis=0)

    def along_z(values, state):
        for dz in far_first(nz):
            zz = lax.rem(z + dz, nz)
            start = pl.multiple_of(zz * (nx * wide), nx * wide)
            part = lax.dot_general(values, xv[:, pl.ds(start, nx * wide)], BY_ROWS, preferred_element_type=F32)
            high = part.astype(BF16)
            rss[zz] = high
            rls[zz] = (part - high.astype(F32)).astype(BF16)
            if dz:
                copy(10, rss.at[zz], rs.at[z], {"samp_0": zz}).start()
        rs[z] = rss[z]
        for dz in far_first(nz):
            zz = lax.rem(z + dz, nz)
            if dz:
                copy(25, rls.at[zz], rl.at[z], {"samp_0": zz}).start()
        rl[z] = rls[z]
        whole(10, rs.at[pl.ds(0, nz - 1)], zx_peers[0][1])
        total = jnp.sum(rs[...].astype(F32), axis=0)
        ridge = (0.5 * lam) * state
        chunks = [total[:, q * wide:(q + 1) * wide] + ridge * jnp.where(x == q, 1.0, 0.0) for q in range(nx)]
        whole(1, sp.at[pl.ds(0, (nx - 1) * nh)], partner)
        project_start(0, chunks, sp[...].reshape(nx * nh * half, rank))
        ring(2)

        whole(25, rl.at[pl.ds(0, nz - 1)], zx_peers[0][1])
        low = jnp.sum(rl[...].astype(F32), axis=0)
        for q in range(nx):
            xs[q] = chunks[q] + low[:, q * wide:(q + 1) * wide]
        for dx in far_first(nx):
            xx = lax.rem(x + dx, nx)
            if dx:
                copy(21, xs.at[xx], xr.at[x], {"samp_1": xx}).start()
        xr[x] = xs[x]
        whole(21, xr.at[pl.ds(0, nx - 1)], {"samp_1": lax.rem(x + 1, nx)})
        vector, full = project_finish(0, jnp.sum(xr[...], axis=0), None)
        ring(5)
        spread_start(0, spread(full))
        return vector, vector + cf[z], gather_rows(1)

    def along_x(values, state, scalars):
        for dx in far_first(nx):
            xx = lax.rem(x + dx, nx)
            part = lax.dot_general(values, xw[:, by_x(xx)], BY_ROWS, preferred_element_type=F32)
            wss[xx] = part.astype(BF16)
            if dx:
                copy(11, wss.at[xx], ws.at[x], {"samp_1": xx}).start()
        ws[x] = wss[x]
        whole(11, ws.at[pl.ds(0, nx - 1)], {"samp_1": lax.rem(x + 1, nx)})
        total = jnp.sum(ws[...].astype(F32), axis=0)
        ridge = (0.5 * lam) * state
        chunks = [total[:, q * wide:(q + 1) * wide] + ridge * jnp.where(z == q, 1.0, 0.0) for q in range(nz)]
        project_start(1, chunks, spz[...].reshape(nz * nh * half, rank))

        for q in range(nz):
            zs[q] = chunks[q]
        for dz in far_first(nz):
            zz = lax.rem(z + dz, nz)
            if dz:
                copy(22, zs.at[zz], zr.at[z], {"samp_0": zz}).start()
        zr[z] = zs[z]
        whole(22, zr.at[pl.ds(0, nz - 1)], zx_peers[0][1])
        vector, full = project_finish(1, jnp.sum(zr[...], axis=0), scalars)
        spread_start(1, spread(full))
        return vector, vector + cf[z], gather_rows(2), jnp.sum(full[:, rank:], axis=0, keepdims=True) * (1.0 / nf)

    def project_start(i, chunks, sketch):
        parts = lax.dot_general(split3(jnp.concatenate(chunks, axis=1)), sketch, BY_ROWS, preferred_element_type=F32)
        projected = parts[:k] + parts[k:2 * k] + parts[2 * k:]
        for q in range(k):
            prs[i, q] = projected[q:q + 1, :]
        for j, peer in y_peers:
            copy(14 + i, prs.at[i, j], pr.at[i, y], peer).start()
        pr[i, y] = prs[i, y]

    def spread(full):
        sketch = spz[...].reshape(nz * nh * half, rank)
        parts = lax.dot_general(split3(ratios * full[:, :rank]), sketch, BY_LANES, preferred_element_type=F32)
        return parts[:k] + parts[k:2 * k] + parts[2 * k:]

    def project_finish(i, part, scalars):
        yhs[i] = part
        copy(12 + i, yhs.at[i], yh.at[i], partner).start()

        whole(14 + i, pr.at[i, pl.ds(0, ny - 1)], y_peers[0][1])
        mine = jnp.sum(pr[i], axis=0)
        if scalars is not None:
            mine = jnp.concatenate([mine, scalars], axis=1)
        across = slice(0, mine.shape[1])
        pzs[i, :, across] = mine
        pz[i, zx, :, across] = mine
        for _, peer in zx_peers:
            copy(16 + i, pzs.at[i, :, across], pz.at[i, zx, :, across], peer).start()
        if i == 0:
            ring(3)

        whole(12 + i, yh.at[i], partner)
        vector = part + yh[i]

        whole(16 + i, pz.at[i, pl.ds(0, nzx - 1), :, across], zx_peers[0][1])
        mine = jnp.sum(pz[i, :, :, across], axis=0)
        pas[i, :, across] = mine
        pa[i, y, :, across] = mine
        for _, peer in y_peers:
            copy(18 + i, pas.at[i, :, across], pa.at[i, y, :, across], peer).start()
        gather_start(1 + i, vector)
        if i == 0:
            ring(4)
        whole(18 + i, pa.at[i, pl.ds(0, ny - 1), :, across], y_peers[0][1])
        return vector, jnp.concatenate([pa[i, q, :, across] for q in range(k)], axis=0)

    loads[0].wait()
    wb[0, :, :half] = w_ref[...]
    wb[0, :, half:] = w_ref[...]
    pl.semaphore_wait(barrier, len(zx_peers) + len(y_peers))
    copy(0, wb.at[0], wb.at[1], partner).start()
    loads[4].wait()
    copy(27, sp.at[x * nh + h], sp.at[x * nh + h], partner).start()
    for load in loads[1:4]:
        load.wait()
    lam = jnp.sum(jnp.where(lax.broadcasted_iota(jnp.int32, (k, k), 0) == lax.broadcasted_iota(jnp.int32, (k, k), 1),
                            lam_ref[...], 0.0), axis=1, keepdims=True)
    values = sv_ref[...].reshape(1, rank)
    ratios = (jnp.min(values, axis=1, keepdims=True) + lam) / (values + lam) - 1.0
    whole(0, wb.at[1], partner)
    own = (lane // half) == h
    weights = jnp.where(own, wb[0], wb[1])
    gather_start(0, weights)
    loads[5].wait()
    pltpu.make_async_copy(x_hbm, xw, local_sem.at[6]).wait()

    logits = feat_sum(0, gather_rows(0))
    probability = jax.nn.sigmoid(logits)
    diag = probability * (1.0 - probability)
    miss = (probability - labels_ref[...].astype(F32)).astype(BF16)
    gradient, gradient_pre, image = along_z(miss, weights)
    residual, direction = -gradient, -gradient_pre
    feat_scalars_start(0, pack(0.5 * lanes(residual * direction), 0.5 * lam * lanes(direction * direction)))
    image = -feat_sum(1, spread_rows(0, image))
    scalars = feat_scalars(0) + pack(jnp.zeros((k, 1), F32), lanes(diag * image * image))
    hess_dir, hess_pre, image_pre, scalars = along_x((diag * image).astype(BF16), direction, scalars)
    res_dot, curvature = unpack(scalars, 0), unpack(scalars, 1)
    step = res_dot / curvature
    residual = residual - step * hess_dir
    precond = direction - step * hess_pre
    feat_scalars_start(1, pack(0.5 * lanes(residual * precond), 0.5 * lam * lanes(precond * precond),
                               0.5 * lam * lanes(precond * direction)))
    image_pre = image - step * feat_sum(2, spread_rows(1, image_pre))
    mine = feat_scalars(1) + pack(jnp.zeros((k, 1), F32), lanes(diag * image_pre * image_pre),
                                  lanes(diag * image_pre * image))
    kzs[...] = mine
    kz[zx * nh + h] = mine
    for dh in reversed(range(nh)):
        for dz in far_first(nz):
            for dx in far_first(nx):
                if dh or dz or dx:
                    peer = {"samp_0": lax.rem(z + dz, nz), "samp_1": lax.rem(x + dx, nx), "samp_2": lax.rem(h + dh, nh)}
                    copy(20, kzs, kz.at[zx * nh + h], peer).start()
    whole(20, kz.at[pl.ds(0, nzx * nh - 1)], partner)
    scalars = jnp.sum(kz[...], axis=0)
    new_dot, pre_pre, pre_dir = (unpack(scalars, place) for place in range(3))
    beta = new_dot / res_dot
    last = new_dot / (pre_pre + 2.0 * beta * pre_dir + beta * beta * curvature)
    update = step * direction + last * (precond + beta * direction)
    update = jnp.where(h == 0, update, pltpu.roll(update, half, 1))
    out_ref[...] = w_ref[...] + update[:, :half]
    for arrived in sent:
        arrived.wait_send()


def shards(sizes, design_matrix, labels, weights, lambdas, sketch, sketch_values):
    nz, nx, nh, nl, nc = sizes
    nzx, nf, ny = nz * nx, nl * nc, nh * nl * nc
    k, half = weights.shape
    wide = 2 * half
    rank = sketch.shape[1]
    vmem = pl.BlockSpec(memory_space=pltpu.VMEM)
    anywhere = pl.BlockSpec(memory_space=pl.ANY)
    dma = pltpu.SemaphoreType.DMA
    return pl.pallas_call(
        functools.partial(kernel, sizes),
        name="step",
        out_shape=jax.ShapeDtypeStruct((k, half), F32),
        in_specs=[anywhere] * 6,
        out_specs=vmem,
        scratch_shapes=[
            pltpu.VMEM(design_matrix.shape, BF16), pltpu.VMEM(design_matrix.shape, BF16),
            pltpu.VMEM((1, design_matrix.shape[0]), jnp.int32), pltpu.VMEM((k, half), F32), pltpu.VMEM((1, k), F32),
            pltpu.VMEM((rank,), F32),
            pltpu.VMEM((nx * nh, half, rank), BF16),
            pltpu.VMEM((2, k, wide), F32),
            pltpu.VMEM((3, nzx, k, wide), BF16), pltpu.VMEM((3, k, wide), BF16),
            pltpu.VMEM((3, nf, k, wide), F32), pltpu.VMEM((3, k, wide), F32),
            pltpu.VMEM((2, nf, 1, wide), F32), pltpu.VMEM((2, 1, wide), F32),
            pltpu.VMEM((nz, k, nx * wide), BF16), pltpu.VMEM((nz, k, nx * wide), BF16),
            pltpu.VMEM((nz, k, nx * wide), BF16), pltpu.VMEM((nz, k, nx * wide), BF16),
            pltpu.VMEM((nx, k, nz * wide), BF16), pltpu.VMEM((nx, k, nz * wide), BF16),
            pltpu.VMEM((nx, k, wide), F32), pltpu.VMEM((nx, k, wide), F32),
            pltpu.VMEM((nz, k, wide), F32), pltpu.VMEM((nz, k, wide), F32),
            pltpu.VMEM((nz, nh, half, rank), BF16),
            pltpu.VMEM((2, k, wide), F32), pltpu.VMEM((2, k, wide), F32),
            pltpu.VMEM((2, ny, 1, rank), F32), pltpu.VMEM((2, ny, 1, rank), F32),
            pltpu.VMEM((2, nzx, 1, rank + wide), F32), pltpu.VMEM((2, 1, rank + wide), F32),
            pltpu.VMEM((2, ny, 1, rank + wide), F32), pltpu.VMEM((2, 1, rank + wide), F32),
            pltpu.VMEM((2, nx, k, nz * wide), BF16), pltpu.VMEM((2, k, nz * wide), BF16),
            pltpu.VMEM((nz, k, wide), F32),
            pltpu.VMEM((nzx * nh, 1, wide), F32), pltpu.VMEM((1, wide), F32),
            dma((7,)), dma((28,)), dma((28,)), dma((3, nz)), dma((nz // 2, 2)), dma((2, nx)),
        ],
        compiler_params=pltpu.CompilerParams(collective_id=0, has_side_effects=True, vmem_limit_bytes=32 << 20),
    )(*(pltpu.with_memory_space_constraint(operand, pltpu.HBM) for operand in (
        design_matrix, labels.reshape(1, -1), weights, lambdas.reshape(1, -1), sketch, sketch_values)))


def solution(mesh):
    sizes = (8, 4, 2, 4, 2)
    finer = Mesh(mesh.devices.reshape(sizes), SAMP + FEAT)
    placed = (P(SAMP, FEAT), P(SAMP), P(None, FEAT_SAMP), P(), P(FEAT_SAMP, None), P())
    return jax.shard_map(
        functools.partial(shards, sizes), mesh=finer, in_specs=placed, out_specs=P(None, FEAT_SAMP), check_vma=False
    )
```

```python
import functools

import jax
import jax.numpy as jnp
from jax import lax
from jax.experimental import pallas as pl
from jax.experimental.pallas import tpu as pltpu
from jax.sharding import Mesh
from jax.sharding import PartitionSpec as P

SAMP = ("samp_0", "samp_1", "samp_2")
FEAT = ("feat_0", "feat_1")
FEAT_SAMP = FEAT + SAMP
F32, BF16 = jnp.float32, jnp.bfloat16
BY_LANES = (((1,), (1,)), ((), ()))
BY_ROWS = (((1,), (0,)), ((), ()))


def far_first(n):
    return sorted(range(n), key=lambda d: -min(d, n - d))


def split3(value):
    high = value.astype(BF16)
    rest = value - high.astype(F32)
    mid = rest.astype(BF16)
    low = (rest - mid.astype(F32)).astype(BF16)
    return jnp.concatenate([high, mid, low], axis=0)


def kernel(sizes, x_hbm, labels_hbm, w_hbm, lam_hbm, s_hbm, sv_hbm, out_ref,
           xv, xw, labels_ref, w_ref, lam_ref, sv_ref, sp, wb, ag, ags, ft, fts, fs, fss, rs, rss, rl, rls, ws, wss, xr, xs, zr, zs, spz, yh, yhs,
           pr, prs, pz, pzs, pa, pas, cx, cxs, cf, kz, kzs, local_sem, send_sem, recv_sem, gather_sem, ring_sem, x_sem):
    nz, nx, nh, nl, nc = sizes
    nzx, nf, ny = nz * nx, nl * nc, nh * nl * nc
    k, half = w_ref.shape
    wide = 2 * half
    rank = s_hbm.shape[1]
    z, x, h, l, c = (lax.axis_index(name) for name in SAMP + FEAT)
    zx, f, y = z * nx + x, l * nc + c, (h * nl + l) * nc + c

    zx_peers = []
    for dz in far_first(nz):
        for dx in far_first(nx):
            if dz or dx:
                zz, xx = lax.rem(z + dz, nz), lax.rem(x + dx, nx)
                zx_peers.append((zz * nx + xx, {"samp_0": zz, "samp_1": xx}))
    y_peers, f_peers = [], []
    for dl in far_first(nl):
        for dh in reversed(range(nh)):
            for dc in reversed(range(nc)):
                if dh or dl or dc:
                    hh, ll, cc = lax.rem(h + dh, nh), lax.rem(l + dl, nl), lax.rem(c + dc, nc)
                    y_peers.append(((hh * nl + ll) * nc + cc, {"samp_2": hh, "feat_0": ll, "feat_1": cc}))
                    if not dh:
                        f_peers.append((ll * nc + cc, {"feat_0": ll, "feat_1": cc}))
    partner = {"samp_2": 1 - h}

    loads = [pltpu.make_async_copy(src, dst, local_sem.at[j]) for j, (src, dst) in enumerate(
        [(w_hbm, w_ref), (lam_hbm, lam_ref), (sv_hbm, sv_ref), (labels_hbm, labels_ref), (s_hbm, sp.at[x * nh + h]), (x_hbm, xv)])]
    loads[0].start()
    loads[4].start()
    barrier = pltpu.get_barrier_semaphore()
    for _, peer in zx_peers + y_peers:
        pl.semaphore_signal(barrier, inc=1, device_id=peer, device_id_type=pl.DeviceIdType.MESH)

    for j in (1, 2, 3, 5):
        loads[j].start()
    for q in range(nx):
        for zz in range(nz):
            pltpu.make_async_copy(x_hbm.at[:, pl.ds((zz * nx + q) * wide, wide)], xw.at[:, pl.ds((q * nz + zz) * wide, wide)],
                                  local_sem.at[6]).start()

    def copy(phase, src, dst, peer):
        return pltpu.make_async_remote_copy(
            src_ref=src, dst_ref=dst, send_sem=send_sem.at[phase], recv_sem=recv_sem.at[phase],
            device_id=peer, device_id_type=pl.DeviceIdType.MESH)

    sent = []

    def whole(phase, buffer, peer):
        arrived = copy(phase, buffer, buffer, peer)
        arrived.wait_recv()
        sent.append(arrived)

    lane = lax.broadcasted_iota(jnp.int32, (k, wide), 1)
    row = lax.broadcasted_iota(jnp.int32, (k, wide), 0)

    def pack(*columns):
        total = 0.0
        for place, column in enumerate(columns):
            total = total + jnp.where(lane == row + place * k, column, 0.0)
        return jnp.sum(total, axis=0, keepdims=True)

    def unpack(packed, place):
        return jnp.sum(jnp.where(lane == row + place * k, packed, 0.0), axis=1, keepdims=True)

    def lanes(value):
        return jnp.sum(value, axis=1, keepdims=True)

    def gather_start(i, value):
        ags[i] = value.astype(BF16)
        ag[i, zx] = value.astype(BF16)
        for dz in far_first(nz):
            for dx in far_first(nx):
                if dz or dx:
                    zz, xx = lax.rem(z + dz, nz), lax.rem(x + dx, nx)
                    pltpu.make_async_remote_copy(
                        src_ref=ags.at[i], dst_ref=ag.at[i, zx], send_sem=send_sem.at[2 + i], recv_sem=gather_sem.at[i, dz],
                        device_id={"samp_0": zz, "samp_1": xx}, device_id_type=pl.DeviceIdType.MESH).start()

    def arrived_group(phase, place, dz, group):
        pltpu.make_async_remote_copy(
            src_ref=group, dst_ref=group, send_sem=send_sem.at[phase], recv_sem=gather_sem.at[place, dz],
            device_id=zx_peers[0][1], device_id_type=pl.DeviceIdType.MESH).wait_recv()

    def rows_of(field, zz):
        start = pl.multiple_of(zz * (nx * wide), nx * wide)
        return lax.dot_general(field, xv[:, pl.ds(start, nx * wide)], BY_LANES, preferred_element_type=F32)

    def gather_rows(i):
        total = jnp.zeros((k, xv.shape[0]), F32)
        for dz in reversed(far_first(nz)):
            if i == 0 and dz == nz // 2:
                whole(27, sp.at[x * nh + 1 - h], partner)
                ring(1)
            arrived_group(2 + i, i, dz, ag.at[i, pl.ds(0, nx if dz else nx - 1)])
            zz = lax.rem(z + (nz - dz), nz)
            total = total + rows_of(jnp.concatenate([ag[i, zz * nx + q] for q in range(nx)], axis=1), zz)
        sent.append(copy(2 + i, ag.at[i, pl.ds(0, nzx - 1)], ag.at[i, pl.ds(0, nzx - 1)], zx_peers[0][1]))
        return total

    def by_x(xx):
        return pl.ds(pl.multiple_of(xx * (nz * wide), nz * wide), nz * wide)

    def spread_start(i, value):
        cxs[i] = value.astype(BF16)
        for dx in far_first(nx):
            if dx:
                pltpu.make_async_remote_copy(
                    src_ref=cxs.at[i], dst_ref=cx.at[i, x], send_sem=send_sem.at[23 + i], recv_sem=x_sem.at[i, dx],
                    device_id={"samp_1": lax.rem(x + dx, nx)}, device_id_type=pl.DeviceIdType.MESH).start()
        for q in range(nz):
            cf[q] = value[:, q * wide:(q + 1) * wide]

    def spread_rows(i, total):
        for dx in reversed(far_first(nx)):
            xx = lax.rem(x + (nx - dx), nx)
            if dx:
                pltpu.make_async_remote_copy(
                    src_ref=cxs.at[i], dst_ref=cx.at[i, xx], send_sem=send_sem.at[23 + i], recv_sem=x_sem.at[i, dx],
                    device_id={"samp_1": xx}, device_id_type=pl.DeviceIdType.MESH).wait_recv()
                field = cx[i, xx]
            else:
                field = cxs[i]
            total = total + lax.dot_general(field, xw[:, by_x(xx)], BY_LANES, preferred_element_type=F32)
        sent.append(copy(23 + i, cx.at[i, pl.ds(0, nx - 1)], cx.at[i, pl.ds(0, nx - 1)], zx_peers[0][1]))
        return total

    def ring(step):
        ahead, behind = {"samp_0": lax.rem(z + 1, nz)}, {"samp_0": lax.rem(z + nz - 1, nz)}
        for way, peer in ((0, ahead), (1, behind)):
            if step > 1 and (way == 0 or step <= nz // 2):
                last = spz.at[0]
                pltpu.make_async_remote_copy(
                    src_ref=last, dst_ref=last, send_sem=send_sem.at[26], recv_sem=ring_sem.at[step - 2, way],
                    device_id=peer, device_id_type=pl.DeviceIdType.MESH).wait_recv()
            if step <= nz // 2 - way:
                offset = step - 1 if way else nz - (step - 1)
                block = lax.rem(z + offset, nz)
                pltpu.make_async_remote_copy(
                    src_ref=sp.at[pl.ds(x * nh, nh)] if step == 1 else spz.at[block], dst_ref=spz.at[block],
                    send_sem=send_sem.at[26], recv_sem=ring_sem.at[step - 1, way],
                    device_id=peer, device_id_type=pl.DeviceIdType.MESH).start()
        if step == 1:
            spz[z] = sp[pl.ds(x * nh, nh)]
        if step == nz // 2 + 1:
            sent.append(copy(26, spz.at[pl.ds(0, nz - 1)], spz.at[pl.ds(0, nz - 1)], ahead))

    def feat_sum(i, value):
        fts[i] = value
        ft[i, f] = value
        for _, peer in f_peers:
            copy(5 + i, fts.at[i], ft.at[i, f], peer).start()
        if i == 0:
            block = sp.at[pl.ds(x * nh, nh)]
            for dx in far_first(nx):
                if dx:
                    copy(1, block, block, {"samp_1": lax.rem(x + dx, nx)}).start()
            ring(2)
        whole(5 + i, ft.at[i, pl.ds(0, nf - 1)], f_peers[0][1])
        return jnp.sum(ft[i], axis=0)

    def feat_scalars_start(i, value):
        fss[i] = value
        fs[i, f] = value
        for _, peer in f_peers:
            copy(8 + i, fss.at[i], fs.at[i, f], peer).start()

    def feat_scalars(i):
        whole(8 + i, fs.at[i, pl.ds(0, nf - 1)], f_peers[0][1])
        return jnp.sum(fs[i], axis=0)

    def along_z(values, state):
        for dz in far_first(nz):
            zz = lax.rem(z + dz, nz)
            start = pl.multiple_of(zz * (nx * wide), nx * wide)
            part = lax.dot_general(values, xv[:, pl.ds(start, nx * wide)], BY_ROWS, preferred_element_type=F32)
            high = part.astype(BF16)
            rss[zz] = high
            rls[zz] = (part - high.astype(F32)).astype(BF16)
            if dz:
                copy(10, rss.at[zz], rs.at[z], {"samp_0": zz}).start()
        rs[z] = rss[z]
        for dz in far_first(nz):
            zz = lax.rem(z + dz, nz)
            if dz:
                copy(25, rls.at[zz], rl.at[z], {"samp_0": zz}).start()
        rl[z] = rls[z]
        whole(10, rs.at[pl.ds(0, nz - 1)], zx_peers[0][1])
        total = jnp.sum(rs[...].astype(F32), axis=0)
        ridge = (0.5 * lam) * state
        chunks = [total[:, q * wide:(q + 1) * wide] + ridge * jnp.where(x == q, 1.0, 0.0) for q in range(nx)]
        whole(1, sp.at[pl.ds(0, (nx - 1) * nh)], partner)
        project_start(0, chunks, sp[...].reshape(nx * nh * half, rank))
        ring(3)

        whole(25, rl.at[pl.ds(0, nz - 1)], zx_peers[0][1])
        low = jnp.sum(rl[...].astype(F32), axis=0)
        for q in range(nx):
            xs[q] = chunks[q] + low[:, q * wide:(q + 1) * wide]
        for dx in far_first(nx):
            xx = lax.rem(x + dx, nx)
            if dx:
                copy(21, xs.at[xx], xr.at[x], {"samp_1": xx}).start()
        xr[x] = xs[x]
        whole(21, xr.at[pl.ds(0, nx - 1)], {"samp_1": lax.rem(x + 1, nx)})
        vector, full = project_finish(0, jnp.sum(xr[...], axis=0), None)
        ring(5)
        spread_start(0, spread(full))
        return vector, vector + cf[z], gather_rows(1)

    def along_x(values, state, scalars):
        for dx in far_first(nx):
            xx = lax.rem(x + dx, nx)
            part = lax.dot_general(values, xw[:, by_x(xx)], BY_ROWS, preferred_element_type=F32)
            wss[xx] = part.astype(BF16)
            if dx:
                copy(11, wss.at[xx], ws.at[x], {"samp_1": xx}).start()
        ws[x] = wss[x]
        whole(11, ws.at[pl.ds(0, nx - 1)], {"samp_1": lax.rem(x + 1, nx)})
        total = jnp.sum(ws[...].astype(F32), axis=0)
        ridge = (0.5 * lam) * state
        chunks = [total[:, q * wide:(q + 1) * wide] + ridge * jnp.where(z == q, 1.0, 0.0) for q in range(nz)]
        project_start(1, chunks, spz[...].reshape(nz * nh * half, rank))

        for q in range(nz):
            zs[q] = chunks[q]
        for dz in far_first(nz):
            zz = lax.rem(z + dz, nz)
            if dz:
                copy(22, zs.at[zz], zr.at[z], {"samp_0": zz}).start()
        zr[z] = zs[z]
        whole(22, zr.at[pl.ds(0, nz - 1)], zx_peers[0][1])
        vector, full = project_finish(1, jnp.sum(zr[...], axis=0), scalars)
        spread_start(1, spread(full))
        return vector, vector + cf[z], gather_rows(2), jnp.sum(full[:, rank:], axis=0, keepdims=True) * (1.0 / nf)

    def project_start(i, chunks, sketch):
        parts = lax.dot_general(split3(jnp.concatenate(chunks, axis=1)), sketch, BY_ROWS, preferred_element_type=F32)
        projected = parts[:k] + parts[k:2 * k] + parts[2 * k:]
        for q in range(k):
            prs[i, q] = projected[q:q + 1, :]
        for j, peer in y_peers:
            copy(14 + i, prs.at[i, j], pr.at[i, y], peer).start()
        pr[i, y] = prs[i, y]

    def spread(full):
        sketch = spz[...].reshape(nz * nh * half, rank)
        parts = lax.dot_general(split3(ratios * full[:, :rank]), sketch, BY_LANES, preferred_element_type=F32)
        return parts[:k] + parts[k:2 * k] + parts[2 * k:]

    def project_finish(i, part, scalars):
        yhs[i] = part
        copy(12 + i, yhs.at[i], yh.at[i], partner).start()

        whole(14 + i, pr.at[i, pl.ds(0, ny - 1)], y_peers[0][1])
        mine = jnp.sum(pr[i], axis=0)
        if scalars is not None:
            mine = jnp.concatenate([mine, scalars], axis=1)
        across = slice(0, mine.shape[1])
        pzs[i, :, across] = mine
        pz[i, zx, :, across] = mine
        for _, peer in zx_peers:
            copy(16 + i, pzs.at[i, :, across], pz.at[i, zx, :, across], peer).start()

        whole(12 + i, yh.at[i], partner)
        vector = part + yh[i]

        whole(16 + i, pz.at[i, pl.ds(0, nzx - 1), :, across], zx_peers[0][1])
        mine = jnp.sum(pz[i, :, :, across], axis=0)
        pas[i, :, across] = mine
        pa[i, y, :, across] = mine
        for _, peer in y_peers:
            copy(18 + i, pas.at[i, :, across], pa.at[i, y, :, across], peer).start()
        gather_start(1 + i, vector)
        if i == 0:
            ring(4)
        whole(18 + i, pa.at[i, pl.ds(0, ny - 1), :, across], y_peers[0][1])
        return vector, jnp.concatenate([pa[i, q, :, across] for q in range(k)], axis=0)

    loads[0].wait()
    wb[0, :, :half] = w_ref[...]
    wb[0, :, half:] = w_ref[...]
    pl.semaphore_wait(barrier, len(zx_peers) + len(y_peers))
    copy(0, wb.at[0], wb.at[1], partner).start()
    loads[4].wait()
    copy(27, sp.at[x * nh + h], sp.at[x * nh + h], partner).start()
    for load in loads[1:4]:
        load.wait()
    lam = jnp.sum(jnp.where(lax.broadcasted_iota(jnp.int32, (k, k), 0) == lax.broadcasted_iota(jnp.int32, (k, k), 1),
                            lam_ref[...], 0.0), axis=1, keepdims=True)
    values = sv_ref[...].reshape(1, rank)
    ratios = (jnp.min(values, axis=1, keepdims=True) + lam) / (values + lam) - 1.0
    whole(0, wb.at[1], partner)
    own = (lane // half) == h
    weights = jnp.where(own, wb[0], wb[1])
    gather_start(0, weights)
    loads[5].wait()
    pltpu.make_async_copy(x_hbm, xw, local_sem.at[6]).wait()

    logits = feat_sum(0, gather_rows(0))
    probability = jax.nn.sigmoid(logits)
    diag = probability * (1.0 - probability)
    miss = (probability - labels_ref[...].astype(F32)).astype(BF16)
    gradient, gradient_pre, image = along_z(miss, weights)
    residual, direction = -gradient, -gradient_pre
    feat_scalars_start(0, pack(0.5 * lanes(residual * direction), 0.5 * lam * lanes(direction * direction)))
    image = -feat_sum(1, spread_rows(0, image))
    scalars = feat_scalars(0) + pack(jnp.zeros((k, 1), F32), lanes(diag * image * image))
    hess_dir, hess_pre, image_pre, scalars = along_x((diag * image).astype(BF16), direction, scalars)
    res_dot, curvature = unpack(scalars, 0), unpack(scalars, 1)
    step = res_dot / curvature
    residual = residual - step * hess_dir
    precond = direction - step * hess_pre
    feat_scalars_start(1, pack(0.5 * lanes(residual * precond), 0.5 * lam * lanes(precond * precond),
                               0.5 * lam * lanes(precond * direction)))
    image_pre = image - step * feat_sum(2, spread_rows(1, image_pre))
    mine = feat_scalars(1) + pack(jnp.zeros((k, 1), F32), lanes(diag * image_pre * image_pre),
                                  lanes(diag * image_pre * image))
    kzs[...] = mine
    kz[zx * nh + h] = mine
    for dh in reversed(range(nh)):
        for dz in far_first(nz):
            for dx in far_first(nx):
                if dh or dz or dx:
                    peer = {"samp_0": lax.rem(z + dz, nz), "samp_1": lax.rem(x + dx, nx), "samp_2": lax.rem(h + dh, nh)}
                    copy(20, kzs, kz.at[zx * nh + h], peer).start()
    whole(20, kz.at[pl.ds(0, nzx * nh - 1)], partner)
    scalars = jnp.sum(kz[...], axis=0)
    new_dot, pre_pre, pre_dir = (unpack(scalars, place) for place in range(3))
    beta = new_dot / res_dot
    last = new_dot / (pre_pre + 2.0 * beta * pre_dir + beta * beta * curvature)
    update = step * direction + last * (precond + beta * direction)
    update = jnp.where(h == 0, update, pltpu.roll(update, half, 1))
    out_ref[...] = w_ref[...] + update[:, :half]
    for arrived in sent:
        arrived.wait_send()


def shards(sizes, design_matrix, labels, weights, lambdas, sketch, sketch_values):
    nz, nx, nh, nl, nc = sizes
    nzx, nf, ny = nz * nx, nl * nc, nh * nl * nc
    k, half = weights.shape
    wide = 2 * half
    rank = sketch.shape[1]
    vmem = pl.BlockSpec(memory_space=pltpu.VMEM)
    anywhere = pl.BlockSpec(memory_space=pl.ANY)
    dma = pltpu.SemaphoreType.DMA
    return pl.pallas_call(
        functools.partial(kernel, sizes),
        name="step",
        out_shape=jax.ShapeDtypeStruct((k, half), F32),
        in_specs=[anywhere] * 6,
        out_specs=vmem,
        scratch_shapes=[
            pltpu.VMEM(design_matrix.shape, BF16), pltpu.VMEM(design_matrix.shape, BF16),
            pltpu.VMEM((1, design_matrix.shape[0]), jnp.int32), pltpu.VMEM((k, half), F32), pltpu.VMEM((1, k), F32),
            pltpu.VMEM((rank,), F32),
            pltpu.VMEM((nx * nh, half, rank), BF16),
            pltpu.VMEM((2, k, wide), F32),
            pltpu.VMEM((3, nzx, k, wide), BF16), pltpu.VMEM((3, k, wide), BF16),
            pltpu.VMEM((3, nf, k, wide), F32), pltpu.VMEM((3, k, wide), F32),
            pltpu.VMEM((2, nf, 1, wide), F32), pltpu.VMEM((2, 1, wide), F32),
            pltpu.VMEM((nz, k, nx * wide), BF16), pltpu.VMEM((nz, k, nx * wide), BF16),
            pltpu.VMEM((nz, k, nx * wide), BF16), pltpu.VMEM((nz, k, nx * wide), BF16),
            pltpu.VMEM((nx, k, nz * wide), BF16), pltpu.VMEM((nx, k, nz * wide), BF16),
            pltpu.VMEM((nx, k, wide), F32), pltpu.VMEM((nx, k, wide), F32),
            pltpu.VMEM((nz, k, wide), F32), pltpu.VMEM((nz, k, wide), F32),
            pltpu.VMEM((nz, nh, half, rank), BF16),
            pltpu.VMEM((2, k, wide), F32), pltpu.VMEM((2, k, wide), F32),
            pltpu.VMEM((2, ny, 1, rank), F32), pltpu.VMEM((2, ny, 1, rank), F32),
            pltpu.VMEM((2, nzx, 1, rank + wide), F32), pltpu.VMEM((2, 1, rank + wide), F32),
            pltpu.VMEM((2, ny, 1, rank + wide), F32), pltpu.VMEM((2, 1, rank + wide), F32),
            pltpu.VMEM((2, nx, k, nz * wide), BF16), pltpu.VMEM((2, k, nz * wide), BF16),
            pltpu.VMEM((nz, k, wide), F32),
            pltpu.VMEM((nzx * nh, 1, wide), F32), pltpu.VMEM((1, wide), F32),
            dma((7,)), dma((28,)), dma((28,)), dma((3, nz)), dma((nz // 2, 2)), dma((2, nx)),
        ],
        compiler_params=pltpu.CompilerParams(collective_id=0, has_side_effects=True, vmem_limit_bytes=32 << 20),
    )(*(pltpu.with_memory_space_constraint(operand, pltpu.HBM) for operand in (
        design_matrix, labels.reshape(1, -1), weights, lambdas.reshape(1, -1), sketch, sketch_values)))


def solution(mesh):
    sizes = (8, 4, 2, 4, 2)
    finer = Mesh(mesh.devices.reshape(sizes), SAMP + FEAT)
    placed = (P(SAMP, FEAT), P(SAMP), P(None, FEAT_SAMP), P(), P(FEAT_SAMP, None), P())
    return jax.shard_map(
        functools.partial(shards, sizes), mesh=finer, in_specs=placed, out_specs=P(None, FEAT_SAMP), check_vma=False
    )
```

```python
import functools

import jax
import jax.numpy as jnp
from jax import lax
from jax.experimental import pallas as pl
from jax.experimental.pallas import tpu as pltpu
from jax.sharding import Mesh
from jax.sharding import PartitionSpec as P

SAMP = ("samp_0", "samp_1", "samp_2")
FEAT = ("feat_0", "feat_1")
FEAT_SAMP = FEAT + SAMP
F32, BF16 = jnp.float32, jnp.bfloat16
BY_LANES = (((1,), (1,)), ((), ()))
BY_ROWS = (((1,), (0,)), ((), ()))


def far_first(n):
    return sorted(range(n), key=lambda d: -min(d, n - d))


def split3(value):
    high = value.astype(BF16)
    rest = value - high.astype(F32)
    mid = rest.astype(BF16)
    low = (rest - mid.astype(F32)).astype(BF16)
    return jnp.concatenate([high, mid, low], axis=0)


def kernel(sizes, x_hbm, labels_hbm, w_hbm, lam_hbm, s_hbm, sv_hbm, out_ref,
           xv, xw, labels_ref, w_ref, lam_ref, sv_ref, sp, wb, ag, ags, ft, fts, fs, fss, rs, rss, rl, rls, lz, lzs, ws, wss, xr, xs, zr, zs, spz, yh, yhs,
           pr, prs, pz, pzs, pa, pas, cx, cxs, cf, kz, kzs, local_sem, send_sem, recv_sem, gather_sem, ring_sem, x_sem):
    nz, nx, nh, nl, nc = sizes
    nzx, nf, ny = nz * nx, nl * nc, nh * nl * nc
    k, half = w_ref.shape
    wide = 2 * half
    rank = s_hbm.shape[1]
    z, x, h, l, c = (lax.axis_index(name) for name in SAMP + FEAT)
    zx, f, y = z * nx + x, l * nc + c, (h * nl + l) * nc + c

    zx_peers = []
    for dz in far_first(nz):
        for dx in far_first(nx):
            if dz or dx:
                zz, xx = lax.rem(z + dz, nz), lax.rem(x + dx, nx)
                zx_peers.append((zz * nx + xx, {"samp_0": zz, "samp_1": xx}))
    y_peers, f_peers = [], []
    for dl in far_first(nl):
        for dh in reversed(range(nh)):
            for dc in reversed(range(nc)):
                if dh or dl or dc:
                    hh, ll, cc = lax.rem(h + dh, nh), lax.rem(l + dl, nl), lax.rem(c + dc, nc)
                    y_peers.append(((hh * nl + ll) * nc + cc, {"samp_2": hh, "feat_0": ll, "feat_1": cc}))
                    if not dh:
                        f_peers.append((ll * nc + cc, {"feat_0": ll, "feat_1": cc}))
    partner = {"samp_2": 1 - h}

    loads = [pltpu.make_async_copy(src, dst, local_sem.at[j]) for j, (src, dst) in enumerate(
        [(w_hbm, w_ref), (lam_hbm, lam_ref), (sv_hbm, sv_ref), (labels_hbm, labels_ref), (s_hbm, sp.at[x * nh + h]), (x_hbm, xv)])]
    loads[0].start()
    loads[4].start()
    barrier = pltpu.get_barrier_semaphore()
    for _, peer in zx_peers + y_peers:
        pl.semaphore_signal(barrier, inc=1, device_id=peer, device_id_type=pl.DeviceIdType.MESH)

    for j in (1, 2, 3, 5):
        loads[j].start()
    for q in range(nx):
        for zz in range(nz):
            pltpu.make_async_copy(x_hbm.at[:, pl.ds((zz * nx + q) * wide, wide)], xw.at[:, pl.ds((q * nz + zz) * wide, wide)],
                                  local_sem.at[6]).start()

    def copy(phase, src, dst, peer):
        return pltpu.make_async_remote_copy(
            src_ref=src, dst_ref=dst, send_sem=send_sem.at[phase], recv_sem=recv_sem.at[phase],
            device_id=peer, device_id_type=pl.DeviceIdType.MESH)

    sent = []

    def whole(phase, buffer, peer):
        arrived = copy(phase, buffer, buffer, peer)
        arrived.wait_recv()
        sent.append(arrived)

    lane = lax.broadcasted_iota(jnp.int32, (k, wide), 1)
    row = lax.broadcasted_iota(jnp.int32, (k, wide), 0)

    def pack(*columns):
        total = 0.0
        for place, column in enumerate(columns):
            total = total + jnp.where(lane == row + place * k, column, 0.0)
        return jnp.sum(total, axis=0, keepdims=True)

    def unpack(packed, place):
        return jnp.sum(jnp.where(lane == row + place * k, packed, 0.0), axis=1, keepdims=True)

    def lanes(value):
        return jnp.sum(value, axis=1, keepdims=True)

    def gather_start(i, value):
        ags[i] = value.astype(BF16)
        ag[i, zx] = value.astype(BF16)
        for dz in far_first(nz):
            for dx in far_first(nx):
                if dz or dx:
                    zz, xx = lax.rem(z + dz, nz), lax.rem(x + dx, nx)
                    pltpu.make_async_remote_copy(
                        src_ref=ags.at[i], dst_ref=ag.at[i, zx], send_sem=send_sem.at[2 + i], recv_sem=gather_sem.at[i, dz],
                        device_id={"samp_0": zz, "samp_1": xx}, device_id_type=pl.DeviceIdType.MESH).start()

    def arrived_group(phase, place, dz, group):
        pltpu.make_async_remote_copy(
            src_ref=group, dst_ref=group, send_sem=send_sem.at[phase], recv_sem=gather_sem.at[place, dz],
            device_id=zx_peers[0][1], device_id_type=pl.DeviceIdType.MESH).wait_recv()

    def rows_of(field, zz):
        start = pl.multiple_of(zz * (nx * wide), nx * wide)
        return lax.dot_general(field, xv[:, pl.ds(start, nx * wide)], BY_LANES, preferred_element_type=F32)

    def gather_rows(i):
        total = jnp.zeros((k, xv.shape[0]), F32)
        for dz in reversed(far_first(nz)):
            arrived_group(2 + i, i, dz, ag.at[i, pl.ds(0, nx if dz else nx - 1)])
            zz = lax.rem(z + (nz - dz), nz)
            total = total + rows_of(jnp.concatenate([ag[i, zz * nx + q] for q in range(nx)], axis=1), zz)
        sent.append(copy(2 + i, ag.at[i, pl.ds(0, nzx - 1)], ag.at[i, pl.ds(0, nzx - 1)], zx_peers[0][1]))
        return total

    def by_x(xx):
        return pl.ds(pl.multiple_of(xx * (nz * wide), nz * wide), nz * wide)

    def spread_start(i, value):
        cxs[i] = value.astype(BF16)
        for dx in far_first(nx):
            if dx:
                pltpu.make_async_remote_copy(
                    src_ref=cxs.at[i], dst_ref=cx.at[i, x], send_sem=send_sem.at[23 + i], recv_sem=x_sem.at[i, dx],
                    device_id={"samp_1": lax.rem(x + dx, nx)}, device_id_type=pl.DeviceIdType.MESH).start()
        for q in range(nz):
            cf[q] = value[:, q * wide:(q + 1) * wide]

    def spread_rows(i, total):
        for dx in reversed(far_first(nx)):
            xx = lax.rem(x + (nx - dx), nx)
            if dx:
                pltpu.make_async_remote_copy(
                    src_ref=cxs.at[i], dst_ref=cx.at[i, xx], send_sem=send_sem.at[23 + i], recv_sem=x_sem.at[i, dx],
                    device_id={"samp_1": xx}, device_id_type=pl.DeviceIdType.MESH).wait_recv()
                field = cx[i, xx]
            else:
                field = cxs[i]
            total = total + lax.dot_general(field, xw[:, by_x(xx)], BY_LANES, preferred_element_type=F32)
        sent.append(copy(23 + i, cx.at[i, pl.ds(0, nx - 1)], cx.at[i, pl.ds(0, nx - 1)], zx_peers[0][1]))
        return total

    def ring(step):
        ahead, behind = {"samp_0": lax.rem(z + 1, nz)}, {"samp_0": lax.rem(z + nz - 1, nz)}
        for way, peer in ((0, ahead), (1, behind)):
            if step > 1 and (way == 0 or step <= nz // 2):
                last = spz.at[0]
                pltpu.make_async_remote_copy(
                    src_ref=last, dst_ref=last, send_sem=send_sem.at[26], recv_sem=ring_sem.at[step - 2, way],
                    device_id=peer, device_id_type=pl.DeviceIdType.MESH).wait_recv()
            if step <= nz // 2 - way:
                offset = step - 1 if way else nz - (step - 1)
                block = lax.rem(z + offset, nz)
                pltpu.make_async_remote_copy(
                    src_ref=sp.at[pl.ds(x * nh, nh)] if step == 1 else spz.at[block], dst_ref=spz.at[block],
                    send_sem=send_sem.at[26], recv_sem=ring_sem.at[step - 1, way],
                    device_id=peer, device_id_type=pl.DeviceIdType.MESH).start()
        if step == 1:
            spz[z] = sp[pl.ds(x * nh, nh)]
        if step == nz // 2 + 1:
            sent.append(copy(26, spz.at[pl.ds(0, nz - 1)], spz.at[pl.ds(0, nz - 1)], ahead))

    def feat_sum(i, value):
        fts[i] = value
        ft[i, f] = value
        for _, peer in f_peers:
            copy(5 + i, fts.at[i], ft.at[i, f], peer).start()
        if i == 0:
            whole(27, sp.at[x * nh + 1 - h], partner)
            block = sp.at[pl.ds(x * nh, nh)]
            for dx in far_first(nx):
                if dx:
                    copy(1, block, block, {"samp_1": lax.rem(x + dx, nx)}).start()
            ring(1)
        whole(5 + i, ft.at[i, pl.ds(0, nf - 1)], f_peers[0][1])
        return jnp.sum(ft[i], axis=0)

    def feat_scalars_start(i, value):
        fss[i] = value
        fs[i, f] = value
        for _, peer in f_peers:
            copy(8 + i, fss.at[i], fs.at[i, f], peer).start()

    def feat_scalars(i):
        whole(8 + i, fs.at[i, pl.ds(0, nf - 1)], f_peers[0][1])
        return jnp.sum(fs[i], axis=0)

    def along_z(values, state):
        for dz in far_first(nz):
            zz = lax.rem(z + dz, nz)
            start = pl.multiple_of(zz * (nx * wide), nx * wide)
            part = lax.dot_general(values, xv[:, pl.ds(start, nx * wide)], BY_ROWS, preferred_element_type=F32)
            high = part.astype(BF16)
            rss[zz] = high
            low = (part - high.astype(F32)).astype(BF16)
            for q in range(nx):
                rls[q, :, pl.ds(pl.multiple_of(zz * wide, wide), wide)] = low[:, q * wide:(q + 1) * wide]
            if dz:
                copy(10, rss.at[zz], rs.at[z], {"samp_0": zz}).start()
        rs[z] = rss[z]
        for dx in far_first(nx):
            xx = lax.rem(x + dx, nx)
            if dx:
                copy(25, rls.at[xx], rl.at[x], {"samp_1": xx}).start()
        rl[x] = rls[x]
        whole(10, rs.at[pl.ds(0, nz - 1)], zx_peers[0][1])
        total = jnp.sum(rs[...].astype(F32), axis=0)
        ridge = (0.5 * lam) * state
        chunks = [total[:, q * wide:(q + 1) * wide] + ridge * jnp.where(x == q, 1.0, 0.0) for q in range(nx)]
        whole(1, sp.at[pl.ds(0, (nx - 1) * nh)], partner)
        project_start(0, chunks, sp[...].reshape(nx * nh * half, rank))
        ring(2)

        whole(25, rl.at[pl.ds(0, nx - 1)], {"samp_1": lax.rem(x + 1, nx)})
        low = jnp.sum(rl[...].astype(F32), axis=0)
        for q in range(nz):
            lzs[q] = low[:, q * wide:(q + 1) * wide]
        for dz in far_first(nz):
            zz = lax.rem(z + dz, nz)
            if dz:
                copy(28, lzs.at[zz], lz.at[z], {"samp_0": zz}).start()
        lz[z] = lzs[z]
        for q in range(nx):
            xs[q] = chunks[q]
        for dx in far_first(nx):
            xx = lax.rem(x + dx, nx)
            if dx:
                copy(21, xs.at[xx], xr.at[x], {"samp_1": xx}).start()
        xr[x] = xs[x]
        whole(21, xr.at[pl.ds(0, nx - 1)], {"samp_1": lax.rem(x + 1, nx)})
        whole(28, lz.at[pl.ds(0, nz - 1)], zx_peers[0][1])
        vector, full = project_finish(0, jnp.sum(xr[...], axis=0) + jnp.sum(lz[...], axis=0), None)
        ring(5)
        spread_start(0, spread(full))
        return vector, vector + cf[z], gather_rows(1)

    def along_x(values, state, scalars):
        for dx in far_first(nx):
            xx = lax.rem(x + dx, nx)
            part = lax.dot_general(values, xw[:, by_x(xx)], BY_ROWS, preferred_element_type=F32)
            wss[xx] = part.astype(BF16)
            if dx:
                copy(11, wss.at[xx], ws.at[x], {"samp_1": xx}).start()
        ws[x] = wss[x]
        whole(11, ws.at[pl.ds(0, nx - 1)], {"samp_1": lax.rem(x + 1, nx)})
        total = jnp.sum(ws[...].astype(F32), axis=0)
        ridge = (0.5 * lam) * state
        chunks = [total[:, q * wide:(q + 1) * wide] + ridge * jnp.where(z == q, 1.0, 0.0) for q in range(nz)]
        project_start(1, chunks, spz[...].reshape(nz * nh * half, rank))

        for q in range(nz):
            zs[q] = chunks[q]
        for dz in far_first(nz):
            zz = lax.rem(z + dz, nz)
            if dz:
                copy(22, zs.at[zz], zr.at[z], {"samp_0": zz}).start()
        zr[z] = zs[z]
        whole(22, zr.at[pl.ds(0, nz - 1)], zx_peers[0][1])
        vector, full = project_finish(1, jnp.sum(zr[...], axis=0), scalars)
        spread_start(1, spread(full))
        return vector, vector + cf[z], gather_rows(2), jnp.sum(full[:, rank:], axis=0, keepdims=True) * (1.0 / nf)

    def project_start(i, chunks, sketch):
        parts = lax.dot_general(split3(jnp.concatenate(chunks, axis=1)), sketch, BY_ROWS, preferred_element_type=F32)
        projected = parts[:k] + parts[k:2 * k] + parts[2 * k:]
        for q in range(k):
            prs[i, q] = projected[q:q + 1, :]
        for j, peer in y_peers:
            copy(14 + i, prs.at[i, j], pr.at[i, y], peer).start()
        pr[i, y] = prs[i, y]

    def spread(full):
        sketch = spz[...].reshape(nz * nh * half, rank)
        parts = lax.dot_general(split3(ratios * full[:, :rank]), sketch, BY_LANES, preferred_element_type=F32)
        return parts[:k] + parts[k:2 * k] + parts[2 * k:]

    def project_finish(i, part, scalars):
        yhs[i] = part
        copy(12 + i, yhs.at[i], yh.at[i], partner).start()

        whole(14 + i, pr.at[i, pl.ds(0, ny - 1)], y_peers[0][1])
        mine = jnp.sum(pr[i], axis=0)
        if scalars is not None:
            mine = jnp.concatenate([mine, scalars], axis=1)
        across = slice(0, mine.shape[1])
        pzs[i, :, across] = mine
        pz[i, zx, :, across] = mine
        for _, peer in zx_peers:
            copy(16 + i, pzs.at[i, :, across], pz.at[i, zx, :, across], peer).start()
        if i == 0:
            ring(3)

        whole(12 + i, yh.at[i], partner)
        vector = part + yh[i]

        whole(16 + i, pz.at[i, pl.ds(0, nzx - 1), :, across], zx_peers[0][1])
        mine = jnp.sum(pz[i, :, :, across], axis=0)
        pas[i, :, across] = mine
        pa[i, y, :, across] = mine
        for _, peer in y_peers:
            copy(18 + i, pas.at[i, :, across], pa.at[i, y, :, across], peer).start()
        gather_start(1 + i, vector)
        if i == 0:
            ring(4)
        whole(18 + i, pa.at[i, pl.ds(0, ny - 1), :, across], y_peers[0][1])
        return vector, jnp.concatenate([pa[i, q, :, across] for q in range(k)], axis=0)

    loads[0].wait()
    wb[0, :, :half] = w_ref[...]
    wb[0, :, half:] = w_ref[...]
    pl.semaphore_wait(barrier, len(zx_peers) + len(y_peers))
    copy(0, wb.at[0], wb.at[1], partner).start()
    loads[4].wait()
    copy(27, sp.at[x * nh + h], sp.at[x * nh + h], partner).start()
    for load in loads[1:4]:
        load.wait()
    lam = jnp.sum(jnp.where(lax.broadcasted_iota(jnp.int32, (k, k), 0) == lax.broadcasted_iota(jnp.int32, (k, k), 1),
                            lam_ref[...], 0.0), axis=1, keepdims=True)
    values = sv_ref[...].reshape(1, rank)
    ratios = (jnp.min(values, axis=1, keepdims=True) + lam) / (values + lam) - 1.0
    whole(0, wb.at[1], partner)
    own = (lane // half) == h
    weights = jnp.where(own, wb[0], wb[1])
    gather_start(0, weights)
    loads[5].wait()
    pltpu.make_async_copy(x_hbm, xw, local_sem.at[6]).wait()

    logits = feat_sum(0, gather_rows(0))
    probability = jax.nn.sigmoid(logits)
    diag = probability * (1.0 - probability)
    miss = (probability - labels_ref[...].astype(F32)).astype(BF16)
    gradient, gradient_pre, image = along_z(miss, weights)
    residual, direction = -gradient, -gradient_pre
    feat_scalars_start(0, pack(0.5 * lanes(residual * direction), 0.5 * lam * lanes(direction * direction)))
    image = -feat_sum(1, spread_rows(0, image))
    scalars = feat_scalars(0) + pack(jnp.zeros((k, 1), F32), lanes(diag * image * image))
    hess_dir, hess_pre, image_pre, scalars = along_x((diag * image).astype(BF16), direction, scalars)
    res_dot, curvature = unpack(scalars, 0), unpack(scalars, 1)
    step = res_dot / curvature
    residual = residual - step * hess_dir
    precond = direction - step * hess_pre
    feat_scalars_start(1, pack(0.5 * lanes(residual * precond), 0.5 * lam * lanes(precond * precond),
                               0.5 * lam * lanes(precond * direction)))
    image_pre = image - step * feat_sum(2, spread_rows(1, image_pre))
    mine = feat_scalars(1) + pack(jnp.zeros((k, 1), F32), lanes(diag * image_pre * image_pre),
                                  lanes(diag * image_pre * image))
    kzs[...] = mine
    kz[zx * nh + h] = mine
    for dh in reversed(range(nh)):
        for dz in far_first(nz):
            for dx in far_first(nx):
                if dh or dz or dx:
                    peer = {"samp_0": lax.rem(z + dz, nz), "samp_1": lax.rem(x + dx, nx), "samp_2": lax.rem(h + dh, nh)}
                    copy(20, kzs, kz.at[zx * nh + h], peer).start()
    whole(20, kz.at[pl.ds(0, nzx * nh - 1)], partner)
    scalars = jnp.sum(kz[...], axis=0)
    new_dot, pre_pre, pre_dir = (unpack(scalars, place) for place in range(3))
    beta = new_dot / res_dot
    last = new_dot / (pre_pre + 2.0 * beta * pre_dir + beta * beta * curvature)
    update = step * direction + last * (precond + beta * direction)
    update = jnp.where(h == 0, update, pltpu.roll(update, half, 1))
    out_ref[...] = w_ref[...] + update[:, :half]
    for arrived in sent:
        arrived.wait_send()


def shards(sizes, design_matrix, labels, weights, lambdas, sketch, sketch_values):
    nz, nx, nh, nl, nc = sizes
    nzx, nf, ny = nz * nx, nl * nc, nh * nl * nc
    k, half = weights.shape
    wide = 2 * half
    rank = sketch.shape[1]
    vmem = pl.BlockSpec(memory_space=pltpu.VMEM)
    anywhere = pl.BlockSpec(memory_space=pl.ANY)
    dma = pltpu.SemaphoreType.DMA
    return pl.pallas_call(
        functools.partial(kernel, sizes),
        name="step",
        out_shape=jax.ShapeDtypeStruct((k, half), F32),
        in_specs=[anywhere] * 6,
        out_specs=vmem,
        scratch_shapes=[
            pltpu.VMEM(design_matrix.shape, BF16), pltpu.VMEM(design_matrix.shape, BF16),
            pltpu.VMEM((1, design_matrix.shape[0]), jnp.int32), pltpu.VMEM((k, half), F32), pltpu.VMEM((1, k), F32),
            pltpu.VMEM((rank,), F32),
            pltpu.VMEM((nx * nh, half, rank), BF16),
            pltpu.VMEM((2, k, wide), F32),
            pltpu.VMEM((3, nzx, k, wide), BF16), pltpu.VMEM((3, k, wide), BF16),
            pltpu.VMEM((3, nf, k, wide), F32), pltpu.VMEM((3, k, wide), F32),
            pltpu.VMEM((2, nf, 1, wide), F32), pltpu.VMEM((2, 1, wide), F32),
            pltpu.VMEM((nz, k, nx * wide), BF16), pltpu.VMEM((nz, k, nx * wide), BF16),
            pltpu.VMEM((nx, k, nz * wide), BF16), pltpu.VMEM((nx, k, nz * wide), BF16),
            pltpu.VMEM((nz, k, wide), F32), pltpu.VMEM((nz, k, wide), F32),
            pltpu.VMEM((nx, k, nz * wide), BF16), pltpu.VMEM((nx, k, nz * wide), BF16),
            pltpu.VMEM((nx, k, wide), F32), pltpu.VMEM((nx, k, wide), F32),
            pltpu.VMEM((nz, k, wide), F32), pltpu.VMEM((nz, k, wide), F32),
            pltpu.VMEM((nz, nh, half, rank), BF16),
            pltpu.VMEM((2, k, wide), F32), pltpu.VMEM((2, k, wide), F32),
            pltpu.VMEM((2, ny, 1, rank), F32), pltpu.VMEM((2, ny, 1, rank), F32),
            pltpu.VMEM((2, nzx, 1, rank + wide), F32), pltpu.VMEM((2, 1, rank + wide), F32),
            pltpu.VMEM((2, ny, 1, rank + wide), F32), pltpu.VMEM((2, 1, rank + wide), F32),
            pltpu.VMEM((2, nx, k, nz * wide), BF16), pltpu.VMEM((2, k, nz * wide), BF16),
            pltpu.VMEM((nz, k, wide), F32),
            pltpu.VMEM((nzx * nh, 1, wide), F32), pltpu.VMEM((1, wide), F32),
            dma((7,)), dma((29,)), dma((29,)), dma((3, nz)), dma((nz // 2, 2)), dma((2, nx)),
        ],
        compiler_params=pltpu.CompilerParams(collective_id=0, has_side_effects=True, vmem_limit_bytes=32 << 20),
    )(*(pltpu.with_memory_space_constraint(operand, pltpu.HBM) for operand in (
        design_matrix, labels.reshape(1, -1), weights, lambdas.reshape(1, -1), sketch, sketch_values)))


def solution(mesh):
    sizes = (8, 4, 2, 4, 2)
    finer = Mesh(mesh.devices.reshape(sizes), SAMP + FEAT)
    placed = (P(SAMP, FEAT), P(SAMP), P(None, FEAT_SAMP), P(), P(FEAT_SAMP, None), P())
    return jax.shard_map(
        functools.partial(shards, sizes), mesh=finer, in_specs=placed, out_specs=P(None, FEAT_SAMP), check_vma=False
    )
```

```python
import functools

import jax
import jax.numpy as jnp
from jax import lax
from jax.experimental import pallas as pl
from jax.experimental.pallas import tpu as pltpu
from jax.sharding import Mesh
from jax.sharding import PartitionSpec as P

SAMP = ("samp_0", "samp_1", "samp_2")
FEAT = ("feat_0", "feat_1")
FEAT_SAMP = FEAT + SAMP
F32, BF16 = jnp.float32, jnp.bfloat16
BY_LANES = (((1,), (1,)), ((), ()))
BY_ROWS = (((1,), (0,)), ((), ()))


def far_first(n):
    return sorted(range(n), key=lambda d: -min(d, n - d))


def split3(value):
    high = value.astype(BF16)
    rest = value - high.astype(F32)
    mid = rest.astype(BF16)
    low = (rest - mid.astype(F32)).astype(BF16)
    return jnp.concatenate([high, mid, low], axis=0)


def kernel(sizes, x_hbm, labels_hbm, w_hbm, lam_hbm, s_hbm, sv_hbm, out_ref,
           xv, xw, labels_ref, w_ref, lam_ref, sv_ref, sp, wb, ag, ags, ft, fts, fs, fss, rs, rss, rl, rls, ws, wss, xr, xs, zr, zs, spz, yh, yhs,
           pr, prs, pz, pzs, pa, pas, cx, cxs, cf, kz, kzs, local_sem, send_sem, recv_sem, gather_sem, ring_sem, x_sem):
    nz, nx, nh, nl, nc = sizes
    nzx, nf, ny = nz * nx, nl * nc, nh * nl * nc
    k, half = w_ref.shape
    wide = 2 * half
    rank = s_hbm.shape[1]
    z, x, h, l, c = (lax.axis_index(name) for name in SAMP + FEAT)
    zx, f, y = z * nx + x, l * nc + c, (h * nl + l) * nc + c

    zx_peers = []
    for dz in far_first(nz):
        for dx in far_first(nx):
            if dz or dx:
                zz, xx = lax.rem(z + dz, nz), lax.rem(x + dx, nx)
                zx_peers.append((zz * nx + xx, {"samp_0": zz, "samp_1": xx}))
    y_peers, f_peers = [], []
    for dl in far_first(nl):
        for dh in reversed(range(nh)):
            for dc in reversed(range(nc)):
                if dh or dl or dc:
                    hh, ll, cc = lax.rem(h + dh, nh), lax.rem(l + dl, nl), lax.rem(c + dc, nc)
                    y_peers.append(((hh * nl + ll) * nc + cc, {"samp_2": hh, "feat_0": ll, "feat_1": cc}))
                    if not dh:
                        f_peers.append((ll * nc + cc, {"feat_0": ll, "feat_1": cc}))
    partner = {"samp_2": 1 - h}

    loads = [pltpu.make_async_copy(src, dst, local_sem.at[j]) for j, (src, dst) in enumerate(
        [(w_hbm, w_ref), (lam_hbm, lam_ref), (sv_hbm, sv_ref), (labels_hbm, labels_ref), (s_hbm, sp.at[x * nh + h]), (x_hbm, xv)])]
    loads[0].start()
    loads[4].start()
    barrier = pltpu.get_barrier_semaphore()
    for _, peer in [y_peers[-2]] + zx_peers + y_peers[:-2] + y_peers[-1:]:
        pl.semaphore_signal(barrier, inc=1, device_id=peer, device_id_type=pl.DeviceIdType.MESH)

    for j in (1, 2, 3, 5):
        loads[j].start()
    for q in range(nx):
        for zz in range(nz):
            pltpu.make_async_copy(x_hbm.at[:, pl.ds((zz * nx + q) * wide, wide)], xw.at[:, pl.ds((q * nz + zz) * wide, wide)],
                                  local_sem.at[6]).start()

    def copy(phase, src, dst, peer):
        return pltpu.make_async_remote_copy(
            src_ref=src, dst_ref=dst, send_sem=send_sem.at[phase], recv_sem=recv_sem.at[phase],
            device_id=peer, device_id_type=pl.DeviceIdType.MESH)

    sent = []

    def whole(phase, buffer, peer):
        arrived = copy(phase, buffer, buffer, peer)
        arrived.wait_recv()
        sent.append(arrived)

    lane = lax.broadcasted_iota(jnp.int32, (k, wide), 1)
    row = lax.broadcasted_iota(jnp.int32, (k, wide), 0)

    def pack(*columns):
        total = 0.0
        for place, column in enumerate(columns):
            total = total + jnp.where(lane == row + place * k, column, 0.0)
        return jnp.sum(total, axis=0, keepdims=True)

    def unpack(packed, place):
        return jnp.sum(jnp.where(lane == row + place * k, packed, 0.0), axis=1, keepdims=True)

    def lanes(value):
        return jnp.sum(value, axis=1, keepdims=True)

    def gather_start(i, value):
        ags[i] = value.astype(BF16)
        ag[i, zx] = value.astype(BF16)
        for dz in far_first(nz):
            for dx in far_first(nx):
                if dz or dx:
                    zz, xx = lax.rem(z + dz, nz), lax.rem(x + dx, nx)
                    pltpu.make_async_remote_copy(
                        src_ref=ags.at[i], dst_ref=ag.at[i, zx], send_sem=send_sem.at[2 + i], recv_sem=gather_sem.at[i, dz],
                        device_id={"samp_0": zz, "samp_1": xx}, device_id_type=pl.DeviceIdType.MESH).start()

    def arrived_group(phase, place, dz, group):
        pltpu.make_async_remote_copy(
            src_ref=group, dst_ref=group, send_sem=send_sem.at[phase], recv_sem=gather_sem.at[place, dz],
            device_id=zx_peers[0][1], device_id_type=pl.DeviceIdType.MESH).wait_recv()

    def rows_of(field, zz):
        start = pl.multiple_of(zz * (nx * wide), nx * wide)
        return lax.dot_general(field, xv[:, pl.ds(start, nx * wide)], BY_LANES, preferred_element_type=F32)

    def gather_rows(i):
        total = jnp.zeros((k, xv.shape[0]), F32)
        for dz in reversed(far_first(nz)):
            arrived_group(2 + i, i, dz, ag.at[i, pl.ds(0, nx if dz else nx - 1)])
            zz = lax.rem(z + (nz - dz), nz)
            total = total + rows_of(jnp.concatenate([ag[i, zz * nx + q] for q in range(nx)], axis=1), zz)
        sent.append(copy(2 + i, ag.at[i, pl.ds(0, nzx - 1)], ag.at[i, pl.ds(0, nzx - 1)], zx_peers[0][1]))
        return total

    def by_x(xx):
        return pl.ds(pl.multiple_of(xx * (nz * wide), nz * wide), nz * wide)

    def spread_start(i, value):
        cxs[i] = value.astype(BF16)
        for dx in far_first(nx):
            if dx:
                pltpu.make_async_remote_copy(
                    src_ref=cxs.at[i], dst_ref=cx.at[i, x], send_sem=send_sem.at[23 + i], recv_sem=x_sem.at[i, dx],
                    device_id={"samp_1": lax.rem(x + dx, nx)}, device_id_type=pl.DeviceIdType.MESH).start()
        for q in range(nz):
            cf[q] = value[:, q * wide:(q + 1) * wide]

    def spread_rows(i, total):
        for dx in reversed(far_first(nx)):
            xx = lax.rem(x + (nx - dx), nx)
            if dx:
                pltpu.make_async_remote_copy(
                    src_ref=cxs.at[i], dst_ref=cx.at[i, xx], send_sem=send_sem.at[23 + i], recv_sem=x_sem.at[i, dx],
                    device_id={"samp_1": xx}, device_id_type=pl.DeviceIdType.MESH).wait_recv()
                field = cx[i, xx]
            else:
                field = cxs[i]
            total = total + lax.dot_general(field, xw[:, by_x(xx)], BY_LANES, preferred_element_type=F32)
        sent.append(copy(23 + i, cx.at[i, pl.ds(0, nx - 1)], cx.at[i, pl.ds(0, nx - 1)], zx_peers[0][1]))
        return total

    def ring(step):
        ahead, behind = {"samp_0": lax.rem(z + 1, nz)}, {"samp_0": lax.rem(z + nz - 1, nz)}
        for way, peer in ((0, ahead), (1, behind)):
            if step > 1 and (way == 0 or step <= nz // 2):
                last = spz.at[0]
                pltpu.make_async_remote_copy(
                    src_ref=last, dst_ref=last, send_sem=send_sem.at[26], recv_sem=ring_sem.at[step - 2, way],
                    device_id=peer, device_id_type=pl.DeviceIdType.MESH).wait_recv()
            if step <= nz // 2 - way:
                offset = step - 1 if way else nz - (step - 1)
                block = lax.rem(z + offset, nz)
                pltpu.make_async_remote_copy(
                    src_ref=sp.at[pl.ds(x * nh, nh)] if step == 1 else spz.at[block], dst_ref=spz.at[block],
                    send_sem=send_sem.at[26], recv_sem=ring_sem.at[step - 1, way],
                    device_id=peer, device_id_type=pl.DeviceIdType.MESH).start()
        if step == 1:
            spz[z] = sp[pl.ds(x * nh, nh)]
        if step == nz // 2 + 1:
            sent.append(copy(26, spz.at[pl.ds(0, nz - 1)], spz.at[pl.ds(0, nz - 1)], ahead))

    def feat_sum(i, value):
        fts[i] = value
        ft[i, f] = value
        for _, peer in f_peers:
            copy(5 + i, fts.at[i], ft.at[i, f], peer).start()
        if i == 0:
            whole(27, sp.at[x * nh + 1 - h], partner)
            block = sp.at[pl.ds(x * nh, nh)]
            for dx in far_first(nx):
                if dx:
                    copy(1, block, block, {"samp_1": lax.rem(x + dx, nx)}).start()
            ring(1)
        whole(5 + i, ft.at[i, pl.ds(0, nf - 1)], f_peers[0][1])
        return jnp.sum(ft[i], axis=0)

    def feat_scalars_start(i, value):
        fss[i] = value
        fs[i, f] = value
        for _, peer in f_peers:
            copy(8 + i, fss.at[i], fs.at[i, f], peer).start()

    def feat_scalars(i):
        whole(8 + i, fs.at[i, pl.ds(0, nf - 1)], f_peers[0][1])
        return jnp.sum(fs[i], axis=0)

    def along_z(values, state):
        for dz in far_first(nz):
            zz = lax.rem(z + dz, nz)
            start = pl.multiple_of(zz * (nx * wide), nx * wide)
            part = lax.dot_general(values, xv[:, pl.ds(start, nx * wide)], BY_ROWS, preferred_element_type=F32)
            high = part.astype(BF16)
            rss[zz] = high
            rls[zz] = (part - high.astype(F32)).astype(BF16)
            if dz:
                copy(10, rss.at[zz], rs.at[z], {"samp_0": zz}).start()
        rs[z] = rss[z]
        for dz in far_first(nz):
            zz = lax.rem(z + dz, nz)
            if dz:
                copy(25, rls.at[zz], rl.at[z], {"samp_0": zz}).start()
        rl[z] = rls[z]
        whole(10, rs.at[pl.ds(0, nz - 1)], zx_peers[0][1])
        total = jnp.sum(rs[...].astype(F32), axis=0)
        ridge = (0.5 * lam) * state
        chunks = [total[:, q * wide:(q + 1) * wide] + ridge * jnp.where(x == q, 1.0, 0.0) for q in range(nx)]
        whole(1, sp.at[pl.ds(0, (nx - 1) * nh)], partner)
        project_start(0, chunks, sp[...].reshape(nx * nh * half, rank))
        ring(2)

        whole(25, rl.at[pl.ds(0, nz - 1)], zx_peers[0][1])
        low = jnp.sum(rl[...].astype(F32), axis=0)
        for q in range(nx):
            xs[q] = chunks[q] + low[:, q * wide:(q + 1) * wide]
        for dx in far_first(nx):
            xx = lax.rem(x + dx, nx)
            if dx:
                copy(21, xs.at[xx], xr.at[x], {"samp_1": xx}).start()
        xr[x] = xs[x]
        whole(21, xr.at[pl.ds(0, nx - 1)], {"samp_1": lax.rem(x + 1, nx)})
        vector, image, full = project_finish(0, jnp.sum(xr[...], axis=0), None)
        ring(5)
        spread_start(0, spread(full))
        return vector, vector + cf[z], image

    def along_x(values, state, scalars):
        for dx in far_first(nx):
            xx = lax.rem(x + dx, nx)
            part = lax.dot_general(values, xw[:, by_x(xx)], BY_ROWS, preferred_element_type=F32)
            wss[xx] = part.astype(BF16)
            if dx:
                copy(11, wss.at[xx], ws.at[x], {"samp_1": xx}).start()
        ws[x] = wss[x]
        whole(11, ws.at[pl.ds(0, nx - 1)], {"samp_1": lax.rem(x + 1, nx)})
        total = jnp.sum(ws[...].astype(F32), axis=0)
        ridge = (0.5 * lam) * state
        chunks = [total[:, q * wide:(q + 1) * wide] + ridge * jnp.where(z == q, 1.0, 0.0) for q in range(nz)]
        project_start(1, chunks, spz[...].reshape(nz * nh * half, rank))

        for q in range(nz):
            zs[q] = chunks[q]
        for dz in far_first(nz):
            zz = lax.rem(z + dz, nz)
            if dz:
                copy(22, zs.at[zz], zr.at[z], {"samp_0": zz}).start()
        zr[z] = zs[z]
        whole(22, zr.at[pl.ds(0, nz - 1)], zx_peers[0][1])
        vector, image, full = project_finish(1, jnp.sum(zr[...], axis=0), scalars)
        spread_start(1, spread(full))
        return vector, vector + cf[z], image, jnp.sum(full[:, rank:], axis=0, keepdims=True) * (1.0 / nf)

    def project_start(i, chunks, sketch):
        parts = lax.dot_general(split3(jnp.concatenate(chunks, axis=1)), sketch, BY_ROWS, preferred_element_type=F32)
        projected = parts[:k] + parts[k:2 * k] + parts[2 * k:]
        for q in range(k):
            prs[i, q] = projected[q:q + 1, :]
        for j, peer in y_peers:
            copy(14 + i, prs.at[i, j], pr.at[i, y], peer).start()
        pr[i, y] = prs[i, y]

    def spread(full):
        sketch = spz[...].reshape(nz * nh * half, rank)
        parts = lax.dot_general(split3(ratios * full[:, :rank]), sketch, BY_LANES, preferred_element_type=F32)
        return parts[:k] + parts[k:2 * k] + parts[2 * k:]

    def project_finish(i, part, scalars):
        yhs[i] = part
        copy(12 + i, yhs.at[i], yh.at[i], partner).start()

        whole(14 + i, pr.at[i, pl.ds(0, ny - 1)], y_peers[0][1])
        mine = jnp.sum(pr[i], axis=0)
        if scalars is not None:
            mine = jnp.concatenate([mine, scalars], axis=1)
        across = slice(0, mine.shape[1])
        pzs[i, :, across] = mine
        pz[i, zx, :, across] = mine
        for _, peer in zx_peers:
            copy(16 + i, pzs.at[i, :, across], pz.at[i, zx, :, across], peer).start()
        if i == 0:
            ring(3)

        whole(12 + i, yh.at[i], partner)
        vector = part + yh[i]
        gather_start(1 + i, vector)

        whole(16 + i, pz.at[i, pl.ds(0, nzx - 1), :, across], zx_peers[0][1])
        mine = jnp.sum(pz[i, :, :, across], axis=0)
        pas[i, :, across] = mine
        pa[i, y, :, across] = mine
        for _, peer in y_peers:
            copy(18 + i, pas.at[i, :, across], pa.at[i, y, :, across], peer).start()
        if i == 0:
            ring(4)
        image = gather_rows(1 + i)
        whole(18 + i, pa.at[i, pl.ds(0, ny - 1), :, across], y_peers[0][1])
        return vector, image, jnp.concatenate([pa[i, q, :, across] for q in range(k)], axis=0)

    loads[0].wait()
    wb[0, :, :half] = w_ref[...]
    wb[0, :, half:] = w_ref[...]
    pl.semaphore_wait(barrier, len(zx_peers) + len(y_peers))
    copy(0, wb.at[0], wb.at[1], partner).start()
    loads[4].wait()
    copy(27, sp.at[x * nh + h], sp.at[x * nh + h], partner).start()
    for load in loads[1:4]:
        load.wait()
    lam = jnp.sum(jnp.where(lax.broadcasted_iota(jnp.int32, (k, k), 0) == lax.broadcasted_iota(jnp.int32, (k, k), 1),
                            lam_ref[...], 0.0), axis=1, keepdims=True)
    values = sv_ref[...].reshape(1, rank)
    ratios = (jnp.min(values, axis=1, keepdims=True) + lam) / (values + lam) - 1.0
    whole(0, wb.at[1], partner)
    own = (lane // half) == h
    weights = jnp.where(own, wb[0], wb[1])
    gather_start(0, weights)
    loads[5].wait()
    pltpu.make_async_copy(x_hbm, xw, local_sem.at[6]).wait()

    logits = feat_sum(0, gather_rows(0))
    probability = jax.nn.sigmoid(logits)
    diag = probability * (1.0 - probability)
    miss = (probability - labels_ref[...].astype(F32)).astype(BF16)
    gradient, gradient_pre, image = along_z(miss, weights)
    residual, direction = -gradient, -gradient_pre
    feat_scalars_start(0, pack(0.5 * lanes(residual * direction), 0.5 * lam * lanes(direction * direction)))
    image = -feat_sum(1, spread_rows(0, image))
    scalars = feat_scalars(0) + pack(jnp.zeros((k, 1), F32), lanes(diag * image * image))
    hess_dir, hess_pre, image_pre, scalars = along_x((diag * image).astype(BF16), direction, scalars)
    res_dot, curvature = unpack(scalars, 0), unpack(scalars, 1)
    step = res_dot / curvature
    residual = residual - step * hess_dir
    precond = direction - step * hess_pre
    feat_scalars_start(1, pack(0.5 * lanes(residual * precond), 0.5 * lam * lanes(precond * precond),
                               0.5 * lam * lanes(precond * direction)))
    image_pre = image - step * feat_sum(2, spread_rows(1, image_pre))
    mine = feat_scalars(1) + pack(jnp.zeros((k, 1), F32), lanes(diag * image_pre * image_pre),
                                  lanes(diag * image_pre * image))
    kzs[...] = mine
    kz[zx * nh + h] = mine
    for dh in reversed(range(nh)):
        for dz in far_first(nz):
            for dx in far_first(nx):
                if dh or dz or dx:
                    peer = {"samp_0": lax.rem(z + dz, nz), "samp_1": lax.rem(x + dx, nx), "samp_2": lax.rem(h + dh, nh)}
                    copy(20, kzs, kz.at[zx * nh + h], peer).start()
    whole(20, kz.at[pl.ds(0, nzx * nh - 1)], partner)
    scalars = jnp.sum(kz[...], axis=0)
    new_dot, pre_pre, pre_dir = (unpack(scalars, place) for place in range(3))
    beta = new_dot / res_dot
    last = new_dot / (pre_pre + 2.0 * beta * pre_dir + beta * beta * curvature)
    update = step * direction + last * (precond + beta * direction)
    update = jnp.where(h == 0, update, pltpu.roll(update, half, 1))
    out_ref[...] = w_ref[...] + update[:, :half]
    for arrived in sent:
        arrived.wait_send()


def shards(sizes, design_matrix, labels, weights, lambdas, sketch, sketch_values):
    nz, nx, nh, nl, nc = sizes
    nzx, nf, ny = nz * nx, nl * nc, nh * nl * nc
    k, half = weights.shape
    wide = 2 * half
    rank = sketch.shape[1]
    vmem = pl.BlockSpec(memory_space=pltpu.VMEM)
    anywhere = pl.BlockSpec(memory_space=pl.ANY)
    dma = pltpu.SemaphoreType.DMA
    return pl.pallas_call(
        functools.partial(kernel, sizes),
        name="step",
        out_shape=jax.ShapeDtypeStruct((k, half), F32),
        in_specs=[anywhere] * 6,
        out_specs=vmem,
        scratch_shapes=[
            pltpu.VMEM(design_matrix.shape, BF16), pltpu.VMEM(design_matrix.shape, BF16),
            pltpu.VMEM((1, design_matrix.shape[0]), jnp.int32), pltpu.VMEM((k, half), F32), pltpu.VMEM((1, k), F32),
            pltpu.VMEM((rank,), F32),
            pltpu.VMEM((nx * nh, half, rank), BF16),
            pltpu.VMEM((2, k, wide), F32),
            pltpu.VMEM((3, nzx, k, wide), BF16), pltpu.VMEM((3, k, wide), BF16),
            pltpu.VMEM((3, nf, k, wide), F32), pltpu.VMEM((3, k, wide), F32),
            pltpu.VMEM((2, nf, 1, wide), F32), pltpu.VMEM((2, 1, wide), F32),
            pltpu.VMEM((nz, k, nx * wide), BF16), pltpu.VMEM((nz, k, nx * wide), BF16),
            pltpu.VMEM((nz, k, nx * wide), BF16), pltpu.VMEM((nz, k, nx * wide), BF16),
            pltpu.VMEM((nx, k, nz * wide), BF16), pltpu.VMEM((nx, k, nz * wide), BF16),
            pltpu.VMEM((nx, k, wide), F32), pltpu.VMEM((nx, k, wide), F32),
            pltpu.VMEM((nz, k, wide), F32), pltpu.VMEM((nz, k, wide), F32),
            pltpu.VMEM((nz, nh, half, rank), BF16),
            pltpu.VMEM((2, k, wide), F32), pltpu.VMEM((2, k, wide), F32),
            pltpu.VMEM((2, ny, 1, rank), F32), pltpu.VMEM((2, ny, 1, rank), F32),
            pltpu.VMEM((2, nzx, 1, rank + wide), F32), pltpu.VMEM((2, 1, rank + wide), F32),
            pltpu.VMEM((2, ny, 1, rank + wide), F32), pltpu.VMEM((2, 1, rank + wide), F32),
            pltpu.VMEM((2, nx, k, nz * wide), BF16), pltpu.VMEM((2, k, nz * wide), BF16),
            pltpu.VMEM((nz, k, wide), F32),
            pltpu.VMEM((nzx * nh, 1, wide), F32), pltpu.VMEM((1, wide), F32),
            dma((7,)), dma((28,)), dma((28,)), dma((3, nz)), dma((nz // 2, 2)), dma((2, nx)),
        ],
        compiler_params=pltpu.CompilerParams(collective_id=0, has_side_effects=True, vmem_limit_bytes=32 << 20),
    )(*(pltpu.with_memory_space_constraint(operand, pltpu.HBM) for operand in (
        design_matrix, labels.reshape(1, -1), weights, lambdas.reshape(1, -1), sketch, sketch_values)))


def solution(mesh):
    sizes = (8, 4, 2, 4, 2)
    finer = Mesh(mesh.devices.reshape(sizes), SAMP + FEAT)
    placed = (P(SAMP, FEAT), P(SAMP), P(None, FEAT_SAMP), P(), P(FEAT_SAMP, None), P())
    return jax.shard_map(
        functools.partial(shards, sizes), mesh=finer, in_specs=placed, out_specs=P(None, FEAT_SAMP), check_vma=False
    )
```
